32 devices in a mesh: batch: 8 (over y, x, core), seq: 4 (over z).
Axes of the slice: x: 2, y: 2, z: 4, core: 2. Of those that a mesh axis runs over, the one named last changes fastest.
Arguments:
- tokens: bfloat16 [32768, 1024], P(('batch', 'seq')), may hold values from -6 to 6
- seq_lengths: int32 [8, 4], P('batch'), may hold values from 0 to 2048, as said below
- attn_gain: float32 [1024], replicated, may hold values from 0.5 to 1.5
- attn_shift: float32 [1024], replicated, may hold values from -2 to 2
- qkv_weight: bfloat16 [1024, 3072], replicated, may hold values from -0.1875 to 0.1875
- qkv_bias: float32 [3072], replicated, may hold values from -3 to 3
- dense_weight: bfloat16 [1024, 1024], replicated, may hold values from -1.5 to 1.5
- dense_bias: float32 [1024], replicated, may hold values from -2 to 2
- mlp_gain: float32 [1024], replicated, may hold values from 0.5 to 1.5
- mlp_shift: float32 [1024], replicated, may hold values from -2 to 2
- expand_weight: bfloat16 [1024, 4096], replicated, may hold values from -0.1875 to 0.1875
- expand_bias: float32 [4096], replicated, may hold values from -3 to 3
- reduce_weight: bfloat16 [4096, 1024], replicated, may hold values from -0.09375 to 0.09375
- reduce_bias: float32 [1024], replicated, may hold values from -2 to 2
- out_grad: bfloat16 [32768, 1024], P(('batch', 'seq')), may hold values from -6 to 6
Outputs:
- layer_out: bfloat16 [32768, 1024], P(('batch', 'seq'))
- input_grad: bfloat16 [32768, 1024], P(('batch', 'seq'))
- attngain_grad: float32 [1024], P(('batch', 'seq'))
- attnshift_grad: float32 [1024], P(('batch', 'seq'))
- qkvweight_grad: float32 [1024, 3072], P(('batch', 'seq'))
- qkvbias_grad: float32 [3072], P(('batch', 'seq'))
- denseweight_grad: float32 [1024, 1024], P(('batch', 'seq'))
- densebias_grad: float32 [1024], P(('batch', 'seq'))
- mlpgain_grad: float32 [1024], P(('batch', 'seq'))
- mlpshift_grad: float32 [1024], P(('batch', 'seq'))
- expandweight_grad: float32 [1024, 4096], P(('batch', 'seq'))
- expandbias_grad: float32 [4096], P(('batch', 'seq'))
- reduceweight_grad: float32 [4096, 1024], P(('batch', 'seq'))
- reducebias_grad: float32 [1024], P(('batch', 'seq'))
The draws below stay inside these ranges and needn't reach their ends.
Inputs may be any that keep to these rules, and one draw needn't show every extreme that they name: `seq_lengths`: row b lists the lengths of the two or three sequences of batch group b in the order in which they lie among its 4096 tokens: each is 1024 or 2048, they add up to 4096, and the unused entries, at the end of the row, are 0. Every group holds a sequence of 2048 tokens.
All inputs are finite; a program needn't handle non-finite values.
Results may differ from the reference program's by a relative error of at most 0.0093.
Values may be sent and summed in bfloat16 or wider, within the bound.
A program may use at most 192 MiB of HBM per device.

```python
import math
import jax
import jax.numpy as jnp
from jax import lax

D = 1024
HEADS = 16
HEAD_DIM = 64
ROT = 16
FF = 4096
TOK_DEV = 1024
BLOCK = 512
GROUPS = 8
TOKENS = 32768


def draw_seq_lengths(key, part):
    patterns = jnp.array([[2, 2, 0, 0], [2, 1, 1, 0], [1, 2, 1, 0], [1, 1, 2, 0]], dtype=jnp.int32)
    picks = jax.random.randint(jax.random.fold_in(key, 23), (GROUPS,), 0, 4).astype(jnp.int32)
    return (patterns[picks] * TOK_DEV).astype(jnp.int32)


def level_of(rng, dims, shards, least, top_value):
    loudness, own = 1.0, jax.random.fold_in(rng, 6)
    for position, shards_of in shards:
        steps = jnp.exp(jax.random.uniform(jax.random.fold_in(own, position), (shards_of,), jnp.float32, least / len(shards), top_value / len(shards)))
        loudness = loudness * jnp.repeat(steps, dims[position] // shards_of).reshape([-1 if axis == position else 1 for axis in range(len(dims))])
    return loudness


def centred(own_key, shape, scale, bound, split=(), kind=jnp.bfloat16):
    values = scale * jax.random.normal(own_key, shape, jnp.float32)
    if split:
        values = values * level_of(own_key, shape, split, -0.22, 0.18)
    return jnp.clip(values, -bound, bound).astype(kind)


def setup_inputs(seed: int = 0) -> dict:
    arg_keys = jax.random.split(jax.random.key(seed), 16)
    tokens = centred(arg_keys[0], (TOKENS, D), 1.0, 6.0, ((0, 32),))
    seq_lengths = draw_seq_lengths(jax.random.fold_in(arg_keys[15], 71), 0)
    attn_gain = jnp.clip(1.0 + 0.1 * jax.random.normal(arg_keys[2], (D,), jnp.float32), 0.5, 1.5)
    attn_shift = centred(arg_keys[3], (D,), 0.3, 2.0, (), jnp.float32)
    qkv_weight = centred(arg_keys[4], (D, 3 * D), D ** -0.5, 0.1875)
    qkv_bias = centred(arg_keys[5], (3 * D,), 0.5, 3.0, (), jnp.float32)
    dense_weight = centred(arg_keys[6], (D, D), 16 ** -0.5, 1.5)
    dense_bias = centred(arg_keys[7], (D,), 0.3, 2.0, (), jnp.float32)
    mlp_gain = jnp.clip(1.0 + 0.1 * jax.random.normal(arg_keys[8], (D,), jnp.float32), 0.5, 1.5)
    mlp_shift = centred(arg_keys[9], (D,), 0.3, 2.0, (), jnp.float32)
    expand_weight = centred(arg_keys[10], (D, FF), D ** -0.5, 0.1875)
    expand_bias = centred(arg_keys[11], (FF,), 0.5, 3.0, (), jnp.float32)
    reduce_weight = centred(arg_keys[12], (FF, D), FF ** -0.5, 0.09375)
    reduce_bias = centred(arg_keys[13], (D,), 0.3, 2.0, (), jnp.float32)
    out_grad = centred(arg_keys[14], (TOKENS, D), 1.0, 6.0, ((0, 32),))
    return dict(tokens=tokens, seq_lengths=seq_lengths, attn_gain=attn_gain, attn_shift=attn_shift, qkv_weight=qkv_weight, qkv_bias=qkv_bias, dense_weight=dense_weight, dense_bias=dense_bias, mlp_gain=mlp_gain, mlp_shift=mlp_shift, expand_weight=expand_weight, expand_bias=expand_bias, reduce_weight=reduce_weight, reduce_bias=reduce_bias, out_grad=out_grad)


@jax.custom_vjp
def low(v):
    return lax.optimization_barrier(v.astype(jnp.bfloat16)).astype(jnp.float32)

@jax.custom_vjp
def low_back(v):
    return v

def low_keep(v):
    return (low(v), None)

def low_pass(kept, grad):
    return (grad,)

def back_keep(v):
    return (v, None)

def back_low(kept, grad):
    return (low(grad),)
low.defvjp(low_keep, low_pass)
low_back.defvjp(back_keep, back_low)
PRECISE = lax.Precision.HIGHEST
EPSILON = 1e-05
MASKED = -1e+30

def matmul(left_op, right_op):
    return jnp.dot(left_op, right_op, precision=PRECISE, preferred_element_type=jnp.float32)

def layer_norm(inputs, norm_gain, norm_shift):
    row_mean = lax.optimization_barrier(jnp.mean(inputs, axis=-1, keepdims=True))
    centered = inputs - row_mean
    variance = lax.optimization_barrier(jnp.mean(centered * centered, axis=-1, keepdims=True))
    return centered * lax.rsqrt(variance + EPSILON) * norm_gain + norm_shift

def angles(positions):
    frequency = jnp.exp(jnp.arange(ROT // 2, dtype=jnp.float32) * (-2.0 * math.log(10000.0) / ROT))
    phases = positions.astype(jnp.float32)[:, None] * frequency[None, :]
    phases = jnp.concatenate([phases, phases], axis=-1)
    return (jnp.cos(phases), jnp.sin(phases))

def rotary(operand, cos_part, sin_part):
    half_rot = ROT // 2
    rotated_part = operand[..., :ROT]
    turned = jnp.concatenate([-rotated_part[..., half_rot:], rotated_part[..., :half_rot]], axis=-1)
    turned_part = rotated_part * cos_part[:, None, :] + turned * sin_part[:, None, :]
    return jnp.concatenate([turned_part, operand[..., ROT:]], axis=-1)

def first_rows(seq_starts, row_index):
    return lax.optimization_barrier(jnp.max(jnp.where(seq_starts[None, :] <= row_index[:, None], seq_starts[None, :], 0), axis=1))

def attend(queries, key_rows, values, row_first):
    row_count = queries.shape[0]
    score_scale = 1.0 / math.sqrt(HEAD_DIM)
    key_index = jnp.arange(row_count, dtype=jnp.int32)

    def one_block(block_index):
        begin = (block_index * BLOCK).astype(jnp.int32)
        query_block = lax.dynamic_slice_in_dim(queries, begin, BLOCK, 0)
        block_first = lax.dynamic_slice_in_dim(row_first, begin, BLOCK, 0)
        row_index = begin + jnp.arange(BLOCK, dtype=jnp.int32)
        scores = low_back(jnp.einsum('qhe,khe->hqk', query_block, key_rows, precision=PRECISE) * score_scale)
        allowed = jnp.logical_and(key_index[None, :] >= block_first[:, None], key_index[None, :] <= row_index[:, None])
        scores = jnp.where(allowed[None], scores, MASKED)
        running_max = lax.optimization_barrier(jnp.max(scores, axis=-1, keepdims=True))
        logsum = running_max + jnp.log(lax.optimization_barrier(jnp.sum(jnp.exp(scores - running_max), axis=-1, keepdims=True)))
        weights = low(jnp.exp(scores - logsum))
        return jnp.einsum('hqk,khe->qhe', weights, values, precision=PRECISE)
    blocks = lax.map(jax.checkpoint(one_block), jnp.arange(row_count // BLOCK, dtype=jnp.int32))
    return blocks.reshape(row_count, HEADS * HEAD_DIM)

def group_layer(inputs, params, cos_part, sin_part, row_first):
    attn_gain, attn_shift, qkv_weight, qkv_bias, dense_weight, dense_bias, mlp_gain, mlp_shift, expand_weight, expand_bias, reduce_weight, reduce_bias = params
    row_count = inputs.shape[0]
    first_norm = low(layer_norm(inputs, attn_gain, attn_shift))
    mixed = low_back(matmul(first_norm, qkv_weight) + qkv_bias).reshape(row_count, HEADS, 3, HEAD_DIM)
    queries = low(rotary(mixed[:, :, 0], cos_part, sin_part))
    key_rows = low(rotary(mixed[:, :, 1], cos_part, sin_part))
    values = low(mixed[:, :, 2])
    joined = low(low_back(attend(queries, key_rows, values, row_first)))
    attn_branch = matmul(joined, dense_weight) + dense_bias
    second_norm = low(layer_norm(inputs, mlp_gain, mlp_shift))
    mlp_input = low_back(matmul(second_norm, expand_weight) + expand_bias)
    active = low(jax.nn.gelu(mlp_input, approximate=False))
    mlp_branch = matmul(active, reduce_weight) + reduce_bias
    return inputs + attn_branch + mlp_branch

def reference(tokens, seq_lengths, attn_gain, attn_shift, qkv_weight, qkv_bias, dense_weight, dense_bias, mlp_gain, mlp_shift, expand_weight, expand_bias, reduce_weight, reduce_bias, out_grad):
    params = tuple((weight.astype(jnp.float32) for weight in (attn_gain, attn_shift, qkv_weight, qkv_bias, dense_weight, dense_bias, mlp_gain, mlp_shift, expand_weight, expand_bias, reduce_weight, reduce_bias)))
    groups = seq_lengths.shape[0]
    model_width = tokens.shape[1]
    group_len = tokens.shape[0] // groups
    group_inputs = tokens.astype(jnp.float32).reshape(groups, group_len, model_width)
    group_cots = out_grad.astype(jnp.float32).reshape(groups, group_len, model_width)

    def scan_step(grad_total, group_item):
        inputs, cotangent, lengths = group_item
        seq_ends = jnp.cumsum(lengths).astype(jnp.int32)
        seq_starts = (seq_ends - lengths).astype(jnp.int32)
        row_index = jnp.arange(group_len, dtype=jnp.int32)
        row_first = first_rows(seq_starts, row_index).astype(jnp.int32)
        cos_part, sin_part = angles(row_index - row_first)

        def forward(inputs_in, params_in):
            return group_layer(inputs_in, params_in, cos_part, sin_part, row_first)
        result, pullback = jax.vjp(forward, inputs, params)
        inputs_grad, param_grads = pullback(cotangent)
        grad_total = jax.tree.map(lambda first_op, second_op: first_op + second_op, grad_total, param_grads)
        return (grad_total, (result.astype(jnp.bfloat16), inputs_grad.astype(jnp.bfloat16)))
    zero_grads = jax.tree.map(jnp.zeros_like, params)
    grad_total, (outputs, inputs_grads) = lax.scan(scan_step, zero_grads, (group_inputs, group_cots, seq_lengths))
    return (outputs.reshape(-1, model_width), inputs_grads.reshape(-1, model_width), grad_total[0], grad_total[1], grad_total[2], grad_total[3], grad_total[4], grad_total[5], grad_total[6], grad_total[7], grad_total[8], grad_total[9], grad_total[10], grad_total[11])
```

```python
from functools import partial
import math

import jax
import jax.numpy as jnp
from jax import lax
from jax.experimental import pallas as pl
from jax.experimental.pallas import tpu as pltpu
from jax.sharding import PartitionSpec as P

HEAD_DIM = 64
ROT = 16
PAIR = 2 * HEAD_DIM
EPSILON = 1e-05
MASKED = -1e30
SCALE = 1.0 / math.sqrt(HEAD_DIM)
QB = 256
FB = 512
ROWS = 128
F32 = jnp.float32
BF16 = jnp.bfloat16
VMEM_LIMIT = 60 << 20


def dot(left, right):
    return jnp.dot(left, right, preferred_element_type=F32)


def dot_t(left, right):
    return lax.dot_general(left, right, (((1,), (1,)), ((), ())), preferred_element_type=F32)


def params():
    return pltpu.CompilerParams(vmem_limit_bytes=VMEM_LIMIT)


def cost(flops, nbytes):
    return pl.CostEstimate(flops=int(flops), bytes_accessed=int(nbytes), transcendentals=0)


def whole(shape):
    return pl.BlockSpec(shape, lambda i: (0,) * len(shape), pipeline_mode=pl.Buffered(1))


def statistics(x):
    mean = jnp.mean(x, axis=-1, keepdims=True)
    centered = x - mean
    variance = jnp.mean(centered * centered, axis=-1, keepdims=True)
    rstd = lax.rsqrt(variance + EPSILON)
    return centered * rstd, rstd


def norm_rows(x_ref, gain_ref, shift_ref, out_ref):
    def step(i, carry):
        rows = pl.ds(pl.multiple_of(i * ROWS, ROWS), ROWS)
        xn, _ = statistics(x_ref[rows, :].astype(F32))
        out_ref[rows, :] = (xn * gain_ref[...] + shift_ref[...]).astype(BF16)
        return carry

    lax.fori_loop(0, x_ref.shape[0] // ROWS, step, 0)


def norm_back(x_ref, gain_ref, grad_ref, gaingrad_ref, shiftgrad_ref, emit):
    gaingrad_ref[...] = jnp.zeros_like(gaingrad_ref)
    shiftgrad_ref[...] = jnp.zeros_like(shiftgrad_ref)

    def step(i, carry):
        rows = pl.ds(pl.multiple_of(i * ROWS, ROWS), ROWS)
        xn, rstd = statistics(x_ref[rows, :].astype(F32))
        grad = grad_ref[rows, :]
        gaingrad_ref[...] += jnp.sum(grad * xn, axis=0, keepdims=True)
        shiftgrad_ref[...] += jnp.sum(grad, axis=0, keepdims=True)
        scaled = grad * gain_ref[...]
        mean_s = jnp.mean(scaled, axis=-1, keepdims=True)
        mean_sx = jnp.mean(scaled * xn, axis=-1, keepdims=True)
        emit(rows, rstd * (scaled - mean_s - xn * mean_sx))
        return carry

    lax.fori_loop(0, x_ref.shape[0] // ROWS, step, 0)


def build_tables(angle_ref, tab_ref):
    half = ROT // 2
    cos8, sin8 = angle_ref[0:half, :], angle_ref[half:ROT, :]
    rest = HEAD_DIM - ROT
    count = cos8.shape[1]
    ones = jnp.ones((rest, count), F32)
    zeros = jnp.zeros((rest, count), F32)
    z8 = jnp.zeros_like(sin8)
    tab_ref[0] = jnp.concatenate([cos8, cos8, ones] * 2, axis=0).T
    tab_ref[1] = jnp.concatenate([-sin8, z8, zeros] * 2, axis=0).T
    tab_ref[2] = jnp.concatenate([z8, sin8, zeros] * 2, axis=0).T


def turn(u, tab_ref, sign):
    half = ROT // 2
    ahead = pltpu.roll(u, PAIR - half, 1)
    behind = pltpu.roll(u, half, 1)
    return u * tab_ref[0] + sign * (ahead * tab_ref[1] + behind * tab_ref[2])


def low_lanes(shape):
    return lax.broadcasted_iota(jnp.int32, shape, 1) < HEAD_DIM


def project_kernel(x_ref, gain_ref, shift_ref, w_ref, b_ref, ang_ref, og_ref, wd_ref,
                   q_ref, kv_ref, do_ref, norm, tab):
    @pl.when(pl.program_id(0) == 0)
    def _():
        norm_rows(x_ref, gain_ref, shift_ref, norm)
        build_tables(ang_ref, tab)

    mixed = dot(norm[...], w_ref[...]) + b_ref[...]
    t0, t1, t2 = mixed[:, :PAIR], mixed[:, PAIR:2 * PAIR], mixed[:, 2 * PAIR:]
    low = low_lanes(t0.shape)
    q = jnp.where(low, t0, t1)
    k = pltpu.roll(jnp.where(low, t2, t0), HEAD_DIM, 1)
    v = jnp.where(low, t1, t2)
    q_ref[...] = turn(q, tab, 1.0).astype(BF16)
    kv_ref[0] = turn(k, tab, 1.0).astype(BF16)
    kv_ref[1] = v.astype(BF16)
    do_ref[...] = dot_t(og_ref[...], wd_ref[...]).astype(BF16)


def project(x, gain, shift, w, b, ang, og, wd):
    rows, width = x.shape
    pairs = width // PAIR
    tok = pl.BlockSpec((rows, PAIR), lambda i: (0, i))
    return pl.pallas_call(
        project_kernel,
        grid=(pairs,),
        out_shape=(
            jax.ShapeDtypeStruct((rows, width), BF16),
            jax.ShapeDtypeStruct((2, rows, width), BF16),
            jax.ShapeDtypeStruct((rows, width), BF16),
        ),
        in_specs=[
            whole((rows, width)), whole((1, width)), whole((1, width)),
            pl.BlockSpec((width, 3 * PAIR), lambda i: (0, i)),
            pl.BlockSpec((1, 3 * PAIR), lambda i: (0, i)),
            whole(ang.shape), whole((rows, width)),
            pl.BlockSpec((PAIR, width), lambda i: (i, 0)),
        ],
        out_specs=(tok, pl.BlockSpec((2, rows, PAIR), lambda i: (0, 0, i)), tok),
        scratch_shapes=[pltpu.VMEM((rows, width), BF16), pltpu.VMEM((3, rows, PAIR), F32)],
        compiler_params=params(),
        cost_estimate=cost(8 * rows * width * width, 24 * rows * width),
        name="project",
    )(x, gain, shift, w, b, ang, og, wd)


def gelu_parts(h):
    z = jnp.abs(h) * math.sqrt(0.5)
    t = 1.0 / (1.0 + 0.5 * z)
    poly = jnp.full_like(t, 0.17087277)
    for c in (-0.82215223, 1.48851587, -1.13520398, 0.27886807, -0.18628806, 0.09678418,
              0.37409196, 1.00002368, -1.26551223):
        poly = poly * t + c
    zz = z * z
    tail = 0.5 * t * jnp.exp(poly - zz)
    cdf = jnp.where(h >= 0, 1.0 - tail, tail)
    slope = cdf + h * (jnp.exp(-zz) * (1.0 / math.sqrt(2.0 * math.pi)))
    return h * cdf, slope


def mlp_kernel(ndev, x_ref, gain_ref, shift_ref, we_ref, be_ref, wr_ref, og_ref,
               mid_ref, part_ref, grads_ref, dbe_ref, dog_ref, dgain_ref, dshift_ref,
               norm, norm_t, sg):
    step = pl.program_id(0)
    width = x_ref.shape[1]
    hidden_all = FB * pl.num_programs(0)
    take = grads_ref.shape[0] // ndev

    @pl.when(step == 0)
    def _():
        norm_rows(x_ref, gain_ref, shift_ref, norm)
        norm_t[...] = norm[...].T
        mid_ref[...] = jnp.zeros_like(mid_ref)
        sg[...] = jnp.zeros_like(sg)
        dog_ref[...] = jnp.sum(og_ref[...].astype(F32), axis=0, keepdims=True)
        grads_ref[:, GRAD_COLS:] = jnp.zeros((grads_ref.shape[0], grads_ref.shape[1] - GRAD_COLS), BF16)

    h = dot(norm[...], we_ref[...]) + be_ref[...]
    active, slope = gelu_parts(h)
    active = active.astype(BF16)
    mid_ref[...] += dot(active, wr_ref[...])
    hidden = (dot_t(og_ref[...], wr_ref[...]) * slope).astype(BF16)
    dwr = dot(active.T, og_ref[...]).astype(BF16)
    ratio = GRAD_COLS // 2 // width
    for piece in range(FB // take):
        group, j = piece // ratio, piece % ratio
        base = pl.multiple_of(step * (FB // ratio), FB // ratio)
        grads_ref[pl.ds(base + group * take, take), GRAD_COLS // 2 + j * width:GRAD_COLS // 2 + (j + 1) * width] = (
            dwr[piece * take:(piece + 1) * take, :])
    cols = pl.ds(pl.multiple_of(step * FB, FB), FB)
    grads_ref[:, cols] = dot(norm_t[...], hidden).astype(BF16)
    dbe_ref[...] = jnp.sum(hidden.astype(F32), axis=0, keepdims=True)
    sg[...] += dot_t(hidden, we_ref[...])

    @pl.when(step == pl.num_programs(0) - 1)
    def _():
        def emit(rows, part):
            part_ref[rows, :] = part

        norm_back(x_ref, gain_ref, sg, dgain_ref, dshift_ref, emit)


GRAD_COLS = 8192
GRAD_PAD = 256


def mlp(ndev, x, gain, shift, we, be, wr, og):
    rows, width = x.shape
    hidden = we.shape[1]
    full = whole((rows, width))
    vec = whole((1, width))
    fshape, vshape = jax.ShapeDtypeStruct((rows, width), F32), jax.ShapeDtypeStruct((1, width), F32)
    gshape = (width, GRAD_COLS + GRAD_PAD)
    return pl.pallas_call(
        partial(mlp_kernel, ndev),
        grid=(hidden // FB,),
        out_shape=(fshape, fshape, jax.ShapeDtypeStruct(gshape, BF16),
                   jax.ShapeDtypeStruct((1, hidden), F32), vshape, vshape, vshape),
        in_specs=[
            full, vec, vec,
            pl.BlockSpec((width, FB), lambda i: (0, i)),
            pl.BlockSpec((1, FB), lambda i: (0, i)),
            pl.BlockSpec((FB, width), lambda i: (i, 0)),
            full,
        ],
        out_specs=(full, full, whole(gshape), pl.BlockSpec((1, FB), lambda i: (0, i)), vec, vec, vec),
        scratch_shapes=[pltpu.VMEM((rows, width), BF16), pltpu.VMEM((width, rows), BF16),
                        pltpu.VMEM((rows, width), F32)],
        compiler_params=params(),
        cost_estimate=cost(12 * rows * width * hidden, 8 * width * hidden),
        name="mlp",
    )(x, gain, shift, we, be, wr, og)


def attend_kernel(flag_ref, q_ref, kv_ref, kvp_ref, do_ref, o_ref, dq_ref, dkv_ref, dkvp_ref,
                  pt, ds, kvt, qm, dom):
    rows_all = q_ref.shape[0]
    nq = rows_all // QB

    def run(prev):
        base = 0 if prev else nq
        sources = [(kvp_ref, i) for i in range(nq)] + [(kv_ref, i) for i in range(nq)]

        def block(which, b):
            ref, i = sources[b]
            return ref[which, i * QB:(i + 1) * QB, :]

        for which in range(2):
            if prev:
                kvt[which, :, :rows_all] = kvp_ref[which].T
            kvt[which, :, rows_all:] = kv_ref[which].T
        lane = lax.broadcasted_iota(jnp.int32, (QB, PAIR), 1)
        sub = lax.broadcasted_iota(jnp.int32, (PAIR, QB), 0)
        causal = lax.broadcasted_iota(jnp.int32, (QB, QB), 0) <= lax.broadcasted_iota(
            jnp.int32, (QB, QB), 1)
        for j in range(nq):
            rows = slice(j * QB, (j + 1) * QB)
            q = q_ref[rows, :] * jnp.asarray(SCALE, BF16)
            qt = q.T
            dot_rows = do_ref[rows, :].astype(F32).T
            blocks = range(base, nq + j + 1)
            k0, k1 = base * QB, (nq + j + 1) * QB
            outs, scaled, dqs = [], [], []
            for h in range(2):
                hs = slice(h * HEAD_DIM, (h + 1) * HEAD_DIM)
                qm[h, rows, :] = jnp.where((lane < HEAD_DIM) == (h == 0), q, jnp.zeros_like(q))
                qtm = jnp.where((sub < HEAD_DIM) == (h == 0), qt, jnp.zeros_like(qt))
                scores, top = [], None
                for b in blocks:
                    s = dot(block(0, b), qtm)
                    if b == nq + j:
                        s = jnp.where(causal, s, MASKED)
                    scores.append(s)
                    part = jnp.max(s.reshape(QB // 8, 8, QB), axis=0)
                    top = part if top is None else jnp.maximum(top, part)
                top = jnp.max(top, axis=0, keepdims=True)
                total = None
                for b, s in zip(blocks, scores):
                    p = jnp.exp(s - top)
                    part = jnp.sum(p.reshape(QB // 8, 8, QB), axis=0)
                    total = part if total is None else total + part
                    pt[h, b * QB:(b + 1) * QB, rows] = p.astype(BF16)
                inv = 1.0 / jnp.sum(total, axis=0, keepdims=True)
                out_t = dot(kvt[1, hs, k0:k1], pt[h, k0:k1, rows]) * inv
                dol_t = dot_rows[hs] * inv
                delta = jnp.sum(dol_t * out_t, axis=0, keepdims=True)
                outs.append(out_t)
                scaled.append(dol_t)
                zero = jnp.zeros((HEAD_DIM, QB), BF16)
                dol_b = dol_t.astype(BF16)
                dol_m = jnp.concatenate([dol_b, zero] if h == 0 else [zero, dol_b], axis=0)
                for b in blocks:
                    dp = dot(block(1, b), dol_m)
                    d = pt[h, b * QB:(b + 1) * QB, rows].astype(F32) * (dp - delta)
                    ds[h, b * QB:(b + 1) * QB, rows] = d.astype(BF16)
                dqs.append(dot(kvt[0, hs, k0:k1], ds[h, k0:k1, rows]) * SCALE)
            o_ref[rows, :] = jnp.concatenate(outs, 0).T.astype(BF16)
            dq_ref[rows, :] = jnp.concatenate(dqs, 0).T.astype(BF16)
            dol = jnp.concatenate(scaled, 0).T.astype(BF16)
            for h in range(2):
                dom[h, rows, :] = jnp.where((lane < HEAD_DIM) == (h == 0), dol, jnp.zeros_like(dol))
        for b in range(base, 2 * nq):
            q0 = max(0, b - nq) * QB
            br = slice(b * QB, (b + 1) * QB)
            dk = dot(ds[0, br, q0:], qm[0, q0:, :]) + dot(ds[1, br, q0:], qm[1, q0:, :])
            dv = dot(pt[0, br, q0:], dom[0, q0:, :]) + dot(pt[1, br, q0:], dom[1, q0:, :])
            ref, i = (dkvp_ref, b) if b < nq else (dkv_ref, b - nq)
            ref[0, i * QB:(i + 1) * QB, :] = dk.astype(BF16)
            ref[1, i * QB:(i + 1) * QB, :] = dv.astype(BF16)

    @pl.when(flag_ref[0] == 1)
    def _():
        run(True)

    @pl.when(flag_ref[0] == 0)
    def _():
        run(False)
        dkvp_ref[...] = jnp.zeros_like(dkvp_ref)


def attend(flag, q, kv, kvp, do, first, pairs):
    rows = q.shape[0]
    width = pairs * PAIR
    tok_in = pl.BlockSpec((rows, PAIR), lambda i, f: (0, first + i))
    kv_in = pl.BlockSpec((2, rows, PAIR), lambda i, f: (0, 0, first + i))
    tok_out = pl.BlockSpec((rows, PAIR), lambda i, f: (0, i))
    kv_out = pl.BlockSpec((2, rows, PAIR), lambda i, f: (0, 0, i))
    tok_shape = jax.ShapeDtypeStruct((rows, width), BF16)
    kv_shape = jax.ShapeDtypeStruct((2, rows, width), BF16)
    return pl.pallas_call(
        attend_kernel,
        out_shape=(tok_shape, tok_shape, kv_shape, kv_shape),
        grid_spec=pltpu.PrefetchScalarGridSpec(
            num_scalar_prefetch=1,
            grid=(pairs,),
            in_specs=[tok_in, kv_in, kv_in, tok_in],
            out_specs=(tok_out, tok_out, kv_out, kv_out),
            scratch_shapes=[
                pltpu.VMEM((2, 2 * rows, rows), BF16),
                pltpu.VMEM((2, 2 * rows, rows), BF16),
                pltpu.VMEM((2, PAIR, 2 * rows), BF16),
                pltpu.VMEM((2, rows, PAIR), BF16),
                pltpu.VMEM((2, rows, PAIR), BF16),
            ],
        ),
        compiler_params=params(),
        cost_estimate=cost(60 * rows * rows * width, 20 * rows * width),
        name="attend",
    )(flag, q, kv, kvp, do)


def qkv_back_kernel(last, x_ref, gain_ref, shift_ref, w_ref, ang_ref, dq_ref, dkv_ref, dkvn_ref, *rest):
    if last:
        (fg_in, og_ref, part_ref, dw_ref, db_ref, ig_ref, dgain_ref, dshift_ref,
         norm, norm_t, tab, fg) = rest
    else:
        dw_ref, db_ref, fg_ref, norm, norm_t, tab, fg = rest
    step = pl.program_id(0)

    @pl.when(step == 0)
    def _():
        norm_rows(x_ref, gain_ref, shift_ref, norm)
        norm_t[...] = norm[...].T
        build_tables(ang_ref, tab)
        if last:
            fg[...] = fg_in[...]
        else:
            fg[...] = jnp.zeros_like(fg)

    dq = turn(dq_ref[...].astype(F32), tab, -1.0)
    dk = turn(dkv_ref[0].astype(F32) + dkvn_ref[0].astype(F32), tab, -1.0)
    dv = dkv_ref[1].astype(F32) + dkvn_ref[1].astype(F32)
    low = low_lanes(dq.shape)
    dk = pltpu.roll(dk, HEAD_DIM, 1)
    dm = jnp.concatenate(
        [jnp.where(low, dq, dk), jnp.where(low, dv, dq), jnp.where(low, dk, dv)], axis=1
    ).astype(BF16)
    db_ref[...] = jnp.sum(dm.astype(F32), axis=0, keepdims=True)
    dw_ref[...] = dot(norm_t[...], dm).astype(BF16)
    fg[...] += dot_t(dm, w_ref[...])

    @pl.when(step == pl.num_programs(0) - 1)
    def _():
        if last:
            def emit(rows, part):
                total = og_ref[rows, :].astype(F32) + part + part_ref[rows, :]
                ig_ref[rows, :] = total.astype(BF16)

            norm_back(x_ref, gain_ref, fg, dgain_ref, dshift_ref, emit)
        else:
            fg_ref[...] = fg[...]


def qkv_back(x, gain, shift, w, ang, dq, dkv, dkvn, first, carry):
    rows, width = x.shape
    last = carry is not None
    pairs = dq.shape[1] // PAIR
    full, vec = whole((rows, width)), whole((1, width))
    cols = 3 * PAIR
    tok = pl.BlockSpec((rows, PAIR), lambda i: (0, i))
    kvs = pl.BlockSpec((2, rows, PAIR), lambda i: (0, 0, i))
    outs = [jax.ShapeDtypeStruct((width, pairs * cols), BF16), jax.ShapeDtypeStruct((1, pairs * cols), F32)]
    specs = [pl.BlockSpec((width, cols), lambda i: (0, i)), pl.BlockSpec((1, cols), lambda i: (0, i))]
    if last:
        outs += [jax.ShapeDtypeStruct((rows, width), BF16)] + [jax.ShapeDtypeStruct((1, width), F32)] * 2
        specs += [full, vec, vec]
    else:
        outs += [jax.ShapeDtypeStruct((rows, width), F32)]
        specs += [full]
    return pl.pallas_call(
        partial(qkv_back_kernel, last),
        grid=(pairs,),
        out_shape=tuple(outs),
        in_specs=[full, vec, vec, pl.BlockSpec((width, cols), lambda i: (0, first + i)),
                  whole(ang.shape), tok, kvs, kvs] + ([full] * 3 if last else []),
        out_specs=tuple(specs),
        scratch_shapes=[pltpu.VMEM((rows, width), BF16), pltpu.VMEM((width, rows), BF16),
                        pltpu.VMEM((3, rows, PAIR), F32), pltpu.VMEM((rows, width), F32)],
        compiler_params=params(),
        cost_estimate=cost(4 * rows * width * pairs * cols, 8 * rows * width),
        name="qkv_back",
    )(x, gain, shift, w, ang, dq, dkv, dkvn, *(carry or ()))


def dense_kernel(o0_ref, o1_ref, wd_ref, db_ref, rb_ref, mid_ref, x_ref, og_ref, out_ref, dwd_ref, ot):
    half = o0_ref.shape[1]

    @pl.when(pl.program_id(0) == 0)
    def _():
        ot[:half, :] = o0_ref[...].T
        ot[half:, :] = o1_ref[...].T

    total = x_ref[...].astype(F32) + mid_ref[...] + (db_ref[...] + rb_ref[...])
    total += dot(o0_ref[...], wd_ref[:half, :]) + dot(o1_ref[...], wd_ref[half:, :])
    out_ref[...] = total.astype(BF16)
    dwd_ref[...] = dot(ot[...], og_ref[...]).astype(BF16)


def dense(o0, o1, wd, db, rb, mid, x, og):
    rows, width = x.shape
    blk = 256
    col = lambda r: pl.BlockSpec((r, blk), lambda i: (0, i))
    return pl.pallas_call(
        dense_kernel,
        grid=(width // blk,),
        out_shape=(jax.ShapeDtypeStruct((rows, width), BF16), jax.ShapeDtypeStruct((width, width), BF16)),
        in_specs=[whole(o0.shape), whole(o1.shape), col(width), col(1), col(1), col(rows), col(rows), col(rows)],
        out_specs=(col(rows), col(width)),
        scratch_shapes=[pltpu.VMEM((width, rows), BF16)],
        compiler_params=params(),
        cost_estimate=cost(4 * rows * width * width, 12 * rows * width),
        name="dense",
    )(o0, o1, wd, db, rb, mid, x, og)


MESH = pl.DeviceIdType.MESH


def scatter_kernel(bits, parts, chunks, vec_sizes, *refs):
    nvec, nmat, nchunk = len(vec_sizes), 3, len(chunks)
    mats, vecs = refs[:nmat], refs[nmat:nmat + nvec]
    outs, vec_out = refs[nmat + nvec:2 * nmat + nvec], refs[2 * nmat + nvec]
    refs = refs[2 * nmat + nvec + 1:]
    recv = [refs[c * (bits + 1):(c + 1) * (bits + 1)] for c in range(nchunk)]
    state, vrecv, send_sem, recv_sem = refs[nchunk * (bits + 1):]
    me_b, me_s = lax.axis_index("batch"), lax.axis_index("seq")
    bit = [lax.rem(me_b // (1 << k), 2) for k in range(bits)]
    mate = [(me_b + (1 << k) - 2 * (1 << k) * bit[k], me_s) for k in range(bits)]
    others = [lax.rem(me_s + d, parts) for d in range(1, parts)]
    peers = mate + [(me_b, o) for o in others]
    npeer = len(peers)

    barrier = pltpu.get_barrier_semaphore()
    for peer in peers:
        pl.semaphore_signal(barrier, inc=1, device_id=peer, device_id_type=MESH)
    pl.semaphore_wait(barrier, npeer)

    copies = {}

    def send(key, slot, n, src, dst, peer):
        copy = pltpu.make_async_remote_copy(
            src_ref=src, dst_ref=dst, send_sem=send_sem.at[slot, n], recv_sem=recv_sem.at[slot, n],
            device_id=peer, device_id_type=MESH)
        copy.start()
        copies[key, n] = copy

    def open_bits(order, stage):
        return [d for d in range(bits - 1, -1, -1) if d not in order[:stage]]

    def start(c, stage):
        mat, col, size, order = chunks[c]
        if stage == bits:
            for n, o in enumerate(others):
                send(c, c, bits + n, recv[c][bits - 1].at[o], recv[c][bits].at[n], (me_b, o))
            return
        k = order[stage]
        index = tuple(1 - bit[k] if d == k else slice(None) for d in open_bits(order, stage))
        if stage == 0:
            src = mats[mat].at[index + (slice(None), slice(None), pl.ds(col, size))]
        else:
            src = recv[c][stage - 1].at[index]
        send(c, c, stage, src, recv[c][stage], mate[k])

    def add(c, stage):
        mat, col, size, order = chunks[c]
        k = order[stage]
        dims = open_bits(order, stage)
        copies[c, stage].wait_recv()
        dst = recv[c][stage]
        lead = bits - 1 - stage

        def one(i, carry):
            part = lax.rem(i, parts)
            rest = i // parts
            sub = tuple(lax.rem(rest // (1 << (lead - 1 - n)), 2) for n in range(lead))
            left = list(sub)
            own_at = tuple(bit[k] if d == k else left.pop(0) for d in dims) + (part,)
            if stage == 0:
                own = mats[mat][own_at + (slice(None), pl.ds(col, size))]
            else:
                own = recv[c][stage - 1][own_at]
            at = sub + (part,)
            dst[at] = (own.astype(F32) + dst[at].astype(F32)).astype(BF16)
            return carry

        lax.fori_loop(0, parts << lead, one, 0)

    def finish(c):
        mat, col, size, _ = chunks[c]
        total = recv[c][bits - 1][me_s].astype(F32)
        for n in range(parts - 1):
            copies[c, bits + n].wait_recv()
            total = total + recv[c][bits][n].astype(F32)
        outs[mat][:, col:col + size] = total

    def vec_start(stage):
        if stage < bits:
            send("v", nchunk, stage, state.at[stage], vrecv.at[stage], mate[stage])
        else:
            for n, o in enumerate(others):
                send("v", nchunk, bits + n, state.at[bits], vrecv.at[bits + n], (me_b, o))

    def vec_add(stage):
        if stage < bits:
            copies["v", stage].wait_recv()
            state[stage + 1] = state[stage] + vrecv[stage]
            vec_start(stage + 1)
        else:
            total = state[bits]
            for n in range(parts - 1):
                copies["v", bits + n].wait_recv()
                total = total + vrecv[bits + n]
            vec_out[...] = total

    for c in range(nchunk):
        start(c, 0)
    at = 0
    for ref, n in zip(vecs, vec_sizes):
        state[0, :, at:at + n] = ref[...]
        at += n
    vec_start(0)
    for t in range(nchunk + bits):
        for stage in range(bits, -1, -1):
            c = t - stage
            if 0 <= c < nchunk:
                if stage < bits:
                    add(c, stage)
                    start(c, stage + 1)
                else:
                    finish(c)
        if t <= bits:
            vec_add(t)
    for copy in copies.values():
        copy.wait_send()


def scatter(bits, parts, mats, vecs):
    shards = parts << bits
    rows = mats[0].shape[0] // shards
    widths = [m.shape[1] for m in mats]
    shaped = [m.reshape((2,) * bits + (parts, rows, m.shape[1])) for m in mats]
    plain = list(range(bits))
    other = [0] + [k for i in range(1, bits, 2) for k in reversed(range(i, min(i + 2, bits)))]
    chunks = []
    for m, w in enumerate(widths):
        chunks += [(m, 0, w // 2, plain), (m, w // 2, w // 2, other)]
    vec_sizes = [v.shape[1] for v in vecs]
    total = sum(vec_sizes)
    npeer = bits + parts - 1
    scratch = []
    for _, _, size, _ in chunks:
        for stage in range(bits):
            scratch.append(pltpu.VMEM((2,) * (bits - 1 - stage) + (parts, rows, size), BF16))
        scratch.append(pltpu.VMEM((parts - 1, rows, size), BF16))
    scratch += [
        pltpu.VMEM((bits + 1, 1, total), F32),
        pltpu.VMEM((npeer, 1, total), F32),
        pltpu.SemaphoreType.DMA((len(chunks) + 1, npeer)),
        pltpu.SemaphoreType.DMA((len(chunks) + 1, npeer)),
    ]
    vmem = pl.BlockSpec(memory_space=pltpu.VMEM)
    return pl.pallas_call(
        partial(scatter_kernel, bits, parts, chunks, vec_sizes),
        out_shape=tuple(jax.ShapeDtypeStruct((rows, w), F32) for w in widths)
        + (jax.ShapeDtypeStruct((1, total), F32),),
        in_specs=[vmem] * (len(mats) + len(vecs)),
        out_specs=tuple([vmem] * (len(mats) + 1)),
        scratch_shapes=scratch,
        compiler_params=pltpu.CompilerParams(
            vmem_limit_bytes=VMEM_LIMIT, collective_id=0, has_side_effects=True),
        name="scatter",
    )(*shaped, *vecs)


def body(
    tokens,
    seq_lengths,
    attn_gain,
    attn_shift,
    qkv_weight,
    qkv_bias,
    dense_weight,
    dense_bias,
    mlp_gain,
    mlp_shift,
    expand_weight,
    expand_bias,
    reduce_weight,
    reduce_bias,
    out_grad,
):
    seq_parts = lax.axis_size("seq")
    place = lax.axis_index("seq")
    rows, width = tokens.shape
    lengths = seq_lengths[0]
    starts = jnp.cumsum(lengths) - lengths
    row0 = place * rows
    offset = row0 - jnp.max(jnp.where(starts <= row0, starts, 0))
    flag = (offset > 0).astype(jnp.int32).reshape(1)
    positions = (offset + jnp.arange(rows, dtype=jnp.int32)).astype(F32)
    frequency = jnp.exp(jnp.arange(ROT // 2, dtype=F32) * (-2.0 * math.log(10000.0) / ROT))
    phases = frequency[:, None] * positions[None, :]
    ang = jnp.concatenate([jnp.cos(phases), jnp.sin(phases)], axis=0)

    row = lambda v: v.reshape(1, -1)
    ag, ash, mg, msh = row(attn_gain), row(attn_shift), row(mlp_gain), row(mlp_shift)
    onward = [(i, i + 1) for i in range(seq_parts - 1)]
    back = [(i + 1, i) for i in range(seq_parts - 1)]

    q, kv, do = project(tokens, ag, ash, qkv_weight, row(qkv_bias), ang, out_grad, dense_weight)
    kvp = lax.ppermute(kv, "seq", onward)
    batch_parts = lax.axis_size("batch")
    ndev = batch_parts * seq_parts
    tokens_b, q = lax.optimization_barrier((tokens, q))
    mid, part, grads, dbe, dog, dmg, dms = mlp(
        ndev, tokens_b, mg, msh, expand_weight, row(expand_bias), reduce_weight, out_grad)
    grads = lax.psum_scatter(grads, ("batch", "seq"), scatter_dimension=0, tiled=True)

    hp = width // PAIR // 2
    o0, dq0, dkv0, dkvp0 = attend(flag, q, kv, kvp, do, 0, hp)
    dkvn0 = lax.ppermute(dkvp0, "seq", back)
    o1, dq1, dkv1, dkvp1 = attend(flag, q, kv, kvp, do, hp, hp)
    dkvn1 = lax.ppermute(dkvp1, "seq", back)
    dw0, db0, fg = qkv_back(tokens, ag, ash, qkv_weight, ang, dq0, dkv0, dkvn0, 0, None)
    layer_out, dwd = dense(o0, o1, dense_weight, row(dense_bias), row(reduce_bias), mid, tokens, out_grad)
    dw1, db1, input_grad, dag, das = qkv_back(
        tokens, ag, ash, qkv_weight, ang, dq1, dkv1, dkvn1, hp, (fg, out_grad, part))
    bits = batch_parts.bit_length() - 1
    vecs = [dag, das, db0, db1, dog, dmg, dms, dbe]
    dw0, dw1, dwd, vsum = scatter(bits, seq_parts, [dw0, dw1, dwd], vecs)
    index = lax.axis_index("batch") * seq_parts + place
    pieces, at = [], 0
    for size in (width, width, 3 * width, width, width, width, dbe.shape[1]):
        own = size // ndev
        pieces.append(lax.dynamic_slice(vsum, (0, at + index * own), (1, own)).reshape(own))
        at += size
    dag, das, dqb, dog, dmg, dms, dbe = pieces
    half = GRAD_COLS // 2
    dwe = grads[:, :half].astype(F32)
    dwr = jnp.concatenate(
        [grads[:, half + j * width:half + (j + 1) * width] for j in range(half // width)], axis=0).astype(F32)
    return (
        layer_out,
        input_grad,
        dag,
        das,
        jnp.concatenate([dw0, dw1], axis=1),
        dqb,
        dwd,
        dog,
        dmg,
        dms,
        dwe,
        dbe,
        dwr,
        dog,
    )


def solution(mesh):
    tok = P(("batch", "seq"), None)
    vec = P(("batch", "seq"))
    in_specs = (tok, P("batch", None)) + (P(),) * 12 + (tok,)
    out_specs = (tok, tok, vec, vec, tok, vec, tok, vec, vec, vec, tok, vec, tok, vec)
    return jax.shard_map(body, mesh=mesh, in_specs=in_specs, out_specs=out_specs, check_vma=False)
```

```python
from functools import partial
import math

import jax
import jax.numpy as jnp
from jax import lax
from jax.experimental import pallas as pl
from jax.experimental.pallas import tpu as pltpu
from jax.sharding import PartitionSpec as P


HEAD_DIM = 64
ROT = 16
PAIR = 2 * HEAD_DIM
EPSILON = 1e-05
MASKED = -1e30
SCALE = 1.0 / math.sqrt(HEAD_DIM)
QB = 256
FB = 1024
STEP_PAIRS = 2
ROWS = 128
F32 = jnp.float32
BF16 = jnp.bfloat16
VMEM_LIMIT = 60 << 20


def dot(left, right):
    return jnp.dot(left, right, preferred_element_type=F32)


def dot_t(left, right):
    return lax.dot_general(left, right, (((1,), (1,)), ((), ())), preferred_element_type=F32)


def params():
    return pltpu.CompilerParams(vmem_limit_bytes=VMEM_LIMIT)


def cost(flops, nbytes):
    return pl.CostEstimate(flops=int(flops), bytes_accessed=int(nbytes), transcendentals=0)


def whole(shape):
    return pl.BlockSpec(shape, lambda i: (0,) * len(shape), pipeline_mode=pl.Buffered(1))


def statistics(x):
    mean = jnp.mean(x, axis=-1, keepdims=True)
    centered = x - mean
    variance = jnp.mean(centered * centered, axis=-1, keepdims=True)
    rstd = lax.rsqrt(variance + EPSILON)
    return centered * rstd, rstd


def norm_rows(x_ref, gain_ref, shift_ref, out_ref):
    def step(i, carry):
        rows = pl.ds(pl.multiple_of(i * ROWS, ROWS), ROWS)
        xn, _ = statistics(x_ref[rows, :].astype(F32))
        out_ref[rows, :] = (xn * gain_ref[...] + shift_ref[...]).astype(BF16)
        return carry

    lax.fori_loop(0, x_ref.shape[0] // ROWS, step, 0)


def norm_back(x_ref, gain_ref, grad_ref, gaingrad_ref, shiftgrad_ref, emit):
    gaingrad_ref[...] = jnp.zeros_like(gaingrad_ref)
    shiftgrad_ref[...] = jnp.zeros_like(shiftgrad_ref)

    def step(i, carry):
        rows = pl.ds(pl.multiple_of(i * ROWS, ROWS), ROWS)
        xn, rstd = statistics(x_ref[rows, :].astype(F32))
        grad = grad_ref[rows, :]
        gaingrad_ref[...] += jnp.sum(grad * xn, axis=0, keepdims=True)
        shiftgrad_ref[...] += jnp.sum(grad, axis=0, keepdims=True)
        scaled = grad * gain_ref[...]
        mean_s = jnp.mean(scaled, axis=-1, keepdims=True)
        mean_sx = jnp.mean(scaled * xn, axis=-1, keepdims=True)
        emit(rows, rstd * (scaled - mean_s - xn * mean_sx))
        return carry

    lax.fori_loop(0, x_ref.shape[0] // ROWS, step, 0)


def build_tables(angle_ref, tab_ref):
    half = ROT // 2
    cos8, sin8 = angle_ref[0:half, :], angle_ref[half:ROT, :]
    rest = HEAD_DIM - ROT
    count = cos8.shape[1]
    ones = jnp.ones((rest, count), F32)
    zeros = jnp.zeros((rest, count), F32)
    z8 = jnp.zeros_like(sin8)
    tab_ref[0] = jnp.concatenate([cos8, cos8, ones] * 2, axis=0).T
    tab_ref[1] = jnp.concatenate([-sin8, z8, zeros] * 2, axis=0).T
    tab_ref[2] = jnp.concatenate([z8, sin8, zeros] * 2, axis=0).T


def turn(u, tab_ref, sign):
    half = ROT // 2
    ahead = pltpu.roll(u, PAIR - half, 1)
    behind = pltpu.roll(u, half, 1)
    return u * tab_ref[0] + sign * (ahead * tab_ref[1] + behind * tab_ref[2])


def low_lanes(shape):
    return lax.broadcasted_iota(jnp.int32, shape, 1) < HEAD_DIM


def project_kernel(x_ref, gain_ref, shift_ref, w_ref, b_ref, ang_ref, og_ref, wd_ref,
                   q_ref, kv_ref, do_ref, norm, tab):
    @pl.when(pl.program_id(0) == 0)
    def _():
        norm_rows(x_ref, gain_ref, shift_ref, norm)
        build_tables(ang_ref, tab)

    for n in range(STEP_PAIRS):
        cols = slice(n * 3 * PAIR, (n + 1) * 3 * PAIR)
        mine = slice(n * PAIR, (n + 1) * PAIR)
        mixed = dot(norm[...], w_ref[:, cols]) + b_ref[:, cols]
        t0, t1, t2 = mixed[:, :PAIR], mixed[:, PAIR:2 * PAIR], mixed[:, 2 * PAIR:]
        low = low_lanes(t0.shape)
        q = jnp.where(low, t0, t1)
        k = pltpu.roll(jnp.where(low, t2, t0), HEAD_DIM, 1)
        v = jnp.where(low, t1, t2)
        q_ref[:, mine] = turn(q, tab, 1.0).astype(BF16)
        kv_ref[0, :, mine] = turn(k, tab, 1.0).astype(BF16)
        kv_ref[1, :, mine] = v.astype(BF16)
    do_ref[...] = dot_t(og_ref[...], wd_ref[...]).astype(BF16)


def project(x, gain, shift, w, b, ang, og, wd):
    rows, width = x.shape
    wide = STEP_PAIRS * PAIR
    tok = pl.BlockSpec((rows, wide), lambda i: (0, i))
    return pl.pallas_call(
        project_kernel,
        grid=(width // wide,),
        out_shape=(
            jax.ShapeDtypeStruct((rows, width), BF16),
            jax.ShapeDtypeStruct((2, rows, width), BF16),
            jax.ShapeDtypeStruct((rows, width), BF16),
        ),
        in_specs=[
            whole((rows, width)), whole((1, width)), whole((1, width)),
            pl.BlockSpec((width, 3 * wide), lambda i: (0, i)),
            pl.BlockSpec((1, 3 * wide), lambda i: (0, i)),
            whole(ang.shape), whole((rows, width)),
            pl.BlockSpec((wide, width), lambda i: (i, 0)),
        ],
        out_specs=(tok, pl.BlockSpec((2, rows, wide), lambda i: (0, 0, i)), tok),
        scratch_shapes=[pltpu.VMEM((rows, width), BF16), pltpu.VMEM((3, rows, PAIR), F32)],
        compiler_params=params(),
        cost_estimate=cost(8 * rows * width * width, 24 * rows * width),
        name="project",
    )(x, gain, shift, w, b, ang, og, wd)


def gelu_parts(h):
    z = jnp.abs(h) * math.sqrt(0.5)
    t = 1.0 / (1.0 + 0.5 * z)
    poly = jnp.full_like(t, 0.17087277)
    for c in (-0.82215223, 1.48851587, -1.13520398, 0.27886807, -0.18628806, 0.09678418,
              0.37409196, 1.00002368, -1.26551223):
        poly = poly * t + c
    zz = z * z
    tail = 0.5 * t * jnp.exp(poly - zz)
    cdf = jnp.where(h >= 0, 1.0 - tail, tail)
    slope = cdf + h * (jnp.exp(-zz) * (1.0 / math.sqrt(2.0 * math.pi)))
    return h * cdf, slope


def mlp_fwd_kernel(take, x_ref, gain_ref, shift_ref, we_ref, be_ref, wr_ref, og_ref,
                   mid_ref, slope_ref, dwr_ref, dog_ref, norm):
    step = pl.program_id(0)
    width = x_ref.shape[1]

    @pl.when(step == 0)
    def _():
        norm_rows(x_ref, gain_ref, shift_ref, norm)
        mid_ref[...] = jnp.zeros_like(mid_ref)
        dog_ref[...] = jnp.sum(og_ref[...].astype(F32), axis=0, keepdims=True)

    h = dot(norm[...], we_ref[...]) + be_ref[...]
    active, slope = gelu_parts(h)
    active = active.astype(BF16)
    slope_ref[...] = slope.astype(BF16)
    mid_ref[...] += dot(active, wr_ref[...])
    dwr = dot(active.T, og_ref[...]).astype(BF16)
    full = dwr_ref.shape[1] - GRAD_PAD
    ratio = full // width
    for piece in range(FB // take):
        group, j = piece // ratio, piece % ratio
        dwr_ref[group * take:(group + 1) * take, j * width:(j + 1) * width] = (
            dwr[piece * take:(piece + 1) * take, :])
    dwr_ref[:, full:] = jnp.zeros((dwr_ref.shape[0], GRAD_PAD), BF16)


def mlp_back_kernel(x_ref, gain_ref, shift_ref, we_ref, wr_ref, og_ref, slope_ref,
                    part_ref, dwe_ref, dbe_ref, dgain_ref, dshift_ref, norm, norm_t, sg):
    step = pl.program_id(0)

    @pl.when(step == 0)
    def _():
        norm_rows(x_ref, gain_ref, shift_ref, norm)
        norm_t[...] = norm[...].T
        sg[...] = jnp.zeros_like(sg)

    hidden = (dot_t(og_ref[...], wr_ref[...]) * slope_ref[...].astype(F32)).astype(BF16)
    dwe_ref[...] = dot(norm_t[...], hidden).astype(BF16)
    dbe_ref[...] = jnp.sum(hidden.astype(F32), axis=0, keepdims=True)
    sg[...] += dot_t(hidden, we_ref[...])

    @pl.when(step == pl.num_programs(0) - 1)
    def _():
        def emit(rows, part):
            part_ref[rows, :] = part

        norm_back(x_ref, gain_ref, sg, dgain_ref, dshift_ref, emit)


GRAD_PAD = 128


def mlp_specs(x):
    rows, width = x.shape
    full = whole((rows, width))
    vec = whole((1, width))
    up = pl.BlockSpec((width, FB), lambda i: (0, i))
    down = pl.BlockSpec((FB, width), lambda i: (i, 0))
    bias = pl.BlockSpec((1, FB), lambda i: (0, i))
    act = pl.BlockSpec((rows, FB), lambda i: (0, i))
    return full, vec, up, down, bias, act


def mlp_fwd(ndev, x, gain, shift, we, be, wr, og):
    rows, width = x.shape
    hidden = we.shape[1]
    full, vec, up, down, bias, act = mlp_specs(x)
    out_rows = hidden // (hidden // width)
    blk = FB * out_rows // hidden
    gshape = (out_rows, hidden + GRAD_PAD)
    return pl.pallas_call(
        partial(mlp_fwd_kernel, out_rows // ndev),
        grid=(hidden // FB,),
        out_shape=(jax.ShapeDtypeStruct((rows, width), F32), jax.ShapeDtypeStruct((rows, hidden), BF16),
                   jax.ShapeDtypeStruct(gshape, BF16), jax.ShapeDtypeStruct((1, width), F32)),
        in_specs=[full, vec, vec, up, bias, down, full],
        out_specs=(full, act, pl.BlockSpec((blk, gshape[1]), lambda i: (i, 0)), vec),
        scratch_shapes=[pltpu.VMEM((rows, width), BF16)],
        compiler_params=params(),
        cost_estimate=cost(6 * rows * width * hidden, 8 * width * hidden),
        name="mlp_fwd",
    )(x, gain, shift, we, be, wr, og)


def mlp_back(x, gain, shift, we, wr, og, slope):
    rows, width = x.shape
    hidden = we.shape[1]
    full, vec, up, down, bias, act = mlp_specs(x)
    vshape = jax.ShapeDtypeStruct((1, width), F32)
    return pl.pallas_call(
        mlp_back_kernel,
        grid=(hidden // FB,),
        out_shape=(jax.ShapeDtypeStruct((rows, width), F32),
                   jax.ShapeDtypeStruct((width, hidden + GRAD_PAD), BF16),
                   jax.ShapeDtypeStruct((1, hidden), F32), vshape, vshape),
        in_specs=[full, vec, vec, up, down, full, act],
        out_specs=(full, up, bias, vec, vec),
        scratch_shapes=[pltpu.VMEM((rows, width), BF16), pltpu.VMEM((width, rows), BF16),
                        pltpu.VMEM((rows, width), F32)],
        compiler_params=params(),
        cost_estimate=cost(6 * rows * width * hidden, 8 * width * hidden),
        name="mlp_back",
    )(x, gain, shift, we, wr, og, slope)


def attend_kernel(flag_ref, q_ref, kv_ref, kvp_ref, do_ref, o_ref, dq_ref, dkv_ref, dkvp_ref,
                  pt, ds, kvt, qm, dom):
    rows_all = q_ref.shape[0]
    nq = rows_all // QB

    def run(prev):
        base = 0 if prev else nq
        sources = [(kvp_ref, i) for i in range(nq)] + [(kv_ref, i) for i in range(nq)]

        def block(which, b):
            ref, i = sources[b]
            return ref[which, i * QB:(i + 1) * QB, :]

        for which in range(2):
            if prev:
                kvt[which, :, :rows_all] = kvp_ref[which].T
            kvt[which, :, rows_all:] = kv_ref[which].T
        lane = lax.broadcasted_iota(jnp.int32, (QB, PAIR), 1)
        sub = lax.broadcasted_iota(jnp.int32, (PAIR, QB), 0)
        causal = lax.broadcasted_iota(jnp.int32, (QB, QB), 0) <= lax.broadcasted_iota(
            jnp.int32, (QB, QB), 1)
        for j in range(nq):
            rows = slice(j * QB, (j + 1) * QB)
            q = q_ref[rows, :] * jnp.asarray(SCALE, BF16)
            qt = q.T
            dot_rows = do_ref[rows, :].astype(F32).T
            blocks = range(base, nq + j + 1)
            k0, k1 = base * QB, (nq + j + 1) * QB
            outs, scaled, dqs = [], [], []
            for h in range(2):
                hs = slice(h * HEAD_DIM, (h + 1) * HEAD_DIM)
                qm[h, rows, :] = jnp.where((lane < HEAD_DIM) == (h == 0), q, jnp.zeros_like(q))
                qtm = jnp.where((sub < HEAD_DIM) == (h == 0), qt, jnp.zeros_like(qt))
                scores, top = [], None
                for b in blocks:
                    s = dot(block(0, b), qtm)
                    if b == nq + j:
                        s = jnp.where(causal, s, MASKED)
                    scores.append(s)
                    part = jnp.max(s.reshape(QB // 8, 8, QB), axis=0)
                    top = part if top is None else jnp.maximum(top, part)
                top = jnp.max(top, axis=0, keepdims=True)
                total = None
                for b, s in zip(blocks, scores):
                    p = jnp.exp(s - top)
                    part = jnp.sum(p.reshape(QB // 8, 8, QB), axis=0)
                    total = part if total is None else total + part
                    pt[h, b * QB:(b + 1) * QB, rows] = p.astype(BF16)
                inv = 1.0 / jnp.sum(total, axis=0, keepdims=True)
                out_t = dot(kvt[1, hs, k0:k1], pt[h, k0:k1, rows]) * inv
                dol_t = dot_rows[hs] * inv
                delta = jnp.sum(dol_t * out_t, axis=0, keepdims=True)
                outs.append(out_t)
                scaled.append(dol_t)
                zero = jnp.zeros((HEAD_DIM, QB), BF16)
                dol_b = dol_t.astype(BF16)
                dol_m = jnp.concatenate([dol_b, zero] if h == 0 else [zero, dol_b], axis=0)
                for b in blocks:
                    dp = dot(block(1, b), dol_m)
                    d = pt[h, b * QB:(b + 1) * QB, rows].astype(F32) * (dp - delta)
                    ds[h, b * QB:(b + 1) * QB, rows] = d.astype(BF16)
                dqs.append(dot(kvt[0, hs, k0:k1], ds[h, k0:k1, rows]) * SCALE)
            o_ref[rows, :] = jnp.concatenate(outs, 0).T.astype(BF16)
            dq_ref[rows, :] = jnp.concatenate(dqs, 0).T.astype(BF16)
            dol = jnp.concatenate(scaled, 0).T.astype(BF16)
            for h in range(2):
                dom[h, rows, :] = jnp.where((lane < HEAD_DIM) == (h == 0), dol, jnp.zeros_like(dol))
        for b in range(base, 2 * nq):
            q0 = max(0, b - nq) * QB
            br = slice(b * QB, (b + 1) * QB)
            dk = dot(ds[0, br, q0:], qm[0, q0:, :]) + dot(ds[1, br, q0:], qm[1, q0:, :])
            dv = dot(pt[0, br, q0:], dom[0, q0:, :]) + dot(pt[1, br, q0:], dom[1, q0:, :])
            ref, i = (dkvp_ref, b) if b < nq else (dkv_ref, b - nq)
            ref[0, i * QB:(i + 1) * QB, :] = dk.astype(BF16)
            ref[1, i * QB:(i + 1) * QB, :] = dv.astype(BF16)

    @pl.when(flag_ref[0] == 1)
    def _():
        run(True)

    @pl.when(flag_ref[0] == 0)
    def _():
        run(False)
        dkvp_ref[...] = jnp.zeros_like(dkvp_ref)


def attend(flag, q, kv, kvp, do, first, pairs):
    rows = q.shape[0]
    width = pairs * PAIR
    tok_in = pl.BlockSpec((rows, PAIR), lambda i, f: (0, first + i))
    kv_in = pl.BlockSpec((2, rows, PAIR), lambda i, f: (0, 0, first + i))
    tok_out = pl.BlockSpec((rows, PAIR), lambda i, f: (0, i))
    kv_out = pl.BlockSpec((2, rows, PAIR), lambda i, f: (0, 0, i))
    tok_shape = jax.ShapeDtypeStruct((rows, width), BF16)
    kv_shape = jax.ShapeDtypeStruct((2, rows, width), BF16)
    return pl.pallas_call(
        attend_kernel,
        out_shape=(tok_shape, tok_shape, kv_shape, kv_shape),
        grid_spec=pltpu.PrefetchScalarGridSpec(
            num_scalar_prefetch=1,
            grid=(pairs,),
            in_specs=[tok_in, kv_in, kv_in, tok_in],
            out_specs=(tok_out, tok_out, kv_out, kv_out),
            scratch_shapes=[
                pltpu.VMEM((2, 2 * rows, rows), BF16),
                pltpu.VMEM((2, 2 * rows, rows), BF16),
                pltpu.VMEM((2, PAIR, 2 * rows), BF16),
                pltpu.VMEM((2, rows, PAIR), BF16),
                pltpu.VMEM((2, rows, PAIR), BF16),
            ],
        ),
        compiler_params=params(),
        cost_estimate=cost(60 * rows * rows * width, 20 * rows * width),
        name="attend",
    )(flag, q, kv, kvp, do)


def qkv_back_kernel(last, x_ref, gain_ref, shift_ref, w_ref, ang_ref, dq_ref, dkv_ref, dkvn_ref, *rest):
    if last:
        (fg_in, og_ref, part_ref, dw_ref, db_ref, ig_ref, dgain_ref, dshift_ref,
         norm, norm_t, tab, fg) = rest
    else:
        dw_ref, db_ref, fg_ref, norm, norm_t, tab, fg = rest
    step = pl.program_id(0)

    @pl.when(step == 0)
    def _():
        norm_rows(x_ref, gain_ref, shift_ref, norm)
        norm_t[...] = norm[...].T
        build_tables(ang_ref, tab)
        if last:
            fg[...] = fg_in[...]
        else:
            fg[...] = jnp.zeros_like(fg)

    blocks = []
    for n in range(STEP_PAIRS):
        mine = slice(n * PAIR, (n + 1) * PAIR)
        dq = turn(dq_ref[:, mine].astype(F32), tab, -1.0)
        dk = turn(dkv_ref[0, :, mine].astype(F32) + dkvn_ref[0, :, mine].astype(F32), tab, -1.0)
        dv = dkv_ref[1, :, mine].astype(F32) + dkvn_ref[1, :, mine].astype(F32)
        low = low_lanes(dq.shape)
        dk = pltpu.roll(dk, HEAD_DIM, 1)
        blocks += [jnp.where(low, dq, dk), jnp.where(low, dv, dq), jnp.where(low, dk, dv)]
    dm = jnp.concatenate(blocks, axis=1).astype(BF16)
    db_ref[...] = jnp.sum(dm.astype(F32), axis=0, keepdims=True)
    dw_ref[...] = dot(norm_t[...], dm).astype(BF16)
    fg[...] += dot_t(dm, w_ref[...])

    @pl.when(step == pl.num_programs(0) - 1)
    def _():
        if last:
            def emit(rows, part):
                total = og_ref[rows, :].astype(F32) + part + part_ref[rows, :]
                ig_ref[rows, :] = total.astype(BF16)

            norm_back(x_ref, gain_ref, fg, dgain_ref, dshift_ref, emit)
        else:
            fg_ref[...] = fg[...]


def qkv_back(x, gain, shift, w, ang, dq, dkv, dkvn, first, carry):
    rows, width = x.shape
    last = carry is not None
    pairs = dq.shape[1] // PAIR
    full, vec = whole((rows, width)), whole((1, width))
    wide = STEP_PAIRS * PAIR
    steps = pairs // STEP_PAIRS
    cols = 3 * wide
    tok = pl.BlockSpec((rows, wide), lambda i: (0, i))
    kvs = pl.BlockSpec((2, rows, wide), lambda i: (0, 0, i))
    outs = [jax.ShapeDtypeStruct((width, steps * cols), BF16), jax.ShapeDtypeStruct((1, steps * cols), F32)]
    specs = [pl.BlockSpec((width, cols), lambda i: (0, i)), pl.BlockSpec((1, cols), lambda i: (0, i))]
    if last:
        outs += [jax.ShapeDtypeStruct((rows, width), BF16)] + [jax.ShapeDtypeStruct((1, width), F32)] * 2
        specs += [full, vec, vec]
    else:
        outs += [jax.ShapeDtypeStruct((rows, width), F32)]
        specs += [full]
    return pl.pallas_call(
        partial(qkv_back_kernel, last),
        grid=(steps,),
        out_shape=tuple(outs),
        in_specs=[full, vec, vec, pl.BlockSpec((width, cols), lambda i: (0, first // STEP_PAIRS + i)),
                  whole(ang.shape), tok, kvs, kvs] + ([full] * 3 if last else []),
        out_specs=tuple(specs),
        scratch_shapes=[pltpu.VMEM((rows, width), BF16), pltpu.VMEM((width, rows), BF16),
                        pltpu.VMEM((3, rows, PAIR), F32), pltpu.VMEM((rows, width), F32)],
        compiler_params=params(),
        cost_estimate=cost(4 * rows * width * steps * cols, 8 * rows * width),
        name="qkv_back",
    )(x, gain, shift, w, ang, dq, dkv, dkvn, *(carry or ()))


def dense_kernel(o0_ref, o1_ref, wd_ref, db_ref, rb_ref, mid_ref, x_ref, og_ref, out_ref, dwd_ref, ot):
    half = o0_ref.shape[1]

    @pl.when(pl.program_id(0) == 0)
    def _():
        ot[:half, :] = o0_ref[...].T
        ot[half:, :] = o1_ref[...].T

    total = x_ref[...].astype(F32) + mid_ref[...] + (db_ref[...] + rb_ref[...])
    total += dot(o0_ref[...], wd_ref[:half, :]) + dot(o1_ref[...], wd_ref[half:, :])
    out_ref[...] = total.astype(BF16)
    dwd_ref[...] = dot(ot[...], og_ref[...]).astype(BF16)


def dense(o0, o1, wd, db, rb, mid, x, og):
    rows, width = x.shape
    blk = 256
    col = lambda r: pl.BlockSpec((r, blk), lambda i: (0, i))
    return pl.pallas_call(
        dense_kernel,
        grid=(width // blk,),
        out_shape=(jax.ShapeDtypeStruct((rows, width), BF16), jax.ShapeDtypeStruct((width, width), BF16)),
        in_specs=[whole(o0.shape), whole(o1.shape), col(width), col(1), col(1), col(rows), col(rows), col(rows)],
        out_specs=(col(rows), col(width)),
        scratch_shapes=[pltpu.VMEM((width, rows), BF16)],
        compiler_params=params(),
        cost_estimate=cost(4 * rows * width * width, 12 * rows * width),
        name="dense",
    )(o0, o1, wd, db, rb, mid, x, og)


MESH = pl.DeviceIdType.MESH


def scatter_kernel(bits, parts, chunks, vec_sizes, *refs):
    nvec, nmat, nchunk = len(vec_sizes), 3, len(chunks)
    mats, vecs = refs[:nmat], refs[nmat:nmat + nvec]
    outs, vec_out = refs[nmat + nvec:2 * nmat + nvec], refs[2 * nmat + nvec]
    refs = refs[2 * nmat + nvec + 1:]
    recv = [refs[c * (bits + 1):(c + 1) * (bits + 1)] for c in range(nchunk)]
    state, vrecv, send_sem, recv_sem = refs[nchunk * (bits + 1):]
    me_b, me_s = lax.axis_index("batch"), lax.axis_index("seq")
    bit = [lax.rem(me_b // (1 << k), 2) for k in range(bits)]
    mate = [(me_b + (1 << k) - 2 * (1 << k) * bit[k], me_s) for k in range(bits)]
    others = [lax.rem(me_s + d, parts) for d in range(1, parts)]
    peers = mate + [(me_b, o) for o in others]
    npeer = len(peers)

    barrier = pltpu.get_barrier_semaphore()
    for peer in peers:
        pl.semaphore_signal(barrier, inc=1, device_id=peer, device_id_type=MESH)
    pl.semaphore_wait(barrier, npeer)

    copies = {}

    def send(key, slot, n, src, dst, peer):
        copy = pltpu.make_async_remote_copy(
            src_ref=src, dst_ref=dst, send_sem=send_sem.at[slot, n], recv_sem=recv_sem.at[slot, n],
            device_id=peer, device_id_type=MESH)
        copy.start()
        copies[key, n] = copy

    def open_bits(order, stage):
        return [d for d in range(bits - 1, -1, -1) if d not in order[:stage]]

    def start(c, stage):
        mat, col, size, order = chunks[c]
        if stage == bits:
            for n, o in enumerate(others):
                send(c, c, bits + n, recv[c][bits - 1].at[o], recv[c][bits].at[n], (me_b, o))
            return
        k = order[stage]
        index = tuple(1 - bit[k] if d == k else slice(None) for d in open_bits(order, stage))
        if stage == 0:
            src = mats[mat].at[index + (slice(None), slice(None), pl.ds(col, size))]
        else:
            src = recv[c][stage - 1].at[index]
        send(c, c, stage, src, recv[c][stage], mate[k])

    def add(c, stage):
        mat, col, size, order = chunks[c]
        k = order[stage]
        dims = open_bits(order, stage)
        copies[c, stage].wait_recv()
        dst = recv[c][stage]
        lead = bits - 1 - stage

        def one(i, carry):
            part = lax.rem(i, parts)
            rest = i // parts
            sub = tuple(lax.rem(rest // (1 << (lead - 1 - n)), 2) for n in range(lead))
            left = list(sub)
            own_at = tuple(bit[k] if d == k else left.pop(0) for d in dims) + (part,)
            if stage == 0:
                own = mats[mat][own_at + (slice(None), pl.ds(col, size))]
            else:
                own = recv[c][stage - 1][own_at]
            at = sub + (part,)
            dst[at] = (own.astype(F32) + dst[at].astype(F32)).astype(BF16)
            return carry

        lax.fori_loop(0, parts << lead, one, 0)

    def finish(c):
        mat, col, size, _ = chunks[c]
        total = recv[c][bits - 1][me_s].astype(F32)
        for n in range(parts - 1):
            copies[c, bits + n].wait_recv()
            total = total + recv[c][bits][n].astype(F32)
        outs[mat][:, col:col + size] = total

    def vec_start(stage):
        if stage < bits:
            send("v", nchunk, stage, state.at[stage], vrecv.at[stage], mate[stage])
        else:
            for n, o in enumerate(others):
                send("v", nchunk, bits + n, state.at[bits], vrecv.at[bits + n], (me_b, o))

    def vec_add(stage):
        if stage < bits:
            copies["v", stage].wait_recv()
            state[stage + 1] = state[stage] + vrecv[stage]
            vec_start(stage + 1)
        else:
            total = state[bits]
            for n in range(parts - 1):
                copies["v", bits + n].wait_recv()
                total = total + vrecv[bits + n]
            vec_out[...] = total

    for c in range(nchunk):
        start(c, 0)
    at = 0
    for ref, n in zip(vecs, vec_sizes):
        state[0, :, at:at + n] = ref[...]
        at += n
    vec_start(0)
    for stage in range(bits + 1):
        for c in range(nchunk):
            if stage < bits:
                add(c, stage)
                start(c, stage + 1)
            else:
                finish(c)
        vec_add(stage)
    for copy in copies.values():
        copy.wait_send()


def scatter(bits, parts, mats, vecs):
    shards = parts << bits
    rows = mats[0].shape[0] // shards
    widths = [m.shape[1] for m in mats]
    shaped = [m.reshape((2,) * bits + (parts, rows, m.shape[1])) for m in mats]
    plain = list(range(bits))
    other = [0] + [k for i in range(1, bits, 2) for k in reversed(range(i, min(i + 2, bits)))]
    chunks = []
    for m, w in enumerate(widths):
        chunks += [(m, 0, w // 2, plain), (m, w // 2, w // 2, other)]
    vec_sizes = [v.shape[1] for v in vecs]
    total = sum(vec_sizes)
    npeer = bits + parts - 1
    scratch = []
    for _, _, size, _ in chunks:
        for stage in range(bits):
            scratch.append(pltpu.VMEM((2,) * (bits - 1 - stage) + (parts, rows, size), BF16))
        scratch.append(pltpu.VMEM((parts - 1, rows, size), BF16))
    scratch += [
        pltpu.VMEM((bits + 1, 1, total), F32),
        pltpu.VMEM((npeer, 1, total), F32),
        pltpu.SemaphoreType.DMA((len(chunks) + 1, npeer)),
        pltpu.SemaphoreType.DMA((len(chunks) + 1, npeer)),
    ]
    vmem = pl.BlockSpec(memory_space=pltpu.VMEM)
    return pl.pallas_call(
        partial(scatter_kernel, bits, parts, chunks, vec_sizes),
        out_shape=tuple(jax.ShapeDtypeStruct((rows, w), F32) for w in widths)
        + (jax.ShapeDtypeStruct((1, total), F32),),
        in_specs=[vmem] * (len(mats) + len(vecs)),
        out_specs=tuple([vmem] * (len(mats) + 1)),
        scratch_shapes=scratch,
        compiler_params=pltpu.CompilerParams(
            vmem_limit_bytes=VMEM_LIMIT, collective_id=0, has_side_effects=True),
        name="scatter",
    )(*shaped, *vecs)


def body(
    tokens,
    seq_lengths,
    attn_gain,
    attn_shift,
    qkv_weight,
    qkv_bias,
    dense_weight,
    dense_bias,
    mlp_gain,
    mlp_shift,
    expand_weight,
    expand_bias,
    reduce_weight,
    reduce_bias,
    out_grad,
):
    seq_parts = lax.axis_size("seq")
    place = lax.axis_index("seq")
    rows, width = tokens.shape
    lengths = seq_lengths[0]
    starts = jnp.cumsum(lengths) - lengths
    row0 = place * rows
    offset = row0 - jnp.max(jnp.where(starts <= row0, starts, 0))
    flag = (offset > 0).astype(jnp.int32).reshape(1)
    positions = (offset + jnp.arange(rows, dtype=jnp.int32)).astype(F32)
    frequency = jnp.exp(jnp.arange(ROT // 2, dtype=F32) * (-2.0 * math.log(10000.0) / ROT))
    phases = frequency[:, None] * positions[None, :]
    ang = jnp.concatenate([jnp.cos(phases), jnp.sin(phases)], axis=0)

    row = lambda v: v.reshape(1, -1)
    ag, ash, mg, msh = row(attn_gain), row(attn_shift), row(mlp_gain), row(mlp_shift)
    onward = [(i, i + 1) for i in range(seq_parts - 1)]
    back = [(i + 1, i) for i in range(seq_parts - 1)]

    batch_parts = lax.axis_size("batch")
    ndev = batch_parts * seq_parts
    both = ("batch", "seq")
    q, kv, do = project(tokens, ag, ash, qkv_weight, row(qkv_bias), ang, out_grad, dense_weight)
    kvp = lax.ppermute(kv, "seq", onward)
    mid, slope, dwr, dog = mlp_fwd(
        ndev, tokens, mg, msh, expand_weight, row(expand_bias), reduce_weight, out_grad)
    dwr = lax.psum_scatter(dwr, both, scatter_dimension=0, tiled=True)
    part, dwe, dbe, dmg, dms = mlp_back(
        tokens, mg, msh, expand_weight, reduce_weight, out_grad, slope)
    dwe = lax.psum_scatter(dwe, both, scatter_dimension=0, tiled=True)

    hp = width // PAIR // 2
    o0, dq0, dkv0, dkvp0 = attend(flag, q, kv, kvp, do, 0, hp)
    dkvn0 = lax.ppermute(dkvp0, "seq", back)
    o1, dq1, dkv1, dkvp1 = attend(flag, q, kv, kvp, do, hp, hp)
    dkvn1 = lax.ppermute(dkvp1, "seq", back)
    dw0, db0, fg = qkv_back(tokens, ag, ash, qkv_weight, ang, dq0, dkv0, dkvn0, 0, None)
    layer_out, dwd = dense(o0, o1, dense_weight, row(dense_bias), row(reduce_bias), mid, tokens, out_grad)
    dw1, db1, input_grad, dag, das = qkv_back(
        tokens, ag, ash, qkv_weight, ang, dq1, dkv1, dkvn1, hp, (fg, out_grad, part))
    bits = batch_parts.bit_length() - 1
    vecs = [dag, das, db0, db1, dog, dmg, dms, dbe]
    dw0, dw1, dwd, vsum = scatter(bits, seq_parts, [dw0, dw1, dwd], vecs)
    index = lax.axis_index("batch") * seq_parts + place
    pieces, at = [], 0
    for size in (width, width, 3 * width, width, width, width, dbe.shape[1]):
        own = size // ndev
        pieces.append(lax.dynamic_slice(vsum, (0, at + index * own), (1, own)).reshape(own))
        at += size
    dag, das, dqb, dog, dmg, dms, dbe = pieces
    hidden = expand_weight.shape[1]
    dwe = dwe[:, :hidden].astype(F32)
    dwr = jnp.concatenate([dwr[:, j * width:(j + 1) * width] for j in range(hidden // width)], axis=0).astype(F32)
    return (
        layer_out,
        input_grad,
        dag,
        das,
        jnp.concatenate([dw0, dw1], axis=1),
        dqb,
        dwd,
        dog,
        dmg,
        dms,
        dwe,
        dbe,
        dwr,
        dog,
    )


def solution(mesh):
    tok = P(("batch", "seq"), None)
    vec = P(("batch", "seq"))
    in_specs = (tok, P("batch", None)) + (P(),) * 12 + (tok,)
    out_specs = (tok, tok, vec, vec, tok, vec, tok, vec, vec, vec, tok, vec, tok, vec)
    return jax.shard_map(body, mesh=mesh, in_specs=in_specs, out_specs=out_specs, check_vma=False)
```

```python
from functools import partial
import math

import jax
import jax.numpy as jnp
from jax import lax
from jax.experimental import pallas as pl
from jax.experimental.pallas import tpu as pltpu
from jax.sharding import PartitionSpec as P


HEAD_DIM = 64
ROT = 16
PAIR = 2 * HEAD_DIM
EPSILON = 1e-05
MASKED = -1e30
SCALE = 1.0 / math.sqrt(HEAD_DIM)
QB = 256
FB = 1024
STEP_PAIRS = 2
ROWS = 128
F32 = jnp.float32
BF16 = jnp.bfloat16
VMEM_LIMIT = 60 << 20


def dot(left, right):
    return jnp.dot(left, right, preferred_element_type=F32)


def dot_t(left, right):
    return lax.dot_general(left, right, (((1,), (1,)), ((), ())), preferred_element_type=F32)


def params():
    return pltpu.CompilerParams(vmem_limit_bytes=VMEM_LIMIT)


def cost(flops, nbytes):
    return pl.CostEstimate(flops=int(flops), bytes_accessed=int(nbytes), transcendentals=0)


def whole(shape):
    return pl.BlockSpec(shape, lambda i: (0,) * len(shape), pipeline_mode=pl.Buffered(1))


def statistics(x):
    mean = jnp.mean(x, axis=-1, keepdims=True)
    centered = x - mean
    variance = jnp.mean(centered * centered, axis=-1, keepdims=True)
    rstd = lax.rsqrt(variance + EPSILON)
    return centered * rstd, rstd


def norm_rows(x_ref, gain_ref, shift_ref, out_ref):
    def step(i, carry):
        rows = pl.ds(pl.multiple_of(i * ROWS, ROWS), ROWS)
        xn, _ = statistics(x_ref[rows, :].astype(F32))
        out_ref[rows, :] = (xn * gain_ref[...] + shift_ref[...]).astype(BF16)
        return carry

    lax.fori_loop(0, x_ref.shape[0] // ROWS, step, 0)


def norm_back(x_ref, gain_ref, grad_ref, gaingrad_ref, shiftgrad_ref, emit):
    gaingrad_ref[...] = jnp.zeros_like(gaingrad_ref)
    shiftgrad_ref[...] = jnp.zeros_like(shiftgrad_ref)

    def step(i, carry):
        rows = pl.ds(pl.multiple_of(i * ROWS, ROWS), ROWS)
        xn, rstd = statistics(x_ref[rows, :].astype(F32))
        grad = grad_ref[rows, :]
        gaingrad_ref[...] += jnp.sum(grad * xn, axis=0, keepdims=True)
        shiftgrad_ref[...] += jnp.sum(grad, axis=0, keepdims=True)
        scaled = grad * gain_ref[...]
        mean_s = jnp.mean(scaled, axis=-1, keepdims=True)
        mean_sx = jnp.mean(scaled * xn, axis=-1, keepdims=True)
        emit(rows, rstd * (scaled - mean_s - xn * mean_sx))
        return carry

    lax.fori_loop(0, x_ref.shape[0] // ROWS, step, 0)


def build_tables(angle_ref, tab_ref):
    half = ROT // 2
    cos8, sin8 = angle_ref[0:half, :], angle_ref[half:ROT, :]
    rest = HEAD_DIM - ROT
    count = cos8.shape[1]
    ones = jnp.ones((rest, count), F32)
    zeros = jnp.zeros((rest, count), F32)
    z8 = jnp.zeros_like(sin8)
    tab_ref[0] = jnp.concatenate([cos8, cos8, ones] * 2, axis=0).T
    tab_ref[1] = jnp.concatenate([-sin8, z8, zeros] * 2, axis=0).T
    tab_ref[2] = jnp.concatenate([z8, sin8, zeros] * 2, axis=0).T


def turn(u, tab_ref, sign):
    half = ROT // 2
    ahead = pltpu.roll(u, PAIR - half, 1)
    behind = pltpu.roll(u, half, 1)
    return u * tab_ref[0] + sign * (ahead * tab_ref[1] + behind * tab_ref[2])


def low_lanes(shape):
    return lax.broadcasted_iota(jnp.int32, shape, 1) < HEAD_DIM


def project_kernel(x_ref, gain_ref, shift_ref, w_ref, b_ref, ang_ref, og_ref, wd_ref,
                   q_ref, kv_ref, do_ref, norm, tab):
    @pl.when(pl.program_id(0) == 0)
    def _():
        norm_rows(x_ref, gain_ref, shift_ref, norm)
        build_tables(ang_ref, tab)

    for n in range(STEP_PAIRS):
        cols = slice(n * 3 * PAIR, (n + 1) * 3 * PAIR)
        mine = slice(n * PAIR, (n + 1) * PAIR)
        mixed = dot(norm[...], w_ref[:, cols]) + b_ref[:, cols]
        t0, t1, t2 = mixed[:, :PAIR], mixed[:, PAIR:2 * PAIR], mixed[:, 2 * PAIR:]
        low = low_lanes(t0.shape)
        q = jnp.where(low, t0, t1)
        k = pltpu.roll(jnp.where(low, t2, t0), HEAD_DIM, 1)
        v = jnp.where(low, t1, t2)
        q_ref[:, mine] = turn(q, tab, 1.0).astype(BF16)
        kv_ref[0, :, mine] = turn(k, tab, 1.0).astype(BF16)
        kv_ref[1, :, mine] = v.astype(BF16)
    do_ref[...] = dot_t(og_ref[...], wd_ref[...]).astype(BF16)


def project(x, gain, shift, w, b, ang, og, wd):
    rows, width = x.shape
    wide = STEP_PAIRS * PAIR
    tok = pl.BlockSpec((rows, wide), lambda i: (0, i))
    return pl.pallas_call(
        project_kernel,
        grid=(width // wide,),
        out_shape=(
            jax.ShapeDtypeStruct((rows, width), BF16),
            jax.ShapeDtypeStruct((2, rows, width), BF16),
            jax.ShapeDtypeStruct((rows, width), BF16),
        ),
        in_specs=[
            whole((rows, width)), whole((1, width)), whole((1, width)),
            pl.BlockSpec((width, 3 * wide), lambda i: (0, i)),
            pl.BlockSpec((1, 3 * wide), lambda i: (0, i)),
            whole(ang.shape), whole((rows, width)),
            pl.BlockSpec((wide, width), lambda i: (i, 0)),
        ],
        out_specs=(tok, pl.BlockSpec((2, rows, wide), lambda i: (0, 0, i)), tok),
        scratch_shapes=[pltpu.VMEM((rows, width), BF16), pltpu.VMEM((3, rows, PAIR), F32)],
        compiler_params=params(),
        cost_estimate=cost(8 * rows * width * width, 24 * rows * width),
        name="project",
    )(x, gain, shift, w, b, ang, og, wd)


def gelu_parts(h):
    z = jnp.abs(h) * math.sqrt(0.5)
    t = 1.0 / (1.0 + 0.5 * z)
    poly = jnp.full_like(t, 0.17087277)
    for c in (-0.82215223, 1.48851587, -1.13520398, 0.27886807, -0.18628806, 0.09678418,
              0.37409196, 1.00002368, -1.26551223):
        poly = poly * t + c
    zz = z * z
    tail = 0.5 * t * jnp.exp(poly - zz)
    cdf = jnp.where(h >= 0, 1.0 - tail, tail)
    slope = cdf + h * (jnp.exp(-zz) * (1.0 / math.sqrt(2.0 * math.pi)))
    return h * cdf, slope


def mlp_fwd_kernel(take, x_ref, gain_ref, shift_ref, we_ref, be_ref, wr_ref, og_ref,
                   mid_ref, slope_ref, dwr_ref, dog_ref, norm):
    step = pl.program_id(0)
    width = x_ref.shape[1]

    @pl.when(step == 0)
    def _():
        norm_rows(x_ref, gain_ref, shift_ref, norm)
        mid_ref[...] = jnp.zeros_like(mid_ref)
        dog_ref[...] = jnp.sum(og_ref[...].astype(F32), axis=0, keepdims=True)

    h = dot(norm[...], we_ref[...]) + be_ref[...]
    active, slope = gelu_parts(h)
    active = active.astype(BF16)
    slope_ref[...] = slope.astype(BF16)
    mid_ref[...] += dot(active, wr_ref[...])
    dwr = dot(active.T, og_ref[...]).astype(BF16)
    full = dwr_ref.shape[1]
    ratio = full // width
    for piece in range(FB // take):
        group, j = piece // ratio, piece % ratio
        dwr_ref[group * take:(group + 1) * take, j * width:(j + 1) * width] = (
            dwr[piece * take:(piece + 1) * take, :])


def mlp_back_kernel(x_ref, gain_ref, shift_ref, we_ref, wr_ref, og_ref, slope_ref,
                    part_ref, dwe_ref, dbe_ref, dgain_ref, dshift_ref, norm, norm_t, sg):
    step = pl.program_id(0)

    @pl.when(step == 0)
    def _():
        norm_rows(x_ref, gain_ref, shift_ref, norm)
        norm_t[...] = norm[...].T
        sg[...] = jnp.zeros_like(sg)

    hidden = (dot_t(og_ref[...], wr_ref[...]) * slope_ref[...].astype(F32)).astype(BF16)
    dwe_ref[...] = dot(norm_t[...], hidden).astype(BF16)
    dbe_ref[...] = jnp.sum(hidden.astype(F32), axis=0, keepdims=True)
    sg[...] += dot_t(hidden, we_ref[...])

    @pl.when(step == pl.num_programs(0) - 1)
    def _():
        def emit(rows, part):
            part_ref[rows, :] = part

        norm_back(x_ref, gain_ref, sg, dgain_ref, dshift_ref, emit)


def mlp_specs(x):
    rows, width = x.shape
    full = whole((rows, width))
    vec = whole((1, width))
    up = pl.BlockSpec((width, FB), lambda i: (0, i))
    down = pl.BlockSpec((FB, width), lambda i: (i, 0))
    bias = pl.BlockSpec((1, FB), lambda i: (0, i))
    act = pl.BlockSpec((rows, FB), lambda i: (0, i))
    return full, vec, up, down, bias, act


def mlp_fwd(ndev, x, gain, shift, we, be, wr, og):
    rows, width = x.shape
    hidden = we.shape[1]
    full, vec, up, down, bias, act = mlp_specs(x)
    out_rows = hidden // (hidden // width)
    blk = FB * out_rows // hidden
    gshape = (out_rows, hidden)
    return pl.pallas_call(
        partial(mlp_fwd_kernel, out_rows // ndev),
        grid=(hidden // FB,),
        out_shape=(jax.ShapeDtypeStruct((rows, width), F32), jax.ShapeDtypeStruct((rows, hidden), BF16),
                   jax.ShapeDtypeStruct(gshape, BF16), jax.ShapeDtypeStruct((1, width), F32)),
        in_specs=[full, vec, vec, up, bias, down, full],
        out_specs=(full, act, pl.BlockSpec((blk, gshape[1]), lambda i: (i, 0)), vec),
        scratch_shapes=[pltpu.VMEM((rows, width), BF16)],
        compiler_params=params(),
        cost_estimate=cost(6 * rows * width * hidden, 8 * width * hidden),
        name="mlp_fwd",
    )(x, gain, shift, we, be, wr, og)


def mlp_back(x, gain, shift, we, wr, og, slope):
    rows, width = x.shape
    hidden = we.shape[1]
    full, vec, up, down, bias, act = mlp_specs(x)
    vshape = jax.ShapeDtypeStruct((1, width), F32)
    return pl.pallas_call(
        mlp_back_kernel,
        grid=(hidden // FB,),
        out_shape=(jax.ShapeDtypeStruct((rows, width), F32),
                   jax.ShapeDtypeStruct((width, hidden), BF16),
                   jax.ShapeDtypeStruct((1, hidden), F32), vshape, vshape),
        in_specs=[full, vec, vec, up, down, full, act],
        out_specs=(full, up, bias, vec, vec),
        scratch_shapes=[pltpu.VMEM((rows, width), BF16), pltpu.VMEM((width, rows), BF16),
                        pltpu.VMEM((rows, width), F32)],
        compiler_params=params(),
        cost_estimate=cost(6 * rows * width * hidden, 8 * width * hidden),
        name="mlp_back",
    )(x, gain, shift, we, wr, og, slope)


MESH = pl.DeviceIdType.MESH


class Halving:
    def __init__(self, bits, parts, chunks, mats, own, recv, send_sem, recv_sem):
        self.bits, self.parts, self.chunks = bits, parts, chunks
        self.mats, self.own, self.recv = mats, own, recv
        self.send_sem, self.recv_sem = send_sem, recv_sem
        self.me_b, self.me_s = lax.axis_index("batch"), lax.axis_index("seq")
        self.bit = [lax.rem(self.me_b // (1 << k), 2) for k in range(bits)]
        self.mate = [
            (self.me_b + (1 << k) - 2 * (1 << k) * self.bit[k], self.me_s) for k in range(bits)]
        self.others = [(self.me_b, lax.rem(self.me_s + d, parts)) for d in range(1, parts)]
        self.peers = self.mate + self.others

    def barrier(self):
        sem = pltpu.get_barrier_semaphore()
        for peer in self.peers:
            pl.semaphore_signal(sem, inc=1, device_id=peer, device_id_type=MESH)
        pl.semaphore_wait(sem, len(self.peers))

    def copy(self, slot, n, src, dst, peer):
        return pltpu.make_async_remote_copy(
            src_ref=src, dst_ref=dst, send_sem=self.send_sem.at[slot, n],
            recv_sem=self.recv_sem.at[slot, n], device_id=peer, device_id_type=MESH)

    def dims(self, order, stage):
        return [d for d in range(self.bits - 1, -1, -1) if d not in order[:stage]]

    def part(self, c, value):
        mat, col, size, order = self.chunks[c]
        index = tuple(value if d == order[0] else slice(None) for d in self.dims(order, 0))
        return self.mats[mat].at[index + (slice(None), slice(None), pl.ds(col, size))]

    def copies(self, c, stage):
        order = self.chunks[c][3]
        if stage == self.bits:
            return [
                self.copy(c, self.bits + n, self.recv[c][stage - 1].at[peer[1]], self.recv[c][stage].at[n], peer)
                for n, peer in enumerate(self.others)]
        k = order[stage]
        if stage == 0:
            src = self.part(c, 1 - self.bit[k])
        else:
            index = tuple(1 - self.bit[k] if d == k else slice(None) for d in self.dims(order, stage))
            src = self.recv[c][stage - 1].at[index]
        return [self.copy(c, stage, src, self.recv[c][stage], self.mate[k])]

    def start(self, c, stage):
        for copy in self.copies(c, stage):
            copy.start()

    def wait_sends(self, c):
        for stage in range(self.bits + 1):
            for copy in self.copies(c, stage):
                copy.wait_send()

    def add(self, c, stage):
        mat, col, size, order = self.chunks[c]
        k = order[stage]
        dims = self.dims(order, stage)
        self.copies(c, stage)[0].wait_recv()
        dst = self.recv[c][stage]
        lead = self.bits - 1 - stage

        def one(i, carry):
            part = lax.rem(i, self.parts)
            rest = i // self.parts
            sub = tuple(lax.rem(rest // (1 << (lead - 1 - n)), 2) for n in range(lead))
            at = sub + (part,)
            left = list(sub)
            own_at = tuple(self.bit[k] if d == k else left.pop(0) for d in dims) + (part,)
            if stage > 0:
                own = self.recv[c][stage - 1][own_at]
            elif self.own is None:
                own = self.mats[mat][own_at + (slice(None), pl.ds(col, size))]
            else:
                own = self.own[c][at]
            dst[at] = (own.astype(F32) + dst[at].astype(F32)).astype(BF16)
            return carry

        lax.fori_loop(0, self.parts << lead, one, 0)

    def total(self, c):
        total = self.recv[c][self.bits - 1][self.me_s].astype(F32)
        for n, copy in enumerate(self.copies(c, self.bits)):
            copy.wait_recv()
            total = total + self.recv[c][self.bits][n].astype(F32)
        return total


def halving_orders(bits):
    plain = list(range(bits))
    other = [0] + [k for i in range(1, bits, 2) for k in reversed(range(i, min(i + 2, bits)))]
    return plain, other


def halving_scratch(bits, parts, rows, chunks):
    scratch = []
    for _, _, size, _ in chunks:
        for stage in range(bits):
            scratch.append(pltpu.VMEM((2,) * (bits - 1 - stage) + (parts, rows, size), BF16))
        scratch.append(pltpu.VMEM((parts - 1, rows, size), BF16))
    return scratch


def attend_pair(flag_ref, q_ref, kv_ref, kvp_ref, do_ref, o_ref, dq_ref, dkv_ref, dkvp_ref,
                pt, ds, kvt, qm, dom):
    rows_all = q_ref.shape[0]
    nq = rows_all // QB
    away = (flag_ref[0] - 1).astype(F32) * (-MASKED)
    sources = [(kvp_ref, i) for i in range(nq)] + [(kv_ref, i) for i in range(nq)]

    def block(which, b):
        ref, i = sources[b]
        return ref[which, i * QB:(i + 1) * QB, :]

    for which in range(2):
        kvt[which, :, :rows_all] = kvp_ref[which].T
        kvt[which, :, rows_all:] = kv_ref[which].T
    lane = lax.broadcasted_iota(jnp.int32, (QB, PAIR), 1)
    sub = lax.broadcasted_iota(jnp.int32, (PAIR, QB), 0)
    causal = lax.broadcasted_iota(jnp.int32, (QB, QB), 0) <= lax.broadcasted_iota(
        jnp.int32, (QB, QB), 1)
    for j in range(nq):
        rows = slice(j * QB, (j + 1) * QB)
        q = q_ref[rows, :] * jnp.asarray(SCALE, BF16)
        qt = q.T
        dot_rows = do_ref[rows, :].astype(F32).T
        blocks = range(nq + j + 1)
        k1 = (nq + j + 1) * QB
        outs, scaled, dqs = [], [], []
        for h in range(2):
            hs = slice(h * HEAD_DIM, (h + 1) * HEAD_DIM)
            qm[h, rows, :] = jnp.where((lane < HEAD_DIM) == (h == 0), q, jnp.zeros_like(q))
            qtm = jnp.where((sub < HEAD_DIM) == (h == 0), qt, jnp.zeros_like(qt))
            scores, tops = [], [None, None]
            for b in blocks:
                s = dot(block(0, b), qtm)
                if b == nq + j:
                    s = jnp.where(causal, s, MASKED)
                scores.append(s)
                part = jnp.max(s.reshape(QB // 8, 8, QB), axis=0)
                side = int(b >= nq)
                tops[side] = part if tops[side] is None else jnp.maximum(tops[side], part)
            top = jnp.max(jnp.maximum(tops[0] + away, tops[1]), axis=0, keepdims=True)
            shift = (top - away, top)
            total = None
            for b, s in zip(blocks, scores):
                p = jnp.exp(s - shift[int(b >= nq)])
                part = jnp.sum(p.reshape(QB // 8, 8, QB), axis=0)
                total = part if total is None else total + part
                pt[h, b * QB:(b + 1) * QB, rows] = p.astype(BF16)
            inv = 1.0 / jnp.sum(total, axis=0, keepdims=True)
            out_t = dot(kvt[1, hs, :k1], pt[h, :k1, rows]) * inv
            dol_t = dot_rows[hs] * inv
            delta = jnp.sum(dol_t * out_t, axis=0, keepdims=True)
            outs.append(out_t)
            scaled.append(dol_t)
            zero = jnp.zeros((HEAD_DIM, QB), BF16)
            dol_b = dol_t.astype(BF16)
            dol_m = jnp.concatenate([dol_b, zero] if h == 0 else [zero, dol_b], axis=0)
            for b in blocks:
                dp = dot(block(1, b), dol_m)
                d = pt[h, b * QB:(b + 1) * QB, rows].astype(F32) * (dp - delta)
                ds[h, b * QB:(b + 1) * QB, rows] = d.astype(BF16)
            dqs.append(dot(kvt[0, hs, :k1], ds[h, :k1, rows]) * SCALE)
        o_ref[rows, :] = jnp.concatenate(outs, 0).T.astype(BF16)
        dq_ref[rows, :] = jnp.concatenate(dqs, 0).T.astype(BF16)
        dol = jnp.concatenate(scaled, 0).T.astype(BF16)
        for h in range(2):
            dom[h, rows, :] = jnp.where((lane < HEAD_DIM) == (h == 0), dol, jnp.zeros_like(dol))
    for b in range(2 * nq):
        q0 = max(0, b - nq) * QB
        br = slice(b * QB, (b + 1) * QB)
        dk = dot(ds[0, br, q0:], qm[0, q0:, :]) + dot(ds[1, br, q0:], qm[1, q0:, :])
        dv = dot(pt[0, br, q0:], dom[0, q0:, :]) + dot(pt[1, br, q0:], dom[1, q0:, :])
        ref, i = (dkvp_ref, b) if b < nq else (dkv_ref, b - nq)
        ref[0, i * QB:(i + 1) * QB, :] = dk.astype(BF16)
        ref[1, i * QB:(i + 1) * QB, :] = dv.astype(BF16)


def attend_kernel(bits, parts, chunks, flag_ref, q_ref, kv_ref, kvp_ref, do_ref, gw_ref, gr_ref,
                  o_ref, dq_ref, dkv_ref, dkvn_ref, outw_ref, outr_ref, *refs):
    nchunk = len(chunks)
    own, refs = refs[:nchunk], refs[nchunk:]
    recv = [refs[c * (bits + 1):(c + 1) * (bits + 1)] for c in range(nchunk)]
    (pt, ds, kvt, qm, dom, back, own_sem, send_sem, recv_sem, back_send, back_recv) = refs[
        nchunk * (bits + 1):]
    red = Halving(bits, parts, chunks, (gw_ref, gr_ref), own, recv, send_sem, recv_sem)
    step = pl.program_id(0)
    steps = dkvn_ref.shape[2] // PAIR

    def own_copy(c):
        return pltpu.make_async_copy(red.part(c, red.bit[chunks[c][3][0]]), own[c], own_sem.at[c])

    def back_copy(i):
        cols = pl.ds(pl.multiple_of(i * PAIR, PAIR), PAIR)
        return pltpu.make_async_remote_copy(
            src_ref=back.at[lax.rem(i, 2)], dst_ref=dkvn_ref.at[:, :, cols],
            send_sem=back_send.at[i], recv_sem=back_recv.at[i],
            device_id=red.others[parts - 2], device_id_type=MESH)

    @pl.when(step == 0)
    def _():
        red.barrier()
        for c in range(nchunk):
            red.start(c, 0)
        for c in range(nchunk):
            own_copy(c).start()

    moments = [max(1, steps * m // 8) for m in (1, 4, 6)]
    moments += [moments[-1]] * (bits - 3)
    for stage in range(bits):
        @pl.when(step == moments[stage])
        def _(stage=stage):
            for c in range(nchunk):
                if stage == 0:
                    own_copy(c).wait()
                red.add(c, stage)
                red.start(c, stage + 1)

    @pl.when(step >= 2)
    def _():
        back_copy(step - 2).wait_send()

    attend_pair(flag_ref, q_ref, kv_ref, kvp_ref, do_ref, o_ref, dq_ref, dkv_ref,
                back.at[lax.rem(step, 2)], pt, ds, kvt, qm, dom)
    back_copy(step).start()

    @pl.when(step == steps - 1)
    def _():
        rows = outw_ref.shape[0]
        width = outr_ref.shape[1]
        for c in range(nchunk):
            mat, col, size, _ = chunks[c]
            total = red.total(c)
            if mat == 0:
                outw_ref[:, col:col + size] = total
            else:
                for n in range(size // width):
                    j = col // width + n
                    outr_ref[j * rows:(j + 1) * rows, :] = total[:, n * width:(n + 1) * width]
        for c in range(nchunk):
            red.wait_sends(c)
        for i in range(max(0, steps - 2), steps):
            back_copy(i).wait_send()
        for i in range(steps):
            back_copy(i).wait_recv()


def attend(bits, parts, flag, q, kv, kvp, do, gw, gr):
    rows, width = q.shape
    steps = width // PAIR
    hidden = gw.shape[1]
    take = gw.shape[0] // (parts << bits)
    shaped = [g.reshape((2,) * bits + (parts, take, hidden)) for g in (gw, gr)]
    plain, other = halving_orders(bits)
    chunks = [(0, 0, hidden // 2, plain), (1, 0, hidden // 2, other),
              (0, hidden // 2, hidden // 2, plain), (1, hidden // 2, hidden // 2, other)]
    npeer = bits + parts - 1
    tok = pl.BlockSpec((rows, PAIR), lambda i: (0, i))
    kvs = pl.BlockSpec((2, rows, PAIR), lambda i: (0, 0, i))
    hbm = pl.BlockSpec(memory_space=pl.ANY)
    tok_shape = jax.ShapeDtypeStruct((rows, width), BF16)
    kv_shape = jax.ShapeDtypeStruct((2, rows, width), BF16)
    fold = hidden // width
    outw, outr = (take, hidden), (take * fold, width)
    return pl.pallas_call(
        partial(attend_kernel, bits, parts, chunks),
        grid=(steps,),
        out_shape=(tok_shape, tok_shape, kv_shape, kv_shape,
                   jax.ShapeDtypeStruct(outw, F32), jax.ShapeDtypeStruct(outr, F32)),
        in_specs=[pl.BlockSpec(memory_space=pltpu.SMEM), tok, kvs, kvs, tok, hbm, hbm],
        out_specs=(tok, tok, kvs, hbm, whole(outw), whole(outr)),
        scratch_shapes=[
            pltpu.VMEM((2,) * (bits - 1) + (parts, take, size), BF16) for _, _, size, _ in chunks
        ] + halving_scratch(bits, parts, take, chunks) + [
            pltpu.VMEM((2, 2 * rows, rows), BF16),
            pltpu.VMEM((2, 2 * rows, rows), BF16),
            pltpu.VMEM((2, PAIR, 2 * rows), BF16),
            pltpu.VMEM((2, rows, PAIR), BF16),
            pltpu.VMEM((2, rows, PAIR), BF16),
            pltpu.VMEM((2, 2, rows, PAIR), BF16),
            pltpu.SemaphoreType.DMA((len(chunks),)),
            pltpu.SemaphoreType.DMA((len(chunks), npeer)),
            pltpu.SemaphoreType.DMA((len(chunks), npeer)),
            pltpu.SemaphoreType.DMA((steps,)),
            pltpu.SemaphoreType.DMA((steps,)),
        ],
        compiler_params=pltpu.CompilerParams(
            vmem_limit_bytes=63 << 20, collective_id=1, has_side_effects=True),
        cost_estimate=cost(60 * rows * rows * width, 20 * rows * width),
        name="attend",
    )(flag, q, kv, kvp, do, *shaped)


def qkv_back_kernel(x_ref, gain_ref, shift_ref, w_ref, ang_ref, dq_ref, dkv_ref, dkvn_ref,
                    og_ref, part_ref, dw_ref, db_ref, ig_ref, dgain_ref, dshift_ref,
                    norm, norm_t, tab, fg):
    step = pl.program_id(0)

    @pl.when(step == 0)
    def _():
        norm_rows(x_ref, gain_ref, shift_ref, norm)
        norm_t[...] = norm[...].T
        build_tables(ang_ref, tab)
        fg[...] = jnp.zeros_like(fg)

    blocks = []
    for n in range(STEP_PAIRS):
        mine = slice(n * PAIR, (n + 1) * PAIR)
        dq = turn(dq_ref[:, mine].astype(F32), tab, -1.0)
        dk = turn(dkv_ref[0, :, mine].astype(F32) + dkvn_ref[0, :, mine].astype(F32), tab, -1.0)
        dv = dkv_ref[1, :, mine].astype(F32) + dkvn_ref[1, :, mine].astype(F32)
        low = low_lanes(dq.shape)
        dk = pltpu.roll(dk, HEAD_DIM, 1)
        blocks += [jnp.where(low, dq, dk), jnp.where(low, dv, dq), jnp.where(low, dk, dv)]
    dm = jnp.concatenate(blocks, axis=1).astype(BF16)
    db_ref[...] = jnp.sum(dm.astype(F32), axis=0, keepdims=True)
    dw_ref[...] = dot(norm_t[...], dm).astype(BF16)
    fg[...] += dot_t(dm, w_ref[...])

    @pl.when(step == pl.num_programs(0) - 1)
    def _():
        def emit(rows, part):
            total = og_ref[rows, :].astype(F32) + part + part_ref[rows, :]
            ig_ref[rows, :] = total.astype(BF16)

        norm_back(x_ref, gain_ref, fg, dgain_ref, dshift_ref, emit)


def qkv_back(x, gain, shift, w, ang, dq, dkv, dkvn, og, part):
    rows, width = x.shape
    full, vec = whole((rows, width)), whole((1, width))
    wide = STEP_PAIRS * PAIR
    cols = 3 * wide
    tok = pl.BlockSpec((rows, wide), lambda i: (0, i))
    kvs = pl.BlockSpec((2, rows, wide), lambda i: (0, 0, i))
    up, bias = pl.BlockSpec((width, cols), lambda i: (0, i)), pl.BlockSpec((1, cols), lambda i: (0, i))
    vshape = jax.ShapeDtypeStruct((1, width), F32)
    return pl.pallas_call(
        qkv_back_kernel,
        grid=(width // wide,),
        out_shape=(jax.ShapeDtypeStruct((width, 3 * width), BF16), jax.ShapeDtypeStruct((1, 3 * width), F32),
                   jax.ShapeDtypeStruct((rows, width), BF16), vshape, vshape),
        in_specs=[full, vec, vec, up, whole(ang.shape), tok, kvs, kvs, full, full],
        out_specs=(up, bias, full, vec, vec),
        scratch_shapes=[pltpu.VMEM((rows, width), BF16), pltpu.VMEM((width, rows), BF16),
                        pltpu.VMEM((3, rows, PAIR), F32), pltpu.VMEM((rows, width), F32)],
        compiler_params=params(),
        cost_estimate=cost(12 * rows * width * width, 8 * rows * width),
        name="qkv_back",
    )(x, gain, shift, w, ang, dq, dkv, dkvn, og, part)


def dense_kernel(o_ref, wd_ref, db_ref, rb_ref, mid_ref, x_ref, og_ref, out_ref, dwd_ref, ot):
    @pl.when(pl.program_id(0) == 0)
    def _():
        ot[...] = o_ref[...].T

    total = x_ref[...].astype(F32) + mid_ref[...] + (db_ref[...] + rb_ref[...])
    out_ref[...] = (total + dot(o_ref[...], wd_ref[...])).astype(BF16)
    dwd_ref[...] = dot(ot[...], og_ref[...]).astype(BF16)


def dense(o, wd, db, rb, mid, x, og):
    rows, width = x.shape
    blk = 256
    col = lambda r: pl.BlockSpec((r, blk), lambda i: (0, i))
    return pl.pallas_call(
        dense_kernel,
        grid=(width // blk,),
        out_shape=(jax.ShapeDtypeStruct((rows, width), BF16), jax.ShapeDtypeStruct((width, width), BF16)),
        in_specs=[whole(o.shape), col(width), col(1), col(1), col(rows), col(rows), col(rows)],
        out_specs=(col(rows), col(width)),
        scratch_shapes=[pltpu.VMEM((width, rows), BF16)],
        compiler_params=params(),
        cost_estimate=cost(4 * rows * width * width, 12 * rows * width),
        name="dense",
    )(o, wd, db, rb, mid, x, og)


def scatter_kernel(bits, parts, nmat, chunks, vec_sizes, *refs):
    nvec, nchunk = len(vec_sizes), len(chunks)
    mats, vecs = refs[:nmat], refs[nmat:nmat + nvec]
    outs, vec_out = refs[nmat + nvec:2 * nmat + nvec], refs[2 * nmat + nvec]
    refs = refs[2 * nmat + nvec + 1:]
    recv = [refs[c * (bits + 1):(c + 1) * (bits + 1)] for c in range(nchunk)]
    state, vrecv, send_sem, recv_sem = refs[nchunk * (bits + 1):]
    red = Halving(bits, parts, chunks, mats, None, recv, send_sem, recv_sem)
    red.barrier()
    for c in range(nchunk):
        red.start(c, 0)
    at = 0
    for ref, n in zip(vecs, vec_sizes):
        state[0, :, at:at + n] = ref[...]
        at += n

    def vec_copies(stage):
        if stage < bits:
            return [red.copy(nchunk, stage, state.at[stage], vrecv.at[stage], red.mate[stage])]
        return [red.copy(nchunk, bits + n, state.at[bits], vrecv.at[bits + n], peer)
                for n, peer in enumerate(red.others)]

    def vec_start(stage):
        for copy in vec_copies(stage):
            copy.start()

    def vec_add(stage):
        copies = vec_copies(stage)
        for copy in copies:
            copy.wait_recv()
        total = state[stage]
        for n in range(len(copies)):
            total = total + vrecv[stage + n]
        if stage < bits:
            state[stage + 1] = total
            vec_start(stage + 1)
        else:
            vec_out[...] = total

    vec_start(0)
    for stage in range(bits + 1):
        for c in range(nchunk):
            if stage < bits:
                red.add(c, stage)
                red.start(c, stage + 1)
            else:
                mat, col, size, _ = chunks[c]
                outs[mat][:, col:col + size] = red.total(c)
        vec_add(stage)
    for c in range(nchunk):
        red.wait_sends(c)
    for stage in range(bits + 1):
        for copy in vec_copies(stage):
            copy.wait_send()


def scatter(bits, parts, mats, vecs):
    shards = parts << bits
    rows = mats[0].shape[0] // shards
    widths = [m.shape[1] for m in mats]
    shaped = [m.reshape((2,) * bits + (parts, rows, m.shape[1])) for m in mats]
    plain, other = halving_orders(bits)
    chunks = []
    for m, w in enumerate(widths):
        size = w // 4 if w > 2048 else w // 2
        for n in range(w // size):
            chunks.append((m, n * size, size, other if n % 2 else plain))
    vec_sizes = [v.shape[1] for v in vecs]
    total = sum(vec_sizes)
    npeer = bits + parts - 1
    scratch = halving_scratch(bits, parts, rows, chunks) + [
        pltpu.VMEM((bits + 1, 1, total), F32),
        pltpu.VMEM((npeer, 1, total), F32),
        pltpu.SemaphoreType.DMA((len(chunks) + 1, npeer)),
        pltpu.SemaphoreType.DMA((len(chunks) + 1, npeer)),
    ]
    vmem = pl.BlockSpec(memory_space=pltpu.VMEM)
    return pl.pallas_call(
        partial(scatter_kernel, bits, parts, len(mats), chunks, vec_sizes),
        out_shape=tuple(jax.ShapeDtypeStruct((rows, w), F32) for w in widths)
        + (jax.ShapeDtypeStruct((1, total), F32),),
        in_specs=[vmem] * (len(mats) + len(vecs)),
        out_specs=tuple([vmem] * (len(mats) + 1)),
        scratch_shapes=scratch,
        compiler_params=pltpu.CompilerParams(
            vmem_limit_bytes=VMEM_LIMIT, collective_id=0, has_side_effects=True),
        name="scatter",
    )(*shaped, *vecs)


def body(
    tokens,
    seq_lengths,
    attn_gain,
    attn_shift,
    qkv_weight,
    qkv_bias,
    dense_weight,
    dense_bias,
    mlp_gain,
    mlp_shift,
    expand_weight,
    expand_bias,
    reduce_weight,
    reduce_bias,
    out_grad,
):
    seq_parts = lax.axis_size("seq")
    place = lax.axis_index("seq")
    rows, width = tokens.shape
    lengths = seq_lengths[0]
    starts = jnp.cumsum(lengths) - lengths
    row0 = place * rows
    offset = row0 - jnp.max(jnp.where(starts <= row0, starts, 0))
    flag = (offset > 0).astype(jnp.int32).reshape(1)
    positions = (offset + jnp.arange(rows, dtype=jnp.int32)).astype(F32)
    frequency = jnp.exp(jnp.arange(ROT // 2, dtype=F32) * (-2.0 * math.log(10000.0) / ROT))
    phases = frequency[:, None] * positions[None, :]
    ang = jnp.concatenate([jnp.cos(phases), jnp.sin(phases)], axis=0)

    row = lambda v: v.reshape(1, -1)
    ag, ash, mg, msh = row(attn_gain), row(attn_shift), row(mlp_gain), row(mlp_shift)
    onward = [(i, i + 1) for i in range(seq_parts - 1)]

    batch_parts = lax.axis_size("batch")
    ndev = batch_parts * seq_parts
    bits = batch_parts.bit_length() - 1
    q, kv, do = project(tokens, ag, ash, qkv_weight, row(qkv_bias), ang, out_grad, dense_weight)
    kvp = lax.ppermute(kv, "seq", onward)
    mid, slope, dwr, dog = mlp_fwd(
        ndev, tokens, mg, msh, expand_weight, row(expand_bias), reduce_weight, out_grad)
    part, dwe, dbe, dmg, dms = mlp_back(
        tokens, mg, msh, expand_weight, reduce_weight, out_grad, slope)

    o, dq, dkv, dkvn, dwe, dwr = attend(bits, seq_parts, flag, q, kv, kvp, do, dwe, dwr)
    layer_out, dwd = dense(o, dense_weight, row(dense_bias), row(reduce_bias), mid, tokens, out_grad)
    dw, db, input_grad, dag, das = qkv_back(
        tokens, ag, ash, qkv_weight, ang, dq, dkv, dkvn, out_grad, part)
    vecs = [dag, das, db, dog, dmg, dms, dbe]
    dw, dwd, vsum = scatter(bits, seq_parts, [dw, dwd], vecs)
    index = lax.axis_index("batch") * seq_parts + place
    pieces, at = [], 0
    for size in (width, width, 3 * width, width, width, width, dbe.shape[1]):
        own = size // ndev
        pieces.append(lax.dynamic_slice(vsum, (0, at + index * own), (1, own)).reshape(own))
        at += size
    dag, das, dqb, dog, dmg, dms, dbe = pieces
    return (
        layer_out,
        input_grad,
        dag,
        das,
        dw,
        dqb,
        dwd,
        dog,
        dmg,
        dms,
        dwe,
        dbe,
        dwr,
        dog,
    )


def solution(mesh):
    tok = P(("batch", "seq"), None)
    vec = P(("batch", "seq"))
    in_specs = (tok, P("batch", None)) + (P(),) * 12 + (tok,)
    out_specs = (tok, tok, vec, vec, tok, vec, tok, vec, vec, vec, tok, vec, tok, vec)
    return jax.shard_map(body, mesh=mesh, in_specs=in_specs, out_specs=out_specs, check_vma=False)
```

```python
from functools import partial
import math

import jax
import jax.numpy as jnp
from jax import lax
from jax.experimental import pallas as pl
from jax.experimental.pallas import tpu as pltpu
from jax.sharding import PartitionSpec as P


HEAD_DIM = 64
ROT = 16
PAIR = 2 * HEAD_DIM
EPSILON = 1e-05
MASKED = -1e30
SCALE = 1.0 / math.sqrt(HEAD_DIM)
QB = 256
FB = 1024
STEP_PAIRS = 2
ROWS = 128
F32 = jnp.float32
BF16 = jnp.bfloat16
VMEM_LIMIT = 60 << 20


def dot(left, right):
    return jnp.dot(left, right, preferred_element_type=F32)


def dot_t(left, right):
    return lax.dot_general(left, right, (((1,), (1,)), ((), ())), preferred_element_type=F32)


def params():
    return pltpu.CompilerParams(vmem_limit_bytes=VMEM_LIMIT)


def cost(flops, nbytes):
    return pl.CostEstimate(flops=int(flops), bytes_accessed=int(nbytes), transcendentals=0)


def whole(shape):
    return pl.BlockSpec(shape, lambda i: (0,) * len(shape), pipeline_mode=pl.Buffered(1))


def statistics(x):
    mean = jnp.mean(x, axis=-1, keepdims=True)
    centered = x - mean
    variance = jnp.mean(centered * centered, axis=-1, keepdims=True)
    rstd = lax.rsqrt(variance + EPSILON)
    return centered * rstd, rstd


def row_block(i):
    return pl.ds(pl.multiple_of(i * ROWS, ROWS), ROWS)


def norm_rows(x_ref, gains, outs):
    def step(i, carry):
        rows = row_block(i)
        xn, _ = statistics(x_ref[rows, :].astype(F32))
        for (gain_ref, shift_ref), out_ref in zip(gains, outs):
            out_ref[rows, :] = (xn * gain_ref[...] + shift_ref[...]).astype(BF16)
        return carry

    lax.fori_loop(0, x_ref.shape[0] // ROWS, step, 0)


def norm_back(x_ref, gains, grads, gain_grads, shift_grads, emit):
    for ref in gain_grads + shift_grads:
        ref[...] = jnp.zeros_like(ref)

    def step(i, carry):
        rows = row_block(i)
        xn, rstd = statistics(x_ref[rows, :].astype(F32))
        scaled = 0.0
        for gain_ref, grad_ref, dgain_ref, dshift_ref in zip(gains, grads, gain_grads, shift_grads):
            grad = grad_ref[rows, :]
            dgain_ref[...] += jnp.sum(grad * xn, axis=0, keepdims=True)
            dshift_ref[...] += jnp.sum(grad, axis=0, keepdims=True)
            scaled = scaled + grad * gain_ref[...]
        mean_s = jnp.mean(scaled, axis=-1, keepdims=True)
        mean_sx = jnp.mean(scaled * xn, axis=-1, keepdims=True)
        emit(rows, rstd * (scaled - mean_s - xn * mean_sx))
        return carry

    lax.fori_loop(0, x_ref.shape[0] // ROWS, step, 0)


def build_tables(angle_ref, tab_ref):
    half = ROT // 2
    cos8, sin8 = angle_ref[0:half, :], angle_ref[half:ROT, :]
    rest = HEAD_DIM - ROT
    count = cos8.shape[1]
    ones = jnp.ones((rest, count), F32)
    zeros = jnp.zeros((rest, count), F32)
    z8 = jnp.zeros_like(sin8)
    tab_ref[0] = jnp.concatenate([cos8, cos8, ones] * 2, axis=0).T
    tab_ref[1] = jnp.concatenate([-sin8, z8, zeros] * 2, axis=0).T
    tab_ref[2] = jnp.concatenate([z8, sin8, zeros] * 2, axis=0).T


def turn(u, tab_ref, sign):
    half = ROT // 2
    ahead = pltpu.roll(u, PAIR - half, 1)
    behind = pltpu.roll(u, half, 1)
    return u * tab_ref[0] + sign * (ahead * tab_ref[1] + behind * tab_ref[2])


def low_lanes(shape):
    return lax.broadcasted_iota(jnp.int32, shape, 1) < HEAD_DIM


def project_kernel(x_ref, gain_ref, shift_ref, gain2_ref, shift2_ref, w_ref, b_ref, ang_ref, og_ref,
                   wd_ref, q_ref, kv_ref, do_ref, n1t_ref, n2_ref, n2t_ref,
                   norm, n1t, n2, n2t, tab, sem):
    saves = [pltpu.make_async_copy(src, dst, sem.at[n]) for n, (src, dst) in enumerate(
        ((n1t, n1t_ref), (n2, n2_ref), (n2t, n2t_ref)))]

    @pl.when(pl.program_id(0) == 0)
    def _():
        norm_rows(x_ref, ((gain_ref, shift_ref), (gain2_ref, shift2_ref)), (norm, n2))
        saves[1].start()
        n1t[...] = norm[...].T
        saves[0].start()
        n2t[...] = n2[...].T
        saves[2].start()
        build_tables(ang_ref, tab)

    for n in range(STEP_PAIRS):
        cols = slice(n * 3 * PAIR, (n + 1) * 3 * PAIR)
        mine = slice(n * PAIR, (n + 1) * PAIR)
        mixed = dot(norm[...], w_ref[:, cols]) + b_ref[:, cols]
        t0, t1, t2 = mixed[:, :PAIR], mixed[:, PAIR:2 * PAIR], mixed[:, 2 * PAIR:]
        low = low_lanes(t0.shape)
        q = jnp.where(low, t0, t1)
        k = pltpu.roll(jnp.where(low, t2, t0), HEAD_DIM, 1)
        v = jnp.where(low, t1, t2)
        q_ref[:, mine] = turn(q, tab, 1.0).astype(BF16)
        kv_ref[0, :, mine] = turn(k, tab, 1.0).astype(BF16)
        kv_ref[1, :, mine] = v.astype(BF16)
    do_ref[...] = dot_t(og_ref[...], wd_ref[...]).astype(BF16)

    @pl.when(pl.program_id(0) == pl.num_programs(0) - 1)
    def _():
        for save in saves:
            save.wait()


def project(x, gain, shift, gain2, shift2, w, b, ang, og, wd):
    rows, width = x.shape
    wide = STEP_PAIRS * PAIR
    tok = pl.BlockSpec((rows, wide), lambda i: (0, i))
    return pl.pallas_call(
        project_kernel,
        grid=(width // wide,),
        out_shape=(
            jax.ShapeDtypeStruct((rows, width), BF16),
            jax.ShapeDtypeStruct((2, rows, width), BF16),
            jax.ShapeDtypeStruct((rows, width), BF16),
            jax.ShapeDtypeStruct((width, rows), BF16),
            jax.ShapeDtypeStruct((rows, width), BF16),
            jax.ShapeDtypeStruct((width, rows), BF16),
        ),
        in_specs=[
            whole((rows, width)), *[whole((1, width))] * 4,
            pl.BlockSpec((width, 3 * wide), lambda i: (0, i)),
            pl.BlockSpec((1, 3 * wide), lambda i: (0, i)),
            whole(ang.shape), whole((rows, width)),
            pl.BlockSpec((wide, width), lambda i: (i, 0)),
        ],
        out_specs=(tok, pl.BlockSpec((2, rows, wide), lambda i: (0, 0, i)), tok,
                   *[pl.BlockSpec(memory_space=pl.ANY)] * 3),
        scratch_shapes=[pltpu.VMEM((rows, width), BF16), pltpu.VMEM((width, rows), BF16),
                        pltpu.VMEM((rows, width), BF16), pltpu.VMEM((width, rows), BF16),
                        pltpu.VMEM((3, rows, PAIR), F32), pltpu.SemaphoreType.DMA((3,))],
        compiler_params=params(),
        cost_estimate=cost(8 * rows * width * width, 24 * rows * width),
        name="project",
    )(x, gain, shift, gain2, shift2, w, b, ang, og, wd)


def gelu_parts(h):
    z = jnp.abs(h) * math.sqrt(0.5)
    t = 1.0 / (1.0 + 0.5 * z)
    poly = jnp.full_like(t, 0.17087277)
    for c in (-0.82215223, 1.48851587, -1.13520398, 0.27886807, -0.18628806, 0.09678418,
              0.37409196, 1.00002368, -1.26551223):
        poly = poly * t + c
    zz = z * z
    tail = 0.5 * t * jnp.exp(poly - zz)
    cdf = jnp.where(h >= 0, 1.0 - tail, tail)
    slope = cdf + h * (jnp.exp(-zz) * (1.0 / math.sqrt(2.0 * math.pi)))
    return h * cdf, slope


def mlp_fwd_kernel(take, norm, we_ref, be_ref, wr_ref, og_ref, mid_ref, slope_ref, dwr_ref, dog_ref):
    step = pl.program_id(0)
    width = norm.shape[1]

    @pl.when(step == 0)
    def _():
        mid_ref[...] = jnp.zeros_like(mid_ref)
        dog_ref[...] = jnp.sum(og_ref[...].astype(F32), axis=0, keepdims=True)

    h = dot(norm[...], we_ref[...]) + be_ref[...]
    active, slope = gelu_parts(h)
    active = active.astype(BF16)
    slope_ref[...] = slope.astype(BF16)
    mid_ref[...] += dot(active, wr_ref[...])
    dwr = dot(active.T, og_ref[...]).astype(BF16)
    full = dwr_ref.shape[1]
    ratio = full // width
    for piece in range(FB // take):
        group, j = piece // ratio, piece % ratio
        dwr_ref[group * take:(group + 1) * take, j * width:(j + 1) * width] = (
            dwr[piece * take:(piece + 1) * take, :])


def mlp_back_kernel(norm_t, we_ref, wr_ref, og_ref, slope_ref, sg, dwe_ref, dbe_ref):
    @pl.when(pl.program_id(0) == 0)
    def _():
        sg[...] = jnp.zeros_like(sg)

    hidden = (dot_t(og_ref[...], wr_ref[...]) * slope_ref[...].astype(F32)).astype(BF16)
    dwe_ref[...] = dot(norm_t[...], hidden).astype(BF16)
    dbe_ref[...] = jnp.sum(hidden.astype(F32), axis=0, keepdims=True)
    sg[...] += dot_t(hidden, we_ref[...])


def mlp_specs(x):
    rows, width = x.shape
    full = whole((rows, width))
    vec = whole((1, width))
    up = pl.BlockSpec((width, FB), lambda i: (0, i))
    down = pl.BlockSpec((FB, width), lambda i: (i, 0))
    bias = pl.BlockSpec((1, FB), lambda i: (0, i))
    act = pl.BlockSpec((rows, FB), lambda i: (0, i))
    return full, vec, up, down, bias, act


def mlp_fwd(ndev, norm, we, be, wr, og):
    rows, width = norm.shape
    hidden = we.shape[1]
    full, vec, up, down, bias, act = mlp_specs(norm)
    out_rows = width
    blk = FB * out_rows // hidden
    gshape = (out_rows, hidden)
    return pl.pallas_call(
        partial(mlp_fwd_kernel, out_rows // ndev),
        grid=(hidden // FB,),
        out_shape=(jax.ShapeDtypeStruct((rows, width), F32), jax.ShapeDtypeStruct((rows, hidden), BF16),
                   jax.ShapeDtypeStruct(gshape, BF16), jax.ShapeDtypeStruct((1, width), F32)),
        in_specs=[full, up, bias, down, full],
        out_specs=(full, act, pl.BlockSpec((blk, hidden), lambda i: (i, 0)), vec),
        compiler_params=params(),
        cost_estimate=cost(6 * rows * width * hidden, 8 * width * hidden),
        name="mlp_fwd",
    )(norm, we, be, wr, og)


def mlp_back(norm_t, we, wr, og, slope):
    rows, width = og.shape
    hidden = we.shape[1]
    full, _, up, down, bias, act = mlp_specs(og)
    return pl.pallas_call(
        mlp_back_kernel,
        grid=(hidden // FB,),
        out_shape=(jax.ShapeDtypeStruct((rows, width), F32), jax.ShapeDtypeStruct((width, hidden), BF16),
                   jax.ShapeDtypeStruct((1, hidden), F32)),
        in_specs=[whole(norm_t.shape), up, down, full, act],
        out_specs=(full, up, bias),
        compiler_params=params(),
        cost_estimate=cost(6 * rows * width * hidden, 8 * width * hidden),
        name="mlp_back",
    )(norm_t, we, wr, og, slope)


MESH = pl.DeviceIdType.MESH


class Halving:
    def __init__(self, bits, parts, chunks, mats, own, recv, send_sem, recv_sem):
        self.bits, self.parts, self.chunks = bits, parts, chunks
        self.mats, self.own, self.recv = mats, own, recv
        self.send_sem, self.recv_sem = send_sem, recv_sem
        self.me_b, self.me_s = lax.axis_index("batch"), lax.axis_index("seq")
        self.bit = [lax.rem(self.me_b // (1 << k), 2) for k in range(bits)]
        self.mate = [
            (self.me_b + (1 << k) - 2 * (1 << k) * self.bit[k], self.me_s) for k in range(bits)]
        self.others = [(self.me_b, lax.rem(self.me_s + d, parts)) for d in range(1, parts)]
        self.peers = self.mate + self.others

    def barrier(self):
        sem = pltpu.get_barrier_semaphore()
        for peer in self.peers:
            pl.semaphore_signal(sem, inc=1, device_id=peer, device_id_type=MESH)
        pl.semaphore_wait(sem, len(self.peers))

    def copy(self, slot, n, src, dst, peer):
        return pltpu.make_async_remote_copy(
            src_ref=src, dst_ref=dst, send_sem=self.send_sem.at[slot, n],
            recv_sem=self.recv_sem.at[slot, n], device_id=peer, device_id_type=MESH)

    def dims(self, order, stage):
        return [d for d in range(self.bits - 1, -1, -1) if d not in order[:stage]]

    def part(self, c, value):
        mat, col, size, order = self.chunks[c]
        index = tuple(value if d == order[0] else slice(None) for d in self.dims(order, 0))
        return self.mats[mat].at[index + (slice(None), slice(None), pl.ds(col, size))]

    def copies(self, c, stage):
        order = self.chunks[c][3]
        if stage == self.bits:
            return [
                self.copy(c, self.bits + n, self.recv[c][stage - 1].at[peer[1]], self.recv[c][stage].at[n], peer)
                for n, peer in enumerate(self.others)]
        k = order[stage]
        if stage == 0:
            src = self.part(c, 1 - self.bit[k])
        else:
            index = tuple(1 - self.bit[k] if d == k else slice(None) for d in self.dims(order, stage))
            src = self.recv[c][stage - 1].at[index]
        return [self.copy(c, stage, src, self.recv[c][stage], self.mate[k])]

    def start(self, c, stage):
        for copy in self.copies(c, stage):
            copy.start()

    def wait_sends(self, c, stages):
        for stage in range(stages):
            for copy in self.copies(c, stage):
                copy.wait_send()

    def add(self, c, stage):
        mat, col, size, order = self.chunks[c]
        k = order[stage]
        dims = self.dims(order, stage)
        self.copies(c, stage)[0].wait_recv()
        dst = self.recv[c][stage]
        lead = self.bits - 1 - stage

        def one(i, carry):
            part = lax.rem(i, self.parts)
            rest = i // self.parts
            sub = tuple(lax.rem(rest // (1 << (lead - 1 - n)), 2) for n in range(lead))
            at = sub + (part,)
            left = list(sub)
            own_at = tuple(self.bit[k] if d == k else left.pop(0) for d in dims) + (part,)
            if stage > 0:
                own = self.recv[c][stage - 1][own_at]
            elif self.own is None:
                own = self.mats[mat][own_at + (slice(None), pl.ds(col, size))]
            else:
                own = self.own[c][at]
            dst[at] = own + dst[at]
            return carry

        lax.fori_loop(0, self.parts << lead, one, 0)

    def total(self, c):
        total = self.recv[c][self.bits - 1][self.me_s].astype(F32)
        for n, copy in enumerate(self.copies(c, self.bits)):
            copy.wait_recv()
            total = total + self.recv[c][self.bits][n].astype(F32)
        return total


def halving_orders(bits):
    plain = list(range(bits))
    other = [0] + [k for i in range(1, bits, 2) for k in reversed(range(i, min(i + 2, bits)))]
    return plain, other


def halving_scratch(bits, parts, rows, chunks, last):
    scratch = []
    for _, _, size, _ in chunks:
        for stage in range(bits):
            scratch.append(pltpu.VMEM((2,) * (bits - 1 - stage) + (parts, rows, size), BF16))
        if last:
            scratch.append(pltpu.VMEM((parts - 1, rows, size), BF16))
    return scratch


def attend_pair(flag_ref, q_ref, kv_ref, kvp_ref, do_ref, o_ref, dq_ref, dkv_ref, dkvp_ref,
                pt, ds, kvt, qm, dom, midway):
    rows_all = q_ref.shape[0]
    nq = rows_all // QB
    away = (flag_ref[0] - 1).astype(F32) * (-MASKED)
    sources = [(kvp_ref, i) for i in range(nq)] + [(kv_ref, i) for i in range(nq)]

    def block(which, b):
        ref, i = sources[b]
        return ref[which, i * QB:(i + 1) * QB, :]

    for which in range(2):
        kvt[which, :, :rows_all] = kvp_ref[which].T
        kvt[which, :, rows_all:] = kv_ref[which].T
    lane = lax.broadcasted_iota(jnp.int32, (QB, PAIR), 1)
    sub = lax.broadcasted_iota(jnp.int32, (PAIR, QB), 0)
    causal = lax.broadcasted_iota(jnp.int32, (QB, QB), 0) <= lax.broadcasted_iota(
        jnp.int32, (QB, QB), 1)
    for j in range(nq):
        if j == nq // 2:
            midway()
        rows = slice(j * QB, (j + 1) * QB)
        q = q_ref[rows, :] * jnp.asarray(SCALE, BF16)
        qt = q.T
        dot_rows = do_ref[rows, :].astype(F32).T
        blocks = range(nq + j + 1)
        k1 = (nq + j + 1) * QB
        outs, scaled, dqs = [], [], []
        for h in range(2):
            hs = slice(h * HEAD_DIM, (h + 1) * HEAD_DIM)
            qm[h, rows, :] = jnp.where((lane < HEAD_DIM) == (h == 0), q, jnp.zeros_like(q))
            qtm = jnp.where((sub < HEAD_DIM) == (h == 0), qt, jnp.zeros_like(qt))
            scores, tops = [], [None, None]
            for b in blocks:
                s = dot(block(0, b), qtm)
                if b == nq + j:
                    s = jnp.where(causal, s, MASKED)
                scores.append(s)
                part = jnp.max(s.reshape(QB // 8, 8, QB), axis=0)
                side = int(b >= nq)
                tops[side] = part if tops[side] is None else jnp.maximum(tops[side], part)
            top = jnp.max(jnp.maximum(tops[0] + away, tops[1]), axis=0, keepdims=True)
            shift = (top - away, top)
            total = None
            for b, s in zip(blocks, scores):
                p = jnp.exp(s - shift[int(b >= nq)])
                part = jnp.sum(p.reshape(QB // 8, 8, QB), axis=0)
                total = part if total is None else total + part
                pt[h, b * QB:(b + 1) * QB, rows] = p.astype(BF16)
            inv = 1.0 / jnp.sum(total, axis=0, keepdims=True)
            out_t = dot(kvt[1, hs, :k1], pt[h, :k1, rows]) * inv
            dol_t = dot_rows[hs] * inv
            delta = jnp.sum(dol_t * out_t, axis=0, keepdims=True)
            outs.append(out_t)
            scaled.append(dol_t)
            zero = jnp.zeros((HEAD_DIM, QB), BF16)
            dol_b = dol_t.astype(BF16)
            dol_m = jnp.concatenate([dol_b, zero] if h == 0 else [zero, dol_b], axis=0)
            for b in blocks:
                dp = dot(block(1, b), dol_m)
                d = pt[h, b * QB:(b + 1) * QB, rows].astype(F32) * (dp - delta)
                ds[h, b * QB:(b + 1) * QB, rows] = d.astype(BF16)
            dqs.append(dot(kvt[0, hs, :k1], ds[h, :k1, rows]) * SCALE)
        o_ref[rows, :] = jnp.concatenate(outs, 0).T.astype(BF16)
        dq_ref[rows, :] = jnp.concatenate(dqs, 0).T.astype(BF16)
        dol = jnp.concatenate(scaled, 0).T.astype(BF16)
        for h in range(2):
            dom[h, rows, :] = jnp.where((lane < HEAD_DIM) == (h == 0), dol, jnp.zeros_like(dol))
    for b in range(2 * nq):
        q0 = max(0, b - nq) * QB
        br = slice(b * QB, (b + 1) * QB)
        dk = dot(ds[0, br, q0:], qm[0, q0:, :]) + dot(ds[1, br, q0:], qm[1, q0:, :])
        dv = dot(pt[0, br, q0:], dom[0, q0:, :]) + dot(pt[1, br, q0:], dom[1, q0:, :])
        ref, i = (dkvp_ref, b) if b < nq else (dkv_ref, b - nq)
        ref[0, i * QB:(i + 1) * QB, :] = dk.astype(BF16)
        ref[1, i * QB:(i + 1) * QB, :] = dv.astype(BF16)


def attend_kernel(bits, parts, chunks, flag_ref, q_ref, kv_ref, kvp_ref, do_ref, gw_ref, gr_ref,
                  o_ref, dq_ref, dkv_ref, dkvn_ref, partw_ref, partr_ref, *refs):
    nchunk = len(chunks)
    own, refs = refs[:nchunk], refs[nchunk:]
    recv = [refs[c * bits:(c + 1) * bits] for c in range(nchunk)]
    (pt, ds, kvt, qm, dom, back, own_sem, send_sem, recv_sem, back_send, back_recv) = refs[
        nchunk * bits:]
    red = Halving(bits, parts, chunks, (gw_ref, gr_ref), own, recv, send_sem, recv_sem)
    step = pl.program_id(0)
    steps = dkvn_ref.shape[2] // PAIR

    def own_copy(c):
        return pltpu.make_async_copy(red.part(c, red.bit[chunks[c][3][0]]), own[c], own_sem.at[c])

    def back_copy(i):
        cols = pl.ds(pl.multiple_of(i * PAIR, PAIR), PAIR)
        return pltpu.make_async_remote_copy(
            src_ref=back.at[lax.rem(i, 2)], dst_ref=dkvn_ref.at[:, :, cols],
            send_sem=back_send.at[i], recv_sem=back_recv.at[i],
            device_id=red.others[parts - 2], device_id_type=MESH)

    @pl.when(step == 0)
    def _():
        red.barrier()
        for c in range(nchunk):
            red.start(c, 0)
            own_copy(c).start()

    moments = {}
    for c in range(nchunk):
        times = (2, 6, 11) if c < 2 else (2, 8, 13)
        for stage in range(bits):
            at = times[min(stage, 2)] + max(0, stage - 2)
            moments.setdefault(min(at * steps // 8, 2 * steps - 1), []).append((c, stage))

    def advance(half):
        for at, work in moments.items():
            if at % 2 == half:
                @pl.when(step == at // 2)
                def _(work=work):
                    for c, stage in work:
                        if stage == 0:
                            own_copy(c).wait()
                        red.add(c, stage)
                        if stage + 1 < bits:
                            red.start(c, stage + 1)

    first, last = red.me_s == 0, red.me_s == parts - 1
    slot = lax.rem(step, 2)

    @pl.when(jnp.logical_and(step == 0, last))
    def _():
        back[1] = jnp.zeros(back.shape[1:], BF16)
        fills = [pltpu.make_async_copy(back.at[1], dkvn_ref.at[:, :, pl.ds(i * PAIR, PAIR)], back_recv.at[i])
                 for i in range(steps)]
        for fill in fills:
            fill.start()
        for fill in fills:
            fill.wait()

    advance(0)

    @pl.when(jnp.logical_and(step >= 2, jnp.logical_not(first)))
    def _():
        back_copy(step - 2).wait_send()

    attend_pair(flag_ref, q_ref, kv_ref, kvp_ref, do_ref, o_ref, dq_ref, dkv_ref,
                back.at[slot], pt, ds, kvt, qm, dom, lambda: advance(1))

    @pl.when(jnp.logical_not(first))
    def _():
        back_copy(step).start()

    @pl.when(step == steps - 1)
    def _():
        for c in range(nchunk):
            mat, col, size, _ = chunks[c]
            (partw_ref, partr_ref)[mat][:, :, col:col + size] = recv[c][bits - 1][...]
            red.wait_sends(c, bits)

        @pl.when(jnp.logical_not(first))
        def _():
            for i in range(max(0, steps - 2), steps):
                back_copy(i).wait_send()

        @pl.when(jnp.logical_not(last))
        def _():
            for i in range(steps):
                back_copy(i).wait_recv()


def attend(bits, parts, flag, q, kv, kvp, do, gw, gr):
    rows, width = q.shape
    steps = width // PAIR
    hidden = gw.shape[1]
    take = gw.shape[0] // (parts << bits)
    shaped = [g.reshape((2,) * bits + (parts, take, hidden)) for g in (gw, gr)]
    plain, other = halving_orders(bits)
    chunks = [(0, 0, hidden // 2, plain), (1, 0, hidden // 2, other),
              (0, hidden // 2, hidden // 2, plain), (1, hidden // 2, hidden // 2, other)]
    npeer = bits + parts - 1
    tok = pl.BlockSpec((rows, PAIR), lambda i: (0, i))
    kvs = pl.BlockSpec((2, rows, PAIR), lambda i: (0, 0, i))
    hbm = pl.BlockSpec(memory_space=pl.ANY)
    tok_shape = jax.ShapeDtypeStruct((rows, width), BF16)
    kv_shape = jax.ShapeDtypeStruct((2, rows, width), BF16)
    part = (parts, take, hidden)
    return pl.pallas_call(
        partial(attend_kernel, bits, parts, chunks),
        grid=(steps,),
        out_shape=(tok_shape, tok_shape, kv_shape, kv_shape,
                   jax.ShapeDtypeStruct(part, BF16), jax.ShapeDtypeStruct(part, BF16)),
        in_specs=[pl.BlockSpec(memory_space=pltpu.SMEM), tok, kvs, kvs, tok, hbm, hbm],
        out_specs=(tok, tok, kvs, hbm, whole(part), whole(part)),
        scratch_shapes=[
            pltpu.VMEM((2,) * (bits - 1) + (parts, take, size), BF16) for _, _, size, _ in chunks
        ] + halving_scratch(bits, parts, take, chunks, False) + [
            pltpu.VMEM((2, 2 * rows, rows), BF16),
            pltpu.VMEM((2, 2 * rows, rows), BF16),
            pltpu.VMEM((2, PAIR, 2 * rows), BF16),
            pltpu.VMEM((2, rows, PAIR), BF16),
            pltpu.VMEM((2, rows, PAIR), BF16),
            pltpu.VMEM((2, 2, rows, PAIR), BF16),
            pltpu.SemaphoreType.DMA((len(chunks),)),
            pltpu.SemaphoreType.DMA((len(chunks), npeer)),
            pltpu.SemaphoreType.DMA((len(chunks), npeer)),
            pltpu.SemaphoreType.DMA((steps,)),
            pltpu.SemaphoreType.DMA((steps,)),
        ],
        compiler_params=pltpu.CompilerParams(
            vmem_limit_bytes=63 << 20, collective_id=1, has_side_effects=True),
        cost_estimate=cost(60 * rows * rows * width, 20 * rows * width),
        name="attend",
    )(flag, q, kv, kvp, do, *shaped)


def dense_kernel(o_ref, wd_ref, db_ref, rb_ref, mid_ref, x_ref, og_ref, out_ref, dwd_ref, ot):
    @pl.when(pl.program_id(0) == 0)
    def _():
        ot[...] = o_ref[...].T

    total = x_ref[...].astype(F32) + mid_ref[...] + (db_ref[...] + rb_ref[...])
    out_ref[...] = (total + dot(o_ref[...], wd_ref[...])).astype(BF16)
    dwd_ref[...] = dot(ot[...], og_ref[...]).astype(BF16)


def dense(o, wd, db, rb, mid, x, og):
    rows, width = x.shape
    blk = 256
    col = lambda r: pl.BlockSpec((r, blk), lambda i: (0, i))
    return pl.pallas_call(
        dense_kernel,
        grid=(width // blk,),
        out_shape=(jax.ShapeDtypeStruct((rows, width), BF16), jax.ShapeDtypeStruct((width, width), BF16)),
        in_specs=[whole(o.shape), col(width), col(1), col(1), col(rows), col(rows), col(rows)],
        out_specs=(col(rows), col(width)),
        scratch_shapes=[pltpu.VMEM((width, rows), BF16)],
        compiler_params=params(),
        cost_estimate=cost(4 * rows * width * width, 12 * rows * width),
        name="dense",
    )(o, wd, db, rb, mid, x, og)


def tail_kernel(bits, parts, chunks, x_ref, gain_ref, gain2_ref, norm_t, w_ref, ang_ref, dq_ref, dkv_ref,
                dkvn_ref, og_ref, sg_ref, dwd_ref, partw_ref, partr_ref, dog_ref, dbe_ref,
                ig_ref, dw_out, dwd_out, dwe_out, dwr_out, vec_out, *refs):
    nchunk = len(chunks)
    recv = [refs[c * (bits + 1):(c + 1) * (bits + 1)] for c in range(nchunk)]
    (tab, fg, dw, db, dgain, dshift, dgain2, dshift2, zw, zr, state, vrecv, send_sem, recv_sem) = refs[
        nchunk * (bits + 1):]
    red = Halving(bits, parts, chunks, (dw, dwd_ref), None, recv, send_sem, recv_sem)
    step = pl.program_id(0)
    steps = pl.num_programs(0)
    width = x_ref.shape[1]
    nstep = width // (STEP_PAIRS * PAIR)
    cols = 3 * STEP_PAIRS * PAIR

    def forward(c, stage):
        red.add(c, stage)
        red.start(c, stage + 1)

    def z_copies():
        return [red.copy(nchunk + 1 + m, bits + n, part.at[peer[1]], dst.at[n], peer)
                for m, (part, dst) in enumerate(((partw_ref, zw), (partr_ref, zr)))
                for n, peer in enumerate(red.others)]

    @pl.when(step == 0)
    def _():
        red.barrier()
        for copy in z_copies():
            copy.start()
        for c in range(nstep, nchunk):
            red.start(c, 0)
        build_tables(ang_ref, tab)
        fg[...] = jnp.zeros_like(fg)

    for c in range(1, nstep):
        @pl.when(step == c)
        def _(c=c):
            red.start(c - 1, 0)
            if c == 1:
                for extra in range(nstep, nchunk):
                    forward(extra, 0)
            else:
                forward(c - 2, 0)

    blocks = []
    for n in range(STEP_PAIRS):
        mine = slice(n * PAIR, (n + 1) * PAIR)
        dq = turn(dq_ref[:, mine].astype(F32), tab, -1.0)
        dk = turn(dkv_ref[0, :, mine].astype(F32) + dkvn_ref[0, :, mine].astype(F32), tab, -1.0)
        dv = dkv_ref[1, :, mine].astype(F32) + dkvn_ref[1, :, mine].astype(F32)
        low = low_lanes(dq.shape)
        dk = pltpu.roll(dk, HEAD_DIM, 1)
        blocks += [jnp.where(low, dq, dk), jnp.where(low, dv, dq), jnp.where(low, dk, dv)]
    dm = jnp.concatenate(blocks, axis=1).astype(BF16)
    at = pl.ds(pl.multiple_of(step * cols, cols), cols)
    db[:, at] = jnp.sum(dm.astype(F32), axis=0, keepdims=True)
    dw[(slice(None),) * (bits + 2) + (at,)] = dot(norm_t[...], dm).reshape(
        dw.shape[:-1] + (cols,)).astype(BF16)
    fg[...] += dot_t(dm, w_ref[...])

    def vec_copies(stage):
        if stage < bits:
            return [red.copy(nchunk, stage, state.at[stage], vrecv.at[stage], red.mate[stage])]
        return [red.copy(nchunk, bits + n, state.at[bits], vrecv.at[bits + n], peer)
                for n, peer in enumerate(red.others)]

    def vec_start(stage):
        for copy in vec_copies(stage):
            copy.start()

    def vec_add(stage):
        copies = vec_copies(stage)
        for copy in copies:
            copy.wait_recv()
        total = state[stage]
        for n in range(len(copies)):
            total = total + vrecv[stage + n]
        if stage < bits:
            state[stage + 1] = total
            vec_start(stage + 1)
        else:
            vec_out[...] = total

    @pl.when(step == steps - 1)
    def _():
        red.start(nstep - 1, 0)
        forward(nstep - 2, 0)

        def emit(rows, part):
            ig_ref[rows, :] = (og_ref[rows, :].astype(F32) + part).astype(BF16)

        forward(nstep - 1, 0)
        norm_back(x_ref, (gain_ref, gain2_ref), (fg, sg_ref), (dgain, dgain2), (dshift, dshift2), emit)
        begin = 0
        for ref in (dgain, dshift, db, dog_ref, dgain2, dshift2, dbe_ref):
            state[0, :, begin:begin + ref.shape[1]] = ref[...]
            begin += ref.shape[1]
        vec_start(0)
        order = list(range(nstep, nchunk)) + list(range(nstep))
        for stage in range(1, bits):
            for c in order:
                forward(c, stage)
            vec_add(stage - 1)
        copies = z_copies()
        for m, (part, got, out) in enumerate(((partw_ref, zw, dwe_out), (partr_ref, zr, dwr_out))):
            total = part[red.me_s].astype(F32)
            for n in range(parts - 1):
                copies[m * (parts - 1) + n].wait_recv()
                total = total + got[n].astype(F32)
            if m == 0:
                out[...] = total
            else:
                take = total.shape[0]
                for j in range(total.shape[1] // width):
                    out[j * take:(j + 1) * take, :] = total[:, j * width:(j + 1) * width]
        vec_add(bits - 1)
        for c in order:
            mat, col, size, _ = chunks[c]
            (dw_out, dwd_out)[mat][:, col:col + size] = red.total(c)
        vec_add(bits)
        for c in range(nchunk):
            red.wait_sends(c, bits + 1)
        for copy in copies:
            copy.wait_send()
        for stage in range(bits + 1):
            for copy in vec_copies(stage):
                copy.wait_send()


def tail(bits, parts, x, gain, gain2, norm_t, w, ang, dq, dkv, dkvn, og, sg, dwd, partw, partr, dog, dbe):
    rows, width = x.shape
    full, vec = whole((rows, width)), whole((1, width))
    wide = STEP_PAIRS * PAIR
    cols = 3 * wide
    nstep = width // wide
    hidden = dbe.shape[1]
    take = width // (parts << bits)
    total = 5 * width + 3 * width + hidden
    npeer = bits + parts - 1
    lead = (2,) * bits + (parts, take)
    plain, other = halving_orders(bits)
    chunks = [(0, n * cols, cols, other if n % 2 else plain) for n in range(nstep)]
    chunks += [(1, n * (width // 2), width // 2, other if n % 2 else plain) for n in range(2)]
    tok = pl.BlockSpec((rows, wide), lambda i: (0, i))
    kvs = pl.BlockSpec((2, rows, wide), lambda i: (0, 0, i))
    up = pl.BlockSpec((width, cols), lambda i: (0, i))
    dwd = dwd.reshape(lead + (width,))
    outs = [((rows, width), BF16), ((take, 3 * width), F32), ((take, width), F32), ((take, hidden), F32),
            ((take * (hidden // width), width), F32), ((1, total), F32)]
    row_vec = pltpu.VMEM((1, width), F32)
    nsem = (len(chunks) + 3, npeer)
    return pl.pallas_call(
        partial(tail_kernel, bits, parts, chunks),
        grid=(nstep,),
        out_shape=tuple(jax.ShapeDtypeStruct(s, d) for s, d in outs),
        in_specs=[full, vec, vec, whole(norm_t.shape), up, whole(ang.shape), tok, kvs, kvs, full, full,
                  whole(dwd.shape), whole(partw.shape), whole(partr.shape), vec, whole(dbe.shape)],
        out_specs=tuple(whole(s) for s, _ in outs),
        scratch_shapes=halving_scratch(bits, parts, take, chunks, True) + [
            pltpu.VMEM((3, rows, PAIR), F32), pltpu.VMEM((rows, width), F32),
            pltpu.VMEM(lead + (3 * width,), BF16), pltpu.VMEM((1, 3 * width), F32),
            row_vec, row_vec, row_vec, row_vec,
            pltpu.VMEM((parts - 1, take, hidden), BF16), pltpu.VMEM((parts - 1, take, hidden), BF16),
            pltpu.VMEM((bits + 1, 1, total), F32), pltpu.VMEM((npeer, 1, total), F32),
            pltpu.SemaphoreType.DMA(nsem), pltpu.SemaphoreType.DMA(nsem),
        ],
        compiler_params=pltpu.CompilerParams(
            vmem_limit_bytes=63 << 20, collective_id=0, has_side_effects=True),
        cost_estimate=cost(12 * rows * width * width, 8 * rows * width),
        name="tail",
    )(x, gain, gain2, norm_t, w, ang, dq, dkv, dkvn, og, sg, dwd, partw, partr, dog, dbe)


def finish_kernel(sizes, index_ref, ig_ref, dw_ref, dwd_ref, dwe_ref, dwr_ref, vec_ref,
                  ig_out, dw_out, dwd_out, dwe_out, dwr_out, *outs):
    for src, dst in ((ig_ref, ig_out), (dw_ref, dw_out), (dwd_ref, dwd_out), (dwe_ref, dwe_out),
                     (dwr_ref, dwr_out)):
        dst[...] = src[...]

    @pl.when(pl.program_id(0) == 0)
    def _():
        at = 0
        for size, out in zip(sizes, outs):
            own = out.shape[1]
            row = jnp.broadcast_to(vec_ref[:, at:at + size], (8, size))
            out[...] = pltpu.roll(row, lax.rem(size - index_ref[0] * own, size), 1)[:1, :own]
            at += size


def finish(index, ndev, sizes, ig, dw, dwd, dwe, dwr, vec):
    mats = (ig, dw, dwd, dwe, dwr)
    return pl.pallas_call(
        partial(finish_kernel, sizes),
        out_shape=tuple(jax.ShapeDtypeStruct(m.shape, m.dtype) for m in mats)
        + tuple(jax.ShapeDtypeStruct((1, n // ndev), F32) for n in sizes),
        grid=(1,),
        in_specs=[pl.BlockSpec(memory_space=pltpu.SMEM)] + [whole(m.shape) for m in mats] + [whole(vec.shape)],
        out_specs=tuple([whole(m.shape) for m in mats] + [whole((1, n // ndev)) for n in sizes]),
        compiler_params=params(),
        name="finish",
    )(index, *mats, vec)


def body(
    tokens,
    seq_lengths,
    attn_gain,
    attn_shift,
    qkv_weight,
    qkv_bias,
    dense_weight,
    dense_bias,
    mlp_gain,
    mlp_shift,
    expand_weight,
    expand_bias,
    reduce_weight,
    reduce_bias,
    out_grad,
):
    seq_parts = lax.axis_size("seq")
    place = lax.axis_index("seq")
    rows, width = tokens.shape
    lengths = seq_lengths[0]
    starts = jnp.cumsum(lengths) - lengths
    row0 = place * rows
    offset = row0 - jnp.max(jnp.where(starts <= row0, starts, 0))
    flag = (offset > 0).astype(jnp.int32).reshape(1)
    positions = (offset + jnp.arange(rows, dtype=jnp.int32)).astype(F32)
    frequency = jnp.exp(jnp.arange(ROT // 2, dtype=F32) * (-2.0 * math.log(10000.0) / ROT))
    phases = frequency[:, None] * positions[None, :]
    ang = jnp.concatenate([jnp.cos(phases), jnp.sin(phases)], axis=0)

    row = lambda v: v.reshape(1, -1)
    ag, ash, mg, msh = row(attn_gain), row(attn_shift), row(mlp_gain), row(mlp_shift)
    onward = [(i, i + 1) for i in range(seq_parts - 1)]

    batch_parts = lax.axis_size("batch")
    ndev = batch_parts * seq_parts
    bits = batch_parts.bit_length() - 1
    q, kv, do, n1t, n2, n2t = project(
        tokens, ag, ash, mg, msh, qkv_weight, row(qkv_bias), ang, out_grad, dense_weight)
    kvp = lax.ppermute(kv, "seq", onward)
    mid, slope, dwr, dog = mlp_fwd(
        ndev, n2, expand_weight, row(expand_bias), reduce_weight, out_grad)
    sg, dwe, dbe = mlp_back(n2t, expand_weight, reduce_weight, out_grad, slope)

    o, dq, dkv, dkvn, partw, partr = attend(bits, seq_parts, flag, q, kv, kvp, do, dwe, dwr)
    layer_out, dwd = dense(o, dense_weight, row(dense_bias), row(reduce_bias), mid, tokens, out_grad)
    input_grad, dw, dwd, dwe, dwr, vsum = tail(
        bits, seq_parts, tokens, ag, mg, n1t, qkv_weight, ang, dq, dkv, dkvn, out_grad, sg, dwd,
        partw, partr, dog, dbe)
    index = lax.axis_index("batch") * seq_parts + place
    sizes = (width, width, 3 * width, width, width, width, dbe.shape[1])
    input_grad, dw, dwd, dwe, dwr, *vectors = finish(
        index.astype(jnp.int32).reshape(1), ndev, sizes, input_grad, dw, dwd, dwe, dwr, vsum)
    dag, das, dqb, dog, dmg, dms, dbe = [v.reshape(-1) for v in vectors]
    return (
        layer_out,
        input_grad,
        dag,
        das,
        dw,
        dqb,
        dwd,
        dog,
        dmg,
        dms,
        dwe,
        dbe,
        dwr,
        dog,
    )


def solution(mesh):
    tok = P(("batch", "seq"), None)
    vec = P(("batch", "seq"))
    in_specs = (tok, P("batch", None)) + (P(),) * 12 + (tok,)
    out_specs = (tok, tok, vec, vec, tok, vec, tok, vec, vec, vec, tok, vec, tok, vec)
    return jax.shard_map(body, mesh=mesh, in_specs=in_specs, out_specs=out_specs, check_vma=False)
```

```python
from functools import partial
import math

import jax
import jax.numpy as jnp
from jax import lax
from jax.experimental import pallas as pl
from jax.experimental.pallas import tpu as pltpu
from jax.sharding import PartitionSpec as P

HEAD_DIM = 64
ROT = 16
PAIR = 2 * HEAD_DIM
EPSILON = 1e-05
MASKED = -1e30
SCALE = 1.0 / math.sqrt(HEAD_DIM)
QB = 256
FB = 1024
STEP_PAIRS = 2
ROWS = 128
F32 = jnp.float32
BF16 = jnp.bfloat16
VMEM_LIMIT = 60 << 20
MESH = pl.DeviceIdType.MESH


def dot(left, right):
    return jnp.dot(left, right, preferred_element_type=F32)


def dot_t(left, right):
    return lax.dot_general(left, right, (((1,), (1,)), ((), ())), preferred_element_type=F32)


def params():
    return pltpu.CompilerParams(vmem_limit_bytes=VMEM_LIMIT)


def cost(flops, nbytes):
    return pl.CostEstimate(flops=int(flops), bytes_accessed=int(nbytes), transcendentals=0)


def whole(shape):
    return pl.BlockSpec(shape, lambda i: (0,) * len(shape), pipeline_mode=pl.Buffered(1))


def statistics(x):
    mean = jnp.mean(x, axis=-1, keepdims=True)
    centered = x - mean
    variance = jnp.mean(centered * centered, axis=-1, keepdims=True)
    rstd = lax.rsqrt(variance + EPSILON)
    return centered * rstd, rstd


def row_block(i):
    return pl.ds(pl.multiple_of(i * ROWS, ROWS), ROWS)


def norm_rows(x_ref, gains, outs):
    def step(i, carry):
        rows = row_block(i)
        xn, _ = statistics(x_ref[rows, :].astype(F32))
        for (gain_ref, shift_ref), out_ref in zip(gains, outs):
            out_ref[rows, :] = (xn * gain_ref[...] + shift_ref[...]).astype(BF16)
        return carry

    lax.fori_loop(0, x_ref.shape[0] // ROWS, step, 0)


def norm_back(x_ref, gains, grads, gain_grads, shift_grads, emit, begin, end):
    if begin == 0:
        for ref in gain_grads + shift_grads:
            ref[...] = jnp.zeros_like(ref)

    def step(i, carry):
        rows = row_block(i)
        xn, rstd = statistics(x_ref[rows, :].astype(F32))
        scaled = 0.0
        for gain_ref, grad_ref, dgain_ref, dshift_ref in zip(gains, grads, gain_grads, shift_grads):
            grad = grad_ref[rows, :]
            dgain_ref[...] += jnp.sum(grad * xn, axis=0, keepdims=True)
            dshift_ref[...] += jnp.sum(grad, axis=0, keepdims=True)
            scaled = scaled + grad * gain_ref[...]
        mean_s = jnp.mean(scaled, axis=-1, keepdims=True)
        mean_sx = jnp.mean(scaled * xn, axis=-1, keepdims=True)
        emit(rows, rstd * (scaled - mean_s - xn * mean_sx))
        return carry

    lax.fori_loop(begin, end, step, 0)


def build_tables(angle_ref, tab_ref):
    half = ROT // 2
    cos8, sin8 = angle_ref[0:half, :], angle_ref[half:ROT, :]
    rest = HEAD_DIM - ROT
    count = cos8.shape[1]
    ones = jnp.ones((rest, count), F32)
    zeros = jnp.zeros((rest, count), F32)
    z8 = jnp.zeros_like(sin8)
    tab_ref[0] = jnp.concatenate([cos8, cos8, ones] * 2, axis=0).T
    tab_ref[1] = jnp.concatenate([-sin8, z8, zeros] * 2, axis=0).T
    tab_ref[2] = jnp.concatenate([z8, sin8, zeros] * 2, axis=0).T


def turn(u, tab_ref, sign):
    half = ROT // 2
    ahead = pltpu.roll(u, PAIR - half, 1)
    behind = pltpu.roll(u, half, 1)
    return u * tab_ref[0] + sign * (ahead * tab_ref[1] + behind * tab_ref[2])


def low_lanes(shape):
    return lax.broadcasted_iota(jnp.int32, shape, 1) < HEAD_DIM


def project_kernel(x_ref, gain_ref, shift_ref, gain2_ref, shift2_ref, w_ref, b_ref, ang_ref, og_ref,
                   wd_ref, q_ref, kv_ref, do_ref, n1t_ref, n2_ref, n2t_ref,
                   norm, n1t, n2, n2t, tab, sem):
    saves = [pltpu.make_async_copy(src, dst, sem.at[n]) for n, (src, dst) in enumerate(
        ((n1t, n1t_ref), (n2, n2_ref), (n2t, n2t_ref)))]

    @pl.when(pl.program_id(0) == 0)
    def _():
        norm_rows(x_ref, ((gain_ref, shift_ref), (gain2_ref, shift2_ref)), (norm, n2))
        saves[1].start()
        n1t[...] = norm[...].T
        saves[0].start()
        n2t[...] = n2[...].T
        saves[2].start()
        build_tables(ang_ref, tab)

    for n in range(STEP_PAIRS):
        cols = slice(n * 3 * PAIR, (n + 1) * 3 * PAIR)
        mine = slice(n * PAIR, (n + 1) * PAIR)
        mixed = dot(norm[...], w_ref[:, cols]) + b_ref[:, cols]
        t0, t1, t2 = mixed[:, :PAIR], mixed[:, PAIR:2 * PAIR], mixed[:, 2 * PAIR:]
        low = low_lanes(t0.shape)
        q = jnp.where(low, t0, t1)
        k = pltpu.roll(jnp.where(low, t2, t0), HEAD_DIM, 1)
        v = jnp.where(low, t1, t2)
        q_ref[:, mine] = turn(q, tab, 1.0).astype(BF16)
        kv_ref[0, :, mine] = turn(k, tab, 1.0).astype(BF16)
        kv_ref[1, :, mine] = v.astype(BF16)
    do_ref[...] = dot_t(og_ref[...], wd_ref[...]).astype(BF16)

    @pl.when(pl.program_id(0) == pl.num_programs(0) - 1)
    def _():
        for save in saves:
            save.wait()


def project(x, gain, shift, gain2, shift2, w, b, ang, og, wd):
    rows, width = x.shape
    wide = STEP_PAIRS * PAIR
    tok = pl.BlockSpec((rows, wide), lambda i: (0, i))
    return pl.pallas_call(
        project_kernel,
        grid=(width // wide,),
        out_shape=(
            jax.ShapeDtypeStruct((rows, width), BF16),
            jax.ShapeDtypeStruct((2, rows, width), BF16),
            jax.ShapeDtypeStruct((rows, width), BF16),
            jax.ShapeDtypeStruct((width, rows), BF16),
            jax.ShapeDtypeStruct((rows, width), BF16),
            jax.ShapeDtypeStruct((width, rows), BF16),
        ),
        in_specs=[
            whole((rows, width)), *[whole((1, width))] * 4,
            pl.BlockSpec((width, 3 * wide), lambda i: (0, i)),
            pl.BlockSpec((1, 3 * wide), lambda i: (0, i)),
            whole(ang.shape), whole((rows, width)),
            pl.BlockSpec((wide, width), lambda i: (i, 0)),
        ],
        out_specs=(tok, pl.BlockSpec((2, rows, wide), lambda i: (0, 0, i)), tok,
                   *[pl.BlockSpec(memory_space=pl.ANY)] * 3),
        scratch_shapes=[pltpu.VMEM((rows, width), BF16), pltpu.VMEM((width, rows), BF16),
                        pltpu.VMEM((rows, width), BF16), pltpu.VMEM((width, rows), BF16),
                        pltpu.VMEM((3, rows, PAIR), F32), pltpu.SemaphoreType.DMA((3,))],
        compiler_params=params(),
        cost_estimate=cost(8 * rows * width * width, 24 * rows * width),
        name="project",
    )(x, gain, shift, gain2, shift2, w, b, ang, og, wd)


def gelu_parts(h):
    z = jnp.abs(h) * math.sqrt(0.5)
    t = 1.0 / (1.0 + 0.5 * z)
    poly = jnp.full_like(t, 0.17087277)
    for c in (-0.82215223, 1.48851587, -1.13520398, 0.27886807, -0.18628806, 0.09678418,
              0.37409196, 1.00002368, -1.26551223):
        poly = poly * t + c
    zz = z * z
    tail = 0.5 * t * jnp.exp(poly - zz)
    cdf = jnp.where(h >= 0, 1.0 - tail, tail)
    slope = cdf + h * (jnp.exp(-zz) * (1.0 / math.sqrt(2.0 * math.pi)))
    return h * cdf, slope


def mlp_kernel(take, parts, n2_ref, n2t_ref, we_ref, be_ref, wr_ref, og_ref, kv_ref,
               mid_ref, dwr_ref, dog_ref, sg_ref, dwe_ref, dbe_ref, kvp_ref, slope, send_sem, recv_sem, fill_sem):
    step = pl.program_id(0)
    blocks = pl.num_programs(0) // 2
    width = n2_ref.shape[1]
    me_b, me_s = lax.axis_index("batch"), lax.axis_index("seq")
    first, last = me_s == 0, me_s == parts - 1
    onward = pltpu.make_async_remote_copy(
        src_ref=kv_ref, dst_ref=kvp_ref, send_sem=send_sem, recv_sem=recv_sem,
        device_id=(me_b, lax.rem(me_s + 1, parts)), device_id_type=MESH)

    @pl.when(step == 0)
    def _():
        sem = pltpu.get_barrier_semaphore()
        for d in range(1, parts):
            pl.semaphore_signal(sem, inc=1, device_id=(me_b, lax.rem(me_s + d, parts)), device_id_type=MESH)
        pl.semaphore_wait(sem, parts - 1)

        @pl.when(jnp.logical_not(last))
        def _():
            onward.start()

        @pl.when(first)
        def _():
            slope[0] = jnp.zeros(slope.shape[1:], BF16)
            fills = [pltpu.make_async_copy(slope.at[0, :, :width], kvp_ref.at[n], fill_sem.at[n]) for n in range(2)]
            for fill in fills:
                fill.start()
            for fill in fills:
                fill.wait()

        mid_ref[...] = jnp.zeros_like(mid_ref)
        sg_ref[...] = jnp.zeros_like(sg_ref)
        dog_ref[...] = jnp.sum(og_ref[...].astype(F32), axis=0, keepdims=True)

    @pl.when(step < blocks)
    def _():
        h = dot(n2_ref[...], we_ref[...]) + be_ref[...]
        active, bend = gelu_parts(h)
        active = active.astype(BF16)
        slope[step] = bend.astype(BF16)
        mid_ref[...] += dot(active, wr_ref[...])
        dwr = dot(active.T, og_ref[...]).astype(BF16)
        ratio = dwr_ref.shape[1] // width
        for piece in range(FB // take):
            group, j = piece // ratio, piece % ratio
            dwr_ref[group * take:(group + 1) * take, j * width:(j + 1) * width] = (
                dwr[piece * take:(piece + 1) * take, :])

    @pl.when(step >= blocks)
    def _():
        hidden = (dot_t(og_ref[...], wr_ref[...]) * slope[step - blocks].astype(F32)).astype(BF16)
        dwe_ref[...] = dot(n2t_ref[...], hidden).astype(BF16)
        dbe_ref[...] = jnp.sum(hidden.astype(F32), axis=0, keepdims=True)
        sg_ref[...] += dot_t(hidden, we_ref[...])

    @pl.when(step == 2 * blocks - 1)
    def _():
        @pl.when(jnp.logical_not(last))
        def _():
            onward.wait_send()

        @pl.when(jnp.logical_not(first))
        def _():
            onward.wait_recv()


def mlp(ndev, parts, n2, n2t, we, be, wr, og, kv):
    rows, width = n2.shape
    hidden = we.shape[1]
    blocks = hidden // FB
    full, vec = whole((rows, width)), whole((1, width))
    gate = FB * width // hidden
    fshape, hbm = jax.ShapeDtypeStruct((rows, width), F32), pl.BlockSpec(memory_space=pl.ANY)
    early = lambda i: jnp.minimum(i, blocks - 1)
    late = lambda i: jnp.maximum(i - blocks, 0)
    return pl.pallas_call(
        partial(mlp_kernel, width // ndev, parts),
        grid=(2 * blocks,),
        out_shape=(fshape, jax.ShapeDtypeStruct((width, hidden), BF16), jax.ShapeDtypeStruct((1, width), F32),
                   fshape, jax.ShapeDtypeStruct((width, hidden), BF16), jax.ShapeDtypeStruct((1, hidden), F32),
                   jax.ShapeDtypeStruct(kv.shape, BF16)),
        in_specs=[full, whole(n2t.shape),
                  pl.BlockSpec((width, FB), lambda i: (0, lax.rem(i, blocks))),
                  pl.BlockSpec((1, FB), lambda i: (0, early(i))),
                  pl.BlockSpec((FB, width), lambda i: (lax.rem(i, blocks), 0)),
                  full, hbm],
        out_specs=(full, pl.BlockSpec((gate, hidden), lambda i: (early(i), 0)), vec, full,
                   pl.BlockSpec((width, FB), lambda i: (0, late(i))),
                   pl.BlockSpec((1, FB), lambda i: (0, late(i))), hbm),
        scratch_shapes=[pltpu.VMEM((blocks, rows, FB), BF16), pltpu.SemaphoreType.DMA,
                        pltpu.SemaphoreType.DMA, pltpu.SemaphoreType.DMA((2,))],
        compiler_params=pltpu.CompilerParams(
            vmem_limit_bytes=63 << 20, collective_id=2, has_side_effects=True),
        cost_estimate=cost(12 * rows * width * hidden, 8 * width * hidden),
        name="mlp",
    )(n2, n2t, we, be, wr, og, kv)


class Halving:
    def __init__(self, bits, parts, chunks, mats, own, recv, send_sem, recv_sem):
        self.bits, self.parts, self.chunks = bits, parts, chunks
        self.mats, self.own, self.recv = mats, own, recv
        self.send_sem, self.recv_sem = send_sem, recv_sem
        self.me_b, self.me_s = lax.axis_index("batch"), lax.axis_index("seq")
        self.bit = [lax.rem(self.me_b // (1 << k), 2) for k in range(bits)]
        self.mate = [
            (self.me_b + (1 << k) - 2 * (1 << k) * self.bit[k], self.me_s) for k in range(bits)]
        self.others = [(self.me_b, lax.rem(self.me_s + d, parts)) for d in range(1, parts)]
        self.peers = self.mate + self.others

    def barrier(self):
        sem = pltpu.get_barrier_semaphore()
        for peer in self.peers:
            pl.semaphore_signal(sem, inc=1, device_id=peer, device_id_type=MESH)
        pl.semaphore_wait(sem, len(self.peers))

    def copy(self, slot, n, src, dst, peer):
        return pltpu.make_async_remote_copy(
            src_ref=src, dst_ref=dst, send_sem=self.send_sem.at[slot, n],
            recv_sem=self.recv_sem.at[slot, n], device_id=peer, device_id_type=MESH)

    def dims(self, order, stage):
        return [d for d in range(self.bits - 1, -1, -1) if d not in order[:stage]]

    def part(self, c, value):
        mat, col, size, order = self.chunks[c]
        index = tuple(value if d == order[0] else slice(None) for d in self.dims(order, 0))
        return self.mats[mat].at[index + (slice(None), slice(None), pl.ds(col, size))]

    def copies(self, c, stage):
        order = self.chunks[c][3]
        if stage == self.bits:
            return [
                self.copy(c, self.bits + n, self.recv[c][stage - 1].at[peer[1]], self.recv[c][stage].at[n], peer)
                for n, peer in enumerate(self.others)]
        k = order[stage]
        if stage == 0:
            src = self.part(c, 1 - self.bit[k])
        else:
            index = tuple(1 - self.bit[k] if d == k else slice(None) for d in self.dims(order, stage))
            src = self.recv[c][stage - 1].at[index]
        return [self.copy(c, stage, src, self.recv[c][stage], self.mate[k])]

    def start(self, c, stage):
        for copy in self.copies(c, stage):
            copy.start()

    def wait_sends(self, c, stages):
        for stage in range(stages):
            for copy in self.copies(c, stage):
                copy.wait_send()

    def add(self, c, stage):
        mat, col, size, order = self.chunks[c]
        k = order[stage]
        dims = self.dims(order, stage)
        self.copies(c, stage)[0].wait_recv()
        dst = self.recv[c][stage]
        lead = self.bits - 1 - stage

        def one(i, carry):
            part = lax.rem(i, self.parts)
            rest = i // self.parts
            sub = tuple(lax.rem(rest // (1 << (lead - 1 - n)), 2) for n in range(lead))
            at = sub + (part,)
            left = list(sub)
            own_at = tuple(self.bit[k] if d == k else left.pop(0) for d in dims) + (part,)
            if stage > 0:
                own = self.recv[c][stage - 1][own_at]
            elif self.own is None:
                own = self.mats[mat][own_at + (slice(None), pl.ds(col, size))]
            else:
                own = self.own[c][at]
            dst[at] = own + dst[at]
            return carry

        lax.fori_loop(0, self.parts << lead, one, 0)

    def total(self, c):
        total = self.recv[c][self.bits - 1][self.me_s].astype(F32)
        for n, copy in enumerate(self.copies(c, self.bits)):
            copy.wait_recv()
            total = total + self.recv[c][self.bits][n].astype(F32)
        return total


def halving_orders(bits):
    plain = list(range(bits))
    other = [0] + [k for i in range(1, bits, 2) for k in reversed(range(i, min(i + 2, bits)))]
    return plain, other


def halving_scratch(bits, parts, rows, chunks, last):
    scratch = []
    for _, _, size, _ in chunks:
        for stage in range(bits):
            scratch.append(pltpu.VMEM((2,) * (bits - 1 - stage) + (parts, rows, size), BF16))
        if last:
            scratch.append(pltpu.VMEM((parts - 1, rows, size), BF16))
    return scratch


def attend_pair(flag_ref, q_ref, kv_ref, kvp_ref, do_ref, o_ref, dq_ref, dkv_ref, dkvp_ref,
                pt, ds, kvt, qm, dom, midway):
    rows_all = q_ref.shape[0]
    nq = rows_all // QB
    away = (flag_ref[0] - 1).astype(F32) * (-MASKED)
    sources = [(kvp_ref, i) for i in range(nq)] + [(kv_ref, i) for i in range(nq)]

    def block(which, b):
        ref, i = sources[b]
        return ref[which, i * QB:(i + 1) * QB, :]

    for which in range(2):
        kvt[which, :, :rows_all] = kvp_ref[which].T
        kvt[which, :, rows_all:] = kv_ref[which].T
    lane = lax.broadcasted_iota(jnp.int32, (QB, PAIR), 1)
    sub = lax.broadcasted_iota(jnp.int32, (PAIR, QB), 0)
    causal = lax.broadcasted_iota(jnp.int32, (QB, QB), 0) <= lax.broadcasted_iota(
        jnp.int32, (QB, QB), 1)
    for j in range(nq):
        if j == nq // 2:
            midway()
        rows = slice(j * QB, (j + 1) * QB)
        q = q_ref[rows, :] * jnp.asarray(SCALE, BF16)
        qt = q.T
        dot_rows = do_ref[rows, :].astype(F32).T
        blocks = range(nq + j + 1)
        k1 = (nq + j + 1) * QB
        outs, scaled, dqs = [], [], []
        for h in range(2):
            hs = slice(h * HEAD_DIM, (h + 1) * HEAD_DIM)
            qm[h, rows, :] = jnp.where((lane < HEAD_DIM) == (h == 0), q, jnp.zeros_like(q))
            qtm = jnp.where((sub < HEAD_DIM) == (h == 0), qt, jnp.zeros_like(qt))
            scores, tops = [], [None, None]
            for b in blocks:
                s = dot(block(0, b), qtm)
                if b == nq + j:
                    s = jnp.where(causal, s, MASKED)
                scores.append(s)
                part = jnp.max(s.reshape(QB // 8, 8, QB), axis=0)
                side = int(b >= nq)
                tops[side] = part if tops[side] is None else jnp.maximum(tops[side], part)
            top = jnp.max(jnp.maximum(tops[0] + away, tops[1]), axis=0, keepdims=True)
            shift = (top - away, top)
            total = None
            for b, s in zip(blocks, scores):
                p = jnp.exp(s - shift[int(b >= nq)])
                part = jnp.sum(p.reshape(QB // 8, 8, QB), axis=0)
                total = part if total is None else total + part
                pt[h, b * QB:(b + 1) * QB, rows] = p.astype(BF16)
            inv = 1.0 / jnp.sum(total, axis=0, keepdims=True)
            out_t = dot(kvt[1, hs, :k1], pt[h, :k1, rows]) * inv
            dol_t = dot_rows[hs] * inv
            delta = jnp.sum(dol_t * out_t, axis=0, keepdims=True)
            outs.append(out_t)
            scaled.append(dol_t)
            zero = jnp.zeros((HEAD_DIM, QB), BF16)
            dol_b = dol_t.astype(BF16)
            dol_m = jnp.concatenate([dol_b, zero] if h == 0 else [zero, dol_b], axis=0)
            for b in blocks:
                dp = dot(block(1, b), dol_m)
                d = pt[h, b * QB:(b + 1) * QB, rows].astype(F32) * (dp - delta)
                ds[h, b * QB:(b + 1) * QB, rows] = d.astype(BF16)
            dqs.append(dot(kvt[0, hs, :k1], ds[h, :k1, rows]) * SCALE)
        o_ref[rows, :] = jnp.concatenate(outs, 0).T.astype(BF16)
        dq_ref[rows, :] = jnp.concatenate(dqs, 0).T.astype(BF16)
        dol = jnp.concatenate(scaled, 0).T.astype(BF16)
        for h in range(2):
            dom[h, rows, :] = jnp.where((lane < HEAD_DIM) == (h == 0), dol, jnp.zeros_like(dol))
    for b in range(2 * nq):
        q0 = max(0, b - nq) * QB
        br = slice(b * QB, (b + 1) * QB)
        dk = dot(ds[0, br, q0:], qm[0, q0:, :]) + dot(ds[1, br, q0:], qm[1, q0:, :])
        dv = dot(pt[0, br, q0:], dom[0, q0:, :]) + dot(pt[1, br, q0:], dom[1, q0:, :])
        ref, i = (dkvp_ref, b) if b < nq else (dkv_ref, b - nq)
        ref[0, i * QB:(i + 1) * QB, :] = dk.astype(BF16)
        ref[1, i * QB:(i + 1) * QB, :] = dv.astype(BF16)


def attend_kernel(bits, parts, chunks, flag_ref, q_ref, kv_ref, kvp_ref, do_ref, gw_ref, gr_ref,
                  o_ref, dq_ref, dkv_ref, dkvn_ref, partw_ref, partr_ref, *refs):
    nchunk = len(chunks)
    own, refs = refs[:nchunk], refs[nchunk:]
    recv = [refs[c * bits:(c + 1) * bits] for c in range(nchunk)]
    (pt, ds, kvt, qm, dom, back, own_sem, send_sem, recv_sem, back_send, back_recv) = refs[
        nchunk * bits:]
    red = Halving(bits, parts, chunks, (gw_ref, gr_ref), own, recv, send_sem, recv_sem)
    step = pl.program_id(0)
    steps = dkvn_ref.shape[2] // PAIR

    def own_copy(c):
        return pltpu.make_async_copy(red.part(c, red.bit[chunks[c][3][0]]), own[c], own_sem.at[c])

    def back_copy(i):
        cols = pl.ds(pl.multiple_of(i * PAIR, PAIR), PAIR)
        return pltpu.make_async_remote_copy(
            src_ref=back.at[lax.rem(i, 2)], dst_ref=dkvn_ref.at[:, :, cols],
            send_sem=back_send.at[i], recv_sem=back_recv.at[i],
            device_id=red.others[parts - 2], device_id_type=MESH)

    @pl.when(step == 0)
    def _():
        red.barrier()
        for c in range(nchunk):
            red.start(c, 0)
            own_copy(c).start()

    moments = {}
    for c in range(nchunk):
        times = (2, 6, 11) if c < 2 else (2, 8, 13)
        for stage in range(bits):
            at = times[min(stage, 2)] + max(0, stage - 2)
            moments.setdefault(min(at * steps // 8, 2 * steps - 1), []).append((c, stage))

    def advance(half):
        for at, work in moments.items():
            if at % 2 == half:
                @pl.when(step == at // 2)
                def _(work=work):
                    for c, stage in work:
                        if stage == 0:
                            own_copy(c).wait()
                        red.add(c, stage)
                        if stage + 1 < bits:
                            red.start(c, stage + 1)

    first, last = red.me_s == 0, red.me_s == parts - 1
    slot = lax.rem(step, 2)

    @pl.when(jnp.logical_and(step == 0, last))
    def _():
        back[1] = jnp.zeros(back.shape[1:], BF16)
        fills = [pltpu.make_async_copy(back.at[1], dkvn_ref.at[:, :, pl.ds(i * PAIR, PAIR)], back_recv.at[i])
                 for i in range(steps)]
        for fill in fills:
            fill.start()
        for fill in fills:
            fill.wait()

    advance(0)

    @pl.when(jnp.logical_and(step >= 2, jnp.logical_not(first)))
    def _():
        back_copy(step - 2).wait_send()

    attend_pair(flag_ref, q_ref, kv_ref, kvp_ref, do_ref, o_ref, dq_ref, dkv_ref,
                back.at[slot], pt, ds, kvt, qm, dom, lambda: advance(1))

    @pl.when(jnp.logical_not(first))
    def _():
        back_copy(step).start()

    @pl.when(step == steps - 1)
    def _():
        for c in range(nchunk):
            mat, col, size, _ = chunks[c]
            (partw_ref, partr_ref)[mat][:, :, col:col + size] = recv[c][bits - 1][...]
            red.wait_sends(c, bits)

        @pl.when(jnp.logical_not(first))
        def _():
            for i in range(max(0, steps - 2), steps):
                back_copy(i).wait_send()

        @pl.when(jnp.logical_not(last))
        def _():
            for i in range(steps):
                back_copy(i).wait_recv()


def attend(bits, parts, flag, q, kv, kvp, do, gw, gr):
    rows, width = q.shape
    steps = width // PAIR
    hidden = gr.shape[1]
    take = gw.shape[0] // (parts << bits)
    shaped = [g.reshape((2,) * bits + (parts, take, g.shape[1])) for g in (gw, gr)]
    plain, other = halving_orders(bits)
    chunks = [(0, 0, hidden // 2, plain), (1, 0, hidden // 2, other),
              (0, hidden // 2, hidden // 2, plain), (1, hidden // 2, hidden // 2, other)]
    npeer = bits + parts - 1
    tok = pl.BlockSpec((rows, PAIR), lambda i: (0, i))
    kvs = pl.BlockSpec((2, rows, PAIR), lambda i: (0, 0, i))
    hbm = pl.BlockSpec(memory_space=pl.ANY)
    tok_shape = jax.ShapeDtypeStruct((rows, width), BF16)
    kv_shape = jax.ShapeDtypeStruct((2, rows, width), BF16)
    part = (parts, take, hidden)
    return pl.pallas_call(
        partial(attend_kernel, bits, parts, chunks),
        grid=(steps,),
        out_shape=(tok_shape, tok_shape, kv_shape, kv_shape,
                   jax.ShapeDtypeStruct(part, BF16), jax.ShapeDtypeStruct(part, BF16)),
        in_specs=[pl.BlockSpec(memory_space=pltpu.SMEM), tok, kvs, kvs, tok, hbm, hbm],
        out_specs=(tok, tok, kvs, hbm, whole(part), whole(part)),
        scratch_shapes=[
            pltpu.VMEM((2,) * (bits - 1) + (parts, take, size), BF16) for _, _, size, _ in chunks
        ] + halving_scratch(bits, parts, take, chunks, False) + [
            pltpu.VMEM((2, 2 * rows, rows), BF16),
            pltpu.VMEM((2, 2 * rows, rows), BF16),
            pltpu.VMEM((2, PAIR, 2 * rows), BF16),
            pltpu.VMEM((2, rows, PAIR), BF16),
            pltpu.VMEM((2, rows, PAIR), BF16),
            pltpu.VMEM((2, 2, rows, PAIR), BF16),
            pltpu.SemaphoreType.DMA((len(chunks),)),
            pltpu.SemaphoreType.DMA((len(chunks), npeer)),
            pltpu.SemaphoreType.DMA((len(chunks), npeer)),
            pltpu.SemaphoreType.DMA((steps,)),
            pltpu.SemaphoreType.DMA((steps,)),
        ],
        compiler_params=pltpu.CompilerParams(
            vmem_limit_bytes=63 << 20, collective_id=1, has_side_effects=True),
        cost_estimate=cost(60 * rows * rows * width, 20 * rows * width),
        name="attend",
    )(flag, q, kv, kvp, do, *shaped)


def dense_kernel(o_ref, wd_ref, db_ref, rb_ref, mid_ref, x_ref, og_ref, out_ref, dwd_ref, ot):
    @pl.when(pl.program_id(0) == 0)
    def _():
        ot[...] = o_ref[...].T

    total = x_ref[...].astype(F32) + mid_ref[...] + (db_ref[...] + rb_ref[...])
    out_ref[...] = (total + dot(o_ref[...], wd_ref[...])).astype(BF16)
    dwd_ref[...] = dot(ot[...], og_ref[...]).astype(BF16)


def dense(o, wd, db, rb, mid, x, og):
    rows, width = x.shape
    blk = 256
    col = lambda r: pl.BlockSpec((r, blk), lambda i: (0, i))
    return pl.pallas_call(
        dense_kernel,
        grid=(width // blk,),
        out_shape=(jax.ShapeDtypeStruct((rows, width), BF16), jax.ShapeDtypeStruct((width, width), BF16)),
        in_specs=[whole(o.shape), col(width), col(1), col(1), col(rows), col(rows), col(rows)],
        out_specs=(col(rows), col(width)),
        scratch_shapes=[pltpu.VMEM((width, rows), BF16)],
        compiler_params=params(),
        cost_estimate=cost(4 * rows * width * width, 12 * rows * width),
        name="dense",
    )(o, wd, db, rb, mid, x, og)


def tail_kernel(bits, parts, chunks, x_ref, gain_ref, gain2_ref, norm_t, w_ref, ang_ref, dq_ref, dkv_ref,
                dkvn_ref, og_ref, sg_ref, dwd_ref, partw_ref, partr_ref, dog_ref, dbe_ref,
                ig_ref, dw_out, dwd_out, dwe_out, dwr_out, vec_out, *refs):
    nchunk = len(chunks)
    recv = [refs[c * (bits + 1):(c + 1) * (bits + 1)] for c in range(nchunk)]
    (tab, fg, dw, db, dgain, dshift, dgain2, dshift2, zw, zr, state, vrecv, send_sem, recv_sem) = refs[
        nchunk * (bits + 1):]
    red = Halving(bits, parts, chunks, (dw, dwd_ref), None, recv, send_sem, recv_sem)
    step = pl.program_id(0)
    steps = pl.num_programs(0)
    width = x_ref.shape[1]
    nstep = width // (STEP_PAIRS * PAIR)
    cols = 3 * STEP_PAIRS * PAIR

    done = set()

    def forward(c, stage):
        if (c, stage) not in done:
            done.add((c, stage))
            red.add(c, stage)
            red.start(c, stage + 1)

    def z_copies():
        return [red.copy(nchunk + 1 + m, bits + n, part.at[peer[1]], dst.at[n], peer)
                for m, (part, dst) in enumerate(((partw_ref, zw), (partr_ref, zr)))
                for n, peer in enumerate(red.others)]

    @pl.when(step == 0)
    def _():
        red.barrier()
        for copy in z_copies():
            copy.start()
        for c in range(nstep, nchunk):
            red.start(c, 0)
        build_tables(ang_ref, tab)
        fg[...] = jnp.zeros_like(fg)

    for c in range(1, nstep):
        @pl.when(step == c)
        def _(c=c):
            red.start(c - 1, 0)
            if c == 1:
                for extra in range(nstep, nchunk):
                    forward(extra, 0)
            else:
                forward(c - 2, 0)
            if c == nstep - 1:
                for extra in range(nstep, nchunk):
                    forward(extra, 1)

    blocks = []
    for n in range(STEP_PAIRS):
        mine = slice(n * PAIR, (n + 1) * PAIR)
        dq = turn(dq_ref[:, mine].astype(F32), tab, -1.0)
        dk = turn(dkv_ref[0, :, mine].astype(F32) + dkvn_ref[0, :, mine].astype(F32), tab, -1.0)
        dv = dkv_ref[1, :, mine].astype(F32) + dkvn_ref[1, :, mine].astype(F32)
        low = low_lanes(dq.shape)
        dk = pltpu.roll(dk, HEAD_DIM, 1)
        blocks += [jnp.where(low, dq, dk), jnp.where(low, dv, dq), jnp.where(low, dk, dv)]
    dm = jnp.concatenate(blocks, axis=1).astype(BF16)
    at = pl.ds(pl.multiple_of(step * cols, cols), cols)
    db[:, at] = jnp.sum(dm.astype(F32), axis=0, keepdims=True)
    dw[(slice(None),) * (bits + 2) + (at,)] = dot(norm_t[...], dm).reshape(
        dw.shape[:-1] + (cols,)).astype(BF16)
    fg[...] += dot_t(dm, w_ref[...])

    def vec_copies(stage):
        if stage < bits:
            return [red.copy(nchunk, stage, state.at[stage], vrecv.at[stage], red.mate[stage])]
        return [red.copy(nchunk, bits + n, state.at[bits], vrecv.at[bits + n], peer)
                for n, peer in enumerate(red.others)]

    def vec_start(stage):
        for copy in vec_copies(stage):
            copy.start()

    def vec_add(stage):
        copies = vec_copies(stage)
        for copy in copies:
            copy.wait_recv()
        total = state[stage]
        for n in range(len(copies)):
            total = total + vrecv[stage + n]
        if stage < bits:
            state[stage + 1] = total
            vec_start(stage + 1)
        else:
            vec_out[...] = total

    @pl.when(step == steps - 1)
    def _():
        red.start(nstep - 1, 0)
        forward(nstep - 2, 0)

        def emit(rows, part):
            ig_ref[rows, :] = (og_ref[rows, :].astype(F32) + part).astype(BF16)

        forward(nstep - 1, 0)
        forward(0, 1)
        norm_args = (x_ref, (gain_ref, gain2_ref), (fg, sg_ref), (dgain, dgain2), (dshift, dshift2), emit)
        row_blocks = x_ref.shape[0] // ROWS
        norm_back(*norm_args, 0, row_blocks // 2)
        forward(1, 1)
        for extra in range(nstep, nchunk):
            forward(extra, 2)
        norm_back(*norm_args, row_blocks // 2, row_blocks)
        begin = 0
        for ref in (dgain, dshift, db, dog_ref, dgain2, dshift2, dbe_ref):
            state[0, :, begin:begin + ref.shape[1]] = ref[...]
            begin += ref.shape[1]
        vec_start(0)
        order = list(range(nstep, nchunk)) + list(range(nstep))
        for stage in range(1, bits):
            for c in order:
                forward(c, stage)
            vec_add(stage - 1)
        copies = z_copies()
        for m, (part, got, out) in enumerate(((partw_ref, zw, dwe_out), (partr_ref, zr, dwr_out))):
            total = part[red.me_s].astype(F32)
            for n in range(parts - 1):
                copies[m * (parts - 1) + n].wait_recv()
                total = total + got[n].astype(F32)
            if m == 0:
                out[...] = total
            else:
                take = total.shape[0]
                for j in range(total.shape[1] // width):
                    out[j * take:(j + 1) * take, :] = total[:, j * width:(j + 1) * width]
        vec_add(bits - 1)
        for c in order:
            mat, col, size, _ = chunks[c]
            (dw_out, dwd_out)[mat][:, col:col + size] = red.total(c)
        vec_add(bits)
        for c in range(nchunk):
            red.wait_sends(c, bits + 1)
        for copy in copies:
            copy.wait_send()
        for stage in range(bits + 1):
            for copy in vec_copies(stage):
                copy.wait_send()


def tail(bits, parts, x, gain, gain2, norm_t, w, ang, dq, dkv, dkvn, og, sg, dwd, partw, partr, dog, dbe):
    rows, width = x.shape
    full, vec = whole((rows, width)), whole((1, width))
    wide = STEP_PAIRS * PAIR
    cols = 3 * wide
    nstep = width // wide
    hidden = dbe.shape[1]
    take = width // (parts << bits)
    total = 5 * width + 3 * width + hidden
    npeer = bits + parts - 1
    lead = (2,) * bits + (parts, take)
    plain, other = halving_orders(bits)
    chunks = [(0, n * cols, cols, other if n % 2 else plain) for n in range(nstep)]
    chunks += [(1, n * (width // 2), width // 2, other if n % 2 else plain) for n in range(2)]
    tok = pl.BlockSpec((rows, wide), lambda i: (0, i))
    kvs = pl.BlockSpec((2, rows, wide), lambda i: (0, 0, i))
    up = pl.BlockSpec((width, cols), lambda i: (0, i))
    dwd = dwd.reshape(lead + (width,))
    outs = [((rows, width), BF16), ((take, 3 * width), F32), ((take, width), F32), ((take, hidden), F32),
            ((take * (hidden // width), width), F32), ((1, total), F32)]
    row_vec = pltpu.VMEM((1, width), F32)
    nsem = (len(chunks) + 3, npeer)
    return pl.pallas_call(
        partial(tail_kernel, bits, parts, chunks),
        grid=(nstep,),
        out_shape=tuple(jax.ShapeDtypeStruct(s, d) for s, d in outs),
        in_specs=[full, vec, vec, whole(norm_t.shape), up, whole(ang.shape), tok, kvs, kvs, full, full,
                  whole(dwd.shape), whole(partw.shape), whole(partr.shape), vec, whole(dbe.shape)],
        out_specs=tuple(whole(s) for s, _ in outs),
        scratch_shapes=halving_scratch(bits, parts, take, chunks, True) + [
            pltpu.VMEM((3, rows, PAIR), F32), pltpu.VMEM((rows, width), F32),
            pltpu.VMEM(lead + (3 * width,), BF16), pltpu.VMEM((1, 3 * width), F32),
            row_vec, row_vec, row_vec, row_vec,
            pltpu.VMEM((parts - 1, take, hidden), BF16), pltpu.VMEM((parts - 1, take, hidden), BF16),
            pltpu.VMEM((bits + 1, 1, total), F32), pltpu.VMEM((npeer, 1, total), F32),
            pltpu.SemaphoreType.DMA(nsem), pltpu.SemaphoreType.DMA(nsem),
        ],
        compiler_params=pltpu.CompilerParams(
            vmem_limit_bytes=63 << 20, collective_id=0, has_side_effects=True),
        cost_estimate=cost(12 * rows * width * width, 8 * rows * width),
        name="tail",
    )(x, gain, gain2, norm_t, w, ang, dq, dkv, dkvn, og, sg, dwd, partw, partr, dog, dbe)


def finish_kernel(sizes, index_ref, ig_ref, dw_ref, dwd_ref, dwe_ref, dwr_ref, vec_ref,
                  ig_out, dw_out, dwd_out, dwe_out, dwr_out, *outs):
    for src, dst in ((ig_ref, ig_out), (dw_ref, dw_out), (dwd_ref, dwd_out), (dwe_ref, dwe_out),
                     (dwr_ref, dwr_out)):
        dst[...] = src[...]

    @pl.when(pl.program_id(0) == 0)
    def _():
        at = 0
        for size, out in zip(sizes, outs):
            own = out.shape[1]
            row = jnp.broadcast_to(vec_ref[:, at:at + size], (8, size))
            out[...] = pltpu.roll(row, lax.rem(size - index_ref[0] * own, size), 1)[:1, :own]
            at += size


def finish(index, ndev, sizes, ig, dw, dwd, dwe, dwr, vec):
    mats = (ig, dw, dwd, dwe, dwr)
    return pl.pallas_call(
        partial(finish_kernel, sizes),
        out_shape=tuple(jax.ShapeDtypeStruct(m.shape, m.dtype) for m in mats)
        + tuple(jax.ShapeDtypeStruct((1, n // ndev), F32) for n in sizes),
        grid=(1,),
        in_specs=[pl.BlockSpec(memory_space=pltpu.SMEM)] + [whole(m.shape) for m in mats] + [whole(vec.shape)],
        out_specs=tuple([whole(m.shape) for m in mats] + [whole((1, n // ndev)) for n in sizes]),
        compiler_params=params(),
        name="finish",
    )(index, *mats, vec)


def body(
    tokens,
    seq_lengths,
    attn_gain,
    attn_shift,
    qkv_weight,
    qkv_bias,
    dense_weight,
    dense_bias,
    mlp_gain,
    mlp_shift,
    expand_weight,
    expand_bias,
    reduce_weight,
    reduce_bias,
    out_grad,
):
    seq_parts = lax.axis_size("seq")
    place = lax.axis_index("seq")
    rows, width = tokens.shape
    lengths = seq_lengths[0]
    starts = jnp.cumsum(lengths) - lengths
    row0 = place * rows
    offset = row0 - jnp.max(jnp.where(starts <= row0, starts, 0))
    flag = (offset > 0).astype(jnp.int32).reshape(1)
    positions = (offset + jnp.arange(rows, dtype=jnp.int32)).astype(F32)
    frequency = jnp.exp(jnp.arange(ROT // 2, dtype=F32) * (-2.0 * math.log(10000.0) / ROT))
    phases = frequency[:, None] * positions[None, :]
    ang = jnp.concatenate([jnp.cos(phases), jnp.sin(phases)], axis=0)

    row = lambda v: v.reshape(1, -1)
    ag, ash, mg, msh = row(attn_gain), row(attn_shift), row(mlp_gain), row(mlp_shift)

    batch_parts = lax.axis_size("batch")
    ndev = batch_parts * seq_parts
    bits = batch_parts.bit_length() - 1
    q, kv, do, n1t, n2, n2t = project(
        tokens, ag, ash, mg, msh, qkv_weight, row(qkv_bias), ang, out_grad, dense_weight)
    mid, dwr, dog, sg, dwe, dbe, kvp = mlp(
        ndev, seq_parts, n2, n2t, expand_weight, row(expand_bias), reduce_weight, out_grad, kv)
    o, dq, dkv, dkvn, partw, partr = attend(bits, seq_parts, flag, q, kv, kvp, do, dwe, dwr)
    layer_out, dwd = dense(o, dense_weight, row(dense_bias), row(reduce_bias), mid, tokens, out_grad)
    input_grad, dw, dwd, dwe, dwr, vsum = tail(
        bits, seq_parts, tokens, ag, mg, n1t, qkv_weight, ang, dq, dkv, dkvn, out_grad, sg, dwd,
        partw, partr, dog, dbe)
    index = lax.axis_index("batch") * seq_parts + place
    sizes = (width, width, 3 * width, width, width, width, dbe.shape[1])
    input_grad, dw, dwd, dwe, dwr, *vectors = finish(
        index.astype(jnp.int32).reshape(1), ndev, sizes, input_grad, dw, dwd, dwe, dwr, vsum)
    dag, das, dqb, dog, dmg, dms, dbe = [v.reshape(-1) for v in vectors]
    return (
        layer_out,
        input_grad,
        dag,
        das,
        dw,
        dqb,
        dwd,
        dog,
        dmg,
        dms,
        dwe,
        dbe,
        dwr,
        dog,
    )


def solution(mesh):
    tok = P(("batch", "seq"), None)
    vec = P(("batch", "seq"))
    in_specs = (tok, P("batch", None)) + (P(),) * 12 + (tok,)
    out_specs = (tok, tok, vec, vec, tok, vec, tok, vec, vec, vec, tok, vec, tok, vec)
    return jax.shard_map(body, mesh=mesh, in_specs=in_specs, out_specs=out_specs, check_vma=False)
```

```python
from functools import partial
import math

import jax
import jax.numpy as jnp
from jax import lax
from jax.experimental import pallas as pl
from jax.experimental.pallas import tpu as pltpu
from jax.sharding import PartitionSpec as P


HEAD_DIM = 64
ROT = 16
PAIR = 2 * HEAD_DIM
EPSILON = 1e-05
MASKED = -1e30
SCALE = 1.0 / math.sqrt(HEAD_DIM)
QB = 256
FB = 1024
STEP_PAIRS = 2
ROWS = 128
F32 = jnp.float32
BF16 = jnp.bfloat16
VMEM_LIMIT = 60 << 20


def dot(left, right):
    return jnp.dot(left, right, preferred_element_type=F32)


def dot_t(left, right):
    return lax.dot_general(left, right, (((1,), (1,)), ((), ())), preferred_element_type=F32)


def params():
    return pltpu.CompilerParams(vmem_limit_bytes=VMEM_LIMIT)


def cost(flops, nbytes):
    return pl.CostEstimate(flops=int(flops), bytes_accessed=int(nbytes), transcendentals=0)


def whole(shape):
    return pl.BlockSpec(shape, lambda i: (0,) * len(shape), pipeline_mode=pl.Buffered(1))


def statistics(x):
    mean = jnp.mean(x, axis=-1, keepdims=True)
    centered = x - mean
    variance = jnp.mean(centered * centered, axis=-1, keepdims=True)
    rstd = lax.rsqrt(variance + EPSILON)
    return centered * rstd, rstd


def row_block(i):
    return pl.ds(pl.multiple_of(i * ROWS, ROWS), ROWS)


def norm_rows(x_ref, gains, outs):
    def step(i, carry):
        rows = row_block(i)
        xn, _ = statistics(x_ref[rows, :].astype(F32))
        for (gain_ref, shift_ref), out_ref in zip(gains, outs):
            out_ref[rows, :] = (xn * gain_ref[...] + shift_ref[...]).astype(BF16)
        return carry

    lax.fori_loop(0, x_ref.shape[0] // ROWS, step, 0)


def norm_back(x_ref, gains, grads, gain_grads, shift_grads, emit, begin, end):
    if begin == 0:
        for ref in gain_grads + shift_grads:
            ref[...] = jnp.zeros_like(ref)

    def step(i, carry):
        rows = row_block(i)
        xn, rstd = statistics(x_ref[rows, :].astype(F32))
        scaled = 0.0
        for gain_ref, grad_ref, dgain_ref, dshift_ref in zip(gains, grads, gain_grads, shift_grads):
            grad = grad_ref[rows, :]
            dgain_ref[...] += jnp.sum(grad * xn, axis=0, keepdims=True)
            dshift_ref[...] += jnp.sum(grad, axis=0, keepdims=True)
            scaled = scaled + grad * gain_ref[...]
        mean_s = jnp.mean(scaled, axis=-1, keepdims=True)
        mean_sx = jnp.mean(scaled * xn, axis=-1, keepdims=True)
        emit(rows, rstd * (scaled - mean_s - xn * mean_sx))
        return carry

    lax.fori_loop(begin, end, step, 0)


def build_tables(angle_ref, tab_ref):
    half = ROT // 2
    cos8, sin8 = angle_ref[0:half, :], angle_ref[half:ROT, :]
    rest = HEAD_DIM - ROT
    count = cos8.shape[1]
    ones = jnp.ones((rest, count), F32)
    zeros = jnp.zeros((rest, count), F32)
    z8 = jnp.zeros_like(sin8)
    tab_ref[0] = jnp.concatenate([cos8, cos8, ones] * 2, axis=0).T
    tab_ref[1] = jnp.concatenate([-sin8, z8, zeros] * 2, axis=0).T
    tab_ref[2] = jnp.concatenate([z8, sin8, zeros] * 2, axis=0).T


def turn(u, tab_ref, sign):
    half = ROT // 2
    ahead = pltpu.roll(u, PAIR - half, 1)
    behind = pltpu.roll(u, half, 1)
    return u * tab_ref[0] + sign * (ahead * tab_ref[1] + behind * tab_ref[2])


def low_lanes(shape):
    return lax.broadcasted_iota(jnp.int32, shape, 1) < HEAD_DIM


def project_kernel(x_ref, gain_ref, shift_ref, gain2_ref, shift2_ref, w_ref, b_ref, ang_ref, og_ref,
                   wd_ref, q_ref, kv_ref, kvh_ref, do_ref, n1t_ref, n2_ref, n2t_ref,
                   norm, n1t, n2, n2t, tab, sem):
    saves = [pltpu.make_async_copy(src, dst, sem.at[n]) for n, (src, dst) in enumerate(
        ((n1t, n1t_ref), (n2, n2_ref), (n2t, n2t_ref)))]

    @pl.when(pl.program_id(0) == 0)
    def _():
        norm_rows(x_ref, ((gain_ref, shift_ref), (gain2_ref, shift2_ref)), (norm, n2))
        saves[1].start()
        n1t[...] = norm[...].T
        saves[0].start()
        n2t[...] = n2[...].T
        saves[2].start()
        build_tables(ang_ref, tab)

    for n in range(STEP_PAIRS):
        cols = slice(n * 3 * PAIR, (n + 1) * 3 * PAIR)
        mine = slice(n * PAIR, (n + 1) * PAIR)
        mixed = dot(norm[...], w_ref[:, cols]) + b_ref[:, cols]
        t0, t1, t2 = mixed[:, :PAIR], mixed[:, PAIR:2 * PAIR], mixed[:, 2 * PAIR:]
        low = low_lanes(t0.shape)
        q = jnp.where(low, t0, t1)
        k = pltpu.roll(jnp.where(low, t2, t0), HEAD_DIM, 1)
        v = jnp.where(low, t1, t2)
        q_ref[:, mine] = turn(q, tab, 1.0).astype(BF16)
        kv_ref[0, :, mine] = turn(k, tab, 1.0).astype(BF16)
        kv_ref[1, :, mine] = v.astype(BF16)
    do_ref[...] = dot_t(og_ref[...], wd_ref[...]).astype(BF16)

    @pl.when(pl.program_id(0) < pl.num_programs(0) // 2)
    def _():
        kvh_ref[...] = kv_ref[...]

    @pl.when(pl.program_id(0) == pl.num_programs(0) - 1)
    def _():
        for save in saves:
            save.wait()


def project(x, gain, shift, gain2, shift2, w, b, ang, og, wd):
    rows, width = x.shape
    wide = STEP_PAIRS * PAIR
    tok = pl.BlockSpec((rows, wide), lambda i: (0, i))
    return pl.pallas_call(
        project_kernel,
        grid=(width // wide,),
        out_shape=(
            jax.ShapeDtypeStruct((rows, width), BF16),
            jax.ShapeDtypeStruct((2, rows, width), BF16),
            jax.ShapeDtypeStruct((2, rows, width // 2), BF16),
            jax.ShapeDtypeStruct((rows, width), BF16),
            jax.ShapeDtypeStruct((width, rows), BF16),
            jax.ShapeDtypeStruct((rows, width), BF16),
            jax.ShapeDtypeStruct((width, rows), BF16),
        ),
        in_specs=[
            whole((rows, width)), *[whole((1, width))] * 4,
            pl.BlockSpec((width, 3 * wide), lambda i: (0, i)),
            pl.BlockSpec((1, 3 * wide), lambda i: (0, i)),
            whole(ang.shape), whole((rows, width)),
            pl.BlockSpec((wide, width), lambda i: (i, 0)),
        ],
        out_specs=(tok, pl.BlockSpec((2, rows, wide), lambda i: (0, 0, i)),
                   pl.BlockSpec((2, rows, wide), lambda i: (0, 0, jnp.minimum(i, width // wide // 2 - 1))), tok,
                   *[pl.BlockSpec(memory_space=pl.ANY)] * 3),
        scratch_shapes=[pltpu.VMEM((rows, width), BF16), pltpu.VMEM((width, rows), BF16),
                        pltpu.VMEM((rows, width), BF16), pltpu.VMEM((width, rows), BF16),
                        pltpu.VMEM((3, rows, PAIR), F32), pltpu.SemaphoreType.DMA((3,))],
        compiler_params=params(),
        cost_estimate=cost(8 * rows * width * width, 24 * rows * width),
        name="project",
    )(x, gain, shift, gain2, shift2, w, b, ang, og, wd)


def gelu_parts(h):
    z = jnp.abs(h) * math.sqrt(0.5)
    t = 1.0 / (1.0 + 0.5 * z)
    poly = jnp.full_like(t, 0.17087277)
    for c in (-0.82215223, 1.48851587, -1.13520398, 0.27886807, -0.18628806, 0.09678418,
              0.37409196, 1.00002368, -1.26551223):
        poly = poly * t + c
    zz = z * z
    tail = 0.5 * t * jnp.exp(poly - zz)
    cdf = jnp.where(h >= 0, 1.0 - tail, tail)
    slope = cdf + h * (jnp.exp(-zz) * (1.0 / math.sqrt(2.0 * math.pi)))
    return h * cdf, slope


def mlp_fwd_kernel(take, norm, we_ref, be_ref, wr_ref, og_ref, mid_ref, slope_ref, dwr_ref, dog_ref):
    step = pl.program_id(0)
    width = norm.shape[1]

    @pl.when(step == 0)
    def _():
        mid_ref[...] = jnp.zeros_like(mid_ref)
        dog_ref[...] = jnp.sum(og_ref[...].astype(F32), axis=0, keepdims=True)

    h = dot(norm[...], we_ref[...]) + be_ref[...]
    active, slope = gelu_parts(h)
    active = active.astype(BF16)
    slope_ref[...] = slope.astype(BF16)
    mid_ref[...] += dot(active, wr_ref[...])
    dwr = dot(active.T, og_ref[...]).astype(BF16)
    full = dwr_ref.shape[1]
    ratio = full // width
    for piece in range(FB // take):
        group, j = piece // ratio, piece % ratio
        dwr_ref[group * take:(group + 1) * take, j * width:(j + 1) * width] = (
            dwr[piece * take:(piece + 1) * take, :])


def mlp_back_kernel(norm_t, we_ref, wr_ref, og_ref, slope_ref, sg, dwe_ref, dbe_ref):
    @pl.when(pl.program_id(0) == 0)
    def _():
        sg[...] = jnp.zeros_like(sg)

    hidden = (dot_t(og_ref[...], wr_ref[...]) * slope_ref[...].astype(F32)).astype(BF16)
    dwe_ref[...] = dot(norm_t[...], hidden).astype(BF16)
    dbe_ref[...] = jnp.sum(hidden.astype(F32), axis=0, keepdims=True)
    sg[...] += dot_t(hidden, we_ref[...])


def mlp_specs(x):
    rows, width = x.shape
    full = whole((rows, width))
    vec = whole((1, width))
    up = pl.BlockSpec((width, FB), lambda i: (0, i))
    down = pl.BlockSpec((FB, width), lambda i: (i, 0))
    bias = pl.BlockSpec((1, FB), lambda i: (0, i))
    act = pl.BlockSpec((rows, FB), lambda i: (0, i))
    return full, vec, up, down, bias, act


def mlp_fwd(ndev, norm, we, be, wr, og):
    rows, width = norm.shape
    hidden = we.shape[1]
    full, vec, up, down, bias, act = mlp_specs(norm)
    out_rows = width
    blk = FB * out_rows // hidden
    gshape = (out_rows, hidden)
    return pl.pallas_call(
        partial(mlp_fwd_kernel, out_rows // ndev),
        grid=(hidden // FB,),
        out_shape=(jax.ShapeDtypeStruct((rows, width), F32), jax.ShapeDtypeStruct((rows, hidden), BF16),
                   jax.ShapeDtypeStruct(gshape, BF16), jax.ShapeDtypeStruct((1, width), F32)),
        in_specs=[full, up, bias, down, full],
        out_specs=(full, act, pl.BlockSpec((blk, hidden), lambda i: (i, 0)), vec),
        compiler_params=params(),
        cost_estimate=cost(6 * rows * width * hidden, 8 * width * hidden),
        name="mlp_fwd",
    )(norm, we, be, wr, og)


def mlp_back(norm_t, we, wr, og, slope):
    rows, width = og.shape
    hidden = we.shape[1]
    full, _, up, down, bias, act = mlp_specs(og)
    return pl.pallas_call(
        mlp_back_kernel,
        grid=(hidden // FB,),
        out_shape=(jax.ShapeDtypeStruct((rows, width), F32), jax.ShapeDtypeStruct((width, hidden), BF16),
                   jax.ShapeDtypeStruct((1, hidden), F32)),
        in_specs=[whole(norm_t.shape), up, down, full, act],
        out_specs=(full, up, bias),
        compiler_params=params(),
        cost_estimate=cost(6 * rows * width * hidden, 8 * width * hidden),
        name="mlp_back",
    )(norm_t, we, wr, og, slope)


MESH = pl.DeviceIdType.MESH


class Halving:
    def __init__(self, bits, parts, chunks, mats, own, recv, send_sem, recv_sem):
        self.bits, self.parts, self.chunks = bits, parts, chunks
        self.mats, self.own, self.recv = mats, own, recv
        self.send_sem, self.recv_sem = send_sem, recv_sem
        self.me_b, self.me_s = lax.axis_index("batch"), lax.axis_index("seq")
        self.bit = [lax.rem(self.me_b // (1 << k), 2) for k in range(bits)]
        self.mate = [
            (self.me_b + (1 << k) - 2 * (1 << k) * self.bit[k], self.me_s) for k in range(bits)]
        self.others = [(self.me_b, lax.rem(self.me_s + d, parts)) for d in range(1, parts)]
        self.peers = self.mate + self.others

    def barrier(self):
        sem = pltpu.get_barrier_semaphore()
        for peer in self.peers:
            pl.semaphore_signal(sem, inc=1, device_id=peer, device_id_type=MESH)
        pl.semaphore_wait(sem, len(self.peers))

    def copy(self, slot, n, src, dst, peer):
        return pltpu.make_async_remote_copy(
            src_ref=src, dst_ref=dst, send_sem=self.send_sem.at[slot, n],
            recv_sem=self.recv_sem.at[slot, n], device_id=peer, device_id_type=MESH)

    def dims(self, order, stage):
        return [d for d in range(self.bits - 1, -1, -1) if d not in order[:stage]]

    def part(self, c, value):
        mat, col, size, order = self.chunks[c]
        index = tuple(value if d == order[0] else slice(None) for d in self.dims(order, 0))
        return self.mats[mat].at[index + (slice(None), slice(None), pl.ds(col, size))]

    def copies(self, c, stage):
        order = self.chunks[c][3]
        if stage == self.bits:
            return [
                self.copy(c, self.bits + n, self.recv[c][stage - 1].at[peer[1]], self.recv[c][stage].at[n], peer)
                for n, peer in enumerate(self.others)]
        k = order[stage]
        if stage == 0:
            src = self.part(c, 1 - self.bit[k])
        else:
            index = tuple(1 - self.bit[k] if d == k else slice(None) for d in self.dims(order, stage))
            src = self.recv[c][stage - 1].at[index]
        return [self.copy(c, stage, src, self.recv[c][stage], self.mate[k])]

    def start(self, c, stage):
        for copy in self.copies(c, stage):
            copy.start()

    def wait_sends(self, c, stages):
        for stage in range(stages):
            for copy in self.copies(c, stage):
                copy.wait_send()

    def add(self, c, stage):
        mat, col, size, order = self.chunks[c]
        k = order[stage]
        dims = self.dims(order, stage)
        self.copies(c, stage)[0].wait_recv()
        dst = self.recv[c][stage]
        lead = self.bits - 1 - stage

        def one(i, carry):
            part = lax.rem(i, self.parts)
            rest = i // self.parts
            sub = tuple(lax.rem(rest // (1 << (lead - 1 - n)), 2) for n in range(lead))
            at = sub + (part,)
            left = list(sub)
            own_at = tuple(self.bit[k] if d == k else left.pop(0) for d in dims) + (part,)
            if stage > 0:
                own = self.recv[c][stage - 1][own_at]
            elif self.own is None:
                own = self.mats[mat][own_at + (slice(None), pl.ds(col, size))]
            else:
                own = self.own[c][at]
            dst[at] = own + dst[at]
            return carry

        lax.fori_loop(0, self.parts << lead, one, 0)

    def total(self, c):
        total = self.recv[c][self.bits - 1][self.me_s].astype(F32)
        for n, copy in enumerate(self.copies(c, self.bits)):
            copy.wait_recv()
            total = total + self.recv[c][self.bits][n].astype(F32)
        return total


def halving_orders(bits):
    plain = list(range(bits))
    other = [0] + [k for i in range(1, bits, 2) for k in reversed(range(i, min(i + 2, bits)))]
    return plain, other


def halving_scratch(bits, parts, rows, chunks, ends):
    scratch = []
    for (_, _, size, _), end in zip(chunks, ends):
        for stage in range(bits):
            scratch.append(pltpu.VMEM((2,) * (bits - 1 - stage) + (parts, rows, size), BF16))
        if end:
            scratch.append(pltpu.VMEM((parts - 1, rows, size), BF16))
    return scratch


def attend_pair(flag_ref, q_ref, kv_ref, kvp_ref, do_ref, o_ref, dq_ref, dkv_ref, dkvp_ref,
                pt, ds, kvt, qm, dom, midway):
    rows_all = q_ref.shape[0]
    nq = rows_all // QB
    away = (flag_ref[0] - 1).astype(F32) * (-MASKED)
    sources = [(kvp_ref, i) for i in range(nq)] + [(kv_ref, i) for i in range(nq)]

    def block(which, b):
        ref, i = sources[b]
        return ref[which, i * QB:(i + 1) * QB, :]

    for which in range(2):
        kvt[which, :, :rows_all] = kvp_ref[which].T
        kvt[which, :, rows_all:] = kv_ref[which].T
    lane = lax.broadcasted_iota(jnp.int32, (QB, PAIR), 1)
    sub = lax.broadcasted_iota(jnp.int32, (PAIR, QB), 0)
    causal = lax.broadcasted_iota(jnp.int32, (QB, QB), 0) <= lax.broadcasted_iota(
        jnp.int32, (QB, QB), 1)
    for j in range(nq):
        if j == nq // 2:
            midway()
        rows = slice(j * QB, (j + 1) * QB)
        q = q_ref[rows, :] * jnp.asarray(SCALE, BF16)
        qt = q.T
        dot_rows = do_ref[rows, :].astype(F32).T
        blocks = range(nq + j + 1)
        k1 = (nq + j + 1) * QB
        outs, scaled, dqs = [], [], []
        for h in range(2):
            hs = slice(h * HEAD_DIM, (h + 1) * HEAD_DIM)
            qm[h, rows, :] = jnp.where((lane < HEAD_DIM) == (h == 0), q, jnp.zeros_like(q))
            qtm = jnp.where((sub < HEAD_DIM) == (h == 0), qt, jnp.zeros_like(qt))
            scores, tops = [], [None, None]
            for b in blocks:
                s = dot(block(0, b), qtm)
                if b == nq + j:
                    s = jnp.where(causal, s, MASKED)
                scores.append(s)
                part = jnp.max(s.reshape(QB // 8, 8, QB), axis=0)
                side = int(b >= nq)
                tops[side] = part if tops[side] is None else jnp.maximum(tops[side], part)
            top = jnp.max(jnp.maximum(tops[0] + away, tops[1]), axis=0, keepdims=True)
            shift = (top - away, top)
            total = None
            for b, s in zip(blocks, scores):
                p = jnp.exp(s - shift[int(b >= nq)])
                part = jnp.sum(p.reshape(QB // 8, 8, QB), axis=0)
                total = part if total is None else total + part
                pt[h, b * QB:(b + 1) * QB, rows] = p.astype(BF16)
            inv = 1.0 / jnp.sum(total, axis=0, keepdims=True)
            out_t = dot(kvt[1, hs, :k1], pt[h, :k1, rows]) * inv
            dol_t = dot_rows[hs] * inv
            delta = jnp.sum(dol_t * out_t, axis=0, keepdims=True)
            outs.append(out_t)
            scaled.append(dol_t)
            zero = jnp.zeros((HEAD_DIM, QB), BF16)
            dol_b = dol_t.astype(BF16)
            dol_m = jnp.concatenate([dol_b, zero] if h == 0 else [zero, dol_b], axis=0)
            for b in blocks:
                dp = dot(block(1, b), dol_m)
                d = pt[h, b * QB:(b + 1) * QB, rows].astype(F32) * (dp - delta)
                ds[h, b * QB:(b + 1) * QB, rows] = d.astype(BF16)
            dqs.append(dot(kvt[0, hs, :k1], ds[h, :k1, rows]) * SCALE)
        o_ref[rows, :] = jnp.concatenate(outs, 0).T.astype(BF16)
        dq_ref[rows, :] = jnp.concatenate(dqs, 0).T.astype(BF16)
        dol = jnp.concatenate(scaled, 0).T.astype(BF16)
        for h in range(2):
            dom[h, rows, :] = jnp.where((lane < HEAD_DIM) == (h == 0), dol, jnp.zeros_like(dol))
    for b in range(2 * nq):
        q0 = max(0, b - nq) * QB
        br = slice(b * QB, (b + 1) * QB)
        dk = dot(ds[0, br, q0:], qm[0, q0:, :]) + dot(ds[1, br, q0:], qm[1, q0:, :])
        dv = dot(pt[0, br, q0:], dom[0, q0:, :]) + dot(pt[1, br, q0:], dom[1, q0:, :])
        ref, i = (dkvp_ref, b) if b < nq else (dkv_ref, b - nq)
        ref[0, i * QB:(i + 1) * QB, :] = dk.astype(BF16)
        ref[1, i * QB:(i + 1) * QB, :] = dv.astype(BF16)


def fold_rows(out_ref, total):
    take, width = total.shape[0], out_ref.shape[1]
    for j in range(total.shape[1] // width):
        out_ref[j * take:(j + 1) * take, :] = total[:, j * width:(j + 1) * width]


def attend_kernel(bits, parts, chunks, ends, flag_ref, q_ref, kv_ref, kv_hbm, kvp_hbm, do_ref, gw_ref, gr_ref,
                  o_ref, dq_ref, dkv_ref, dkvn_ref, partw_ref, partr_ref, totw_ref, totr_ref, *refs):
    nchunk = len(chunks)
    own, refs = refs[:nchunk], refs[nchunk:]
    recv = []
    for end in ends:
        recv.append(refs[:bits + end])
        refs = refs[bits + end:]
    (pt, ds, kvt, qm, dom, back, kvp, own_sem, send_sem, recv_sem, back_send, back_recv,
     kv_load, kv_send, kv_recv) = refs
    red = Halving(bits, parts, chunks, (gw_ref, gr_ref), own, recv, send_sem, recv_sem)
    step = pl.program_id(0)
    steps = dkvn_ref.shape[2] // PAIR

    def own_copy(c):
        return pltpu.make_async_copy(red.part(c, red.bit[chunks[c][3][0]]), own[c], own_sem.at[c])

    def back_copy(i):
        cols = pl.ds(pl.multiple_of(i * PAIR, PAIR), PAIR)
        return pltpu.make_async_remote_copy(
            src_ref=back.at[lax.rem(i, 2)], dst_ref=dkvn_ref.at[:, :, cols],
            send_sem=back_send.at[i], recv_sem=back_recv.at[i],
            device_id=red.others[parts - 2], device_id_type=MESH)

    first, last = red.me_s == 0, red.me_s == parts - 1
    half_steps = steps // 2

    def pair_cols(i):
        return pl.ds(pl.multiple_of(i * PAIR, PAIR), PAIR)

    def load_copy(i):
        return pltpu.make_async_copy(kvp_hbm.at[:, :, pair_cols(i)], kvp.at[i], kv_load.at[i])

    def onward_copy(i):
        return pltpu.make_async_remote_copy(
            src_ref=kv_hbm.at[:, :, pair_cols(i)], dst_ref=kvp.at[i],
            send_sem=kv_send.at[i - half_steps], recv_sem=kv_recv.at[i - half_steps],
            device_id=red.others[0], device_id_type=MESH)

    @pl.when(step == 0)
    def _():
        red.barrier()
        for i in range(half_steps):
            load_copy(i).start()
        for c in range(nchunk):
            red.start(c, 0)
            own_copy(c).start()

    @pl.when(jnp.logical_and(step == 0, jnp.logical_not(last)))
    def _():
        for i in range(half_steps, steps):
            onward_copy(i).start()

    @pl.when(jnp.logical_and(step == 0, first))
    def _():
        kvp[half_steps:] = jnp.zeros((steps - half_steps,) + kvp.shape[1:], BF16)

    moments = {}
    for c in range(nchunk):
        times = (2, 7, 11) if ends[c] else (2, 8, 13)
        for stage in range(bits):
            at = times[min(stage, 2)] + max(0, stage - 2)
            moments.setdefault(min(at * steps // 8, 2 * steps - 1), []).append((c, stage))

    def advance(half):
        for at, work in moments.items():
            if at % 2 == half:
                @pl.when(step == at // 2)
                def _(work=work):
                    for c, stage in work:
                        if stage == 0:
                            own_copy(c).wait()
                        red.add(c, stage)
                        if stage + 1 < bits + ends[c]:
                            red.start(c, stage + 1)

    slot = lax.rem(step, 2)

    @pl.when(jnp.logical_and(step == 0, last))
    def _():
        back[1] = jnp.zeros(back.shape[1:], BF16)
        fills = [pltpu.make_async_copy(back.at[1], dkvn_ref.at[:, :, pl.ds(i * PAIR, PAIR)], back_recv.at[i])
                 for i in range(steps)]
        for fill in fills:
            fill.start()
        for fill in fills:
            fill.wait()

    advance(0)

    @pl.when(jnp.logical_and(step >= 2, jnp.logical_not(first)))
    def _():
        back_copy(step - 2).wait_send()

    @pl.when(step < half_steps)
    def _():
        load_copy(step).wait()

    @pl.when(jnp.logical_and(step >= half_steps, jnp.logical_not(first)))
    def _():
        onward_copy(step).wait_recv()

    attend_pair(flag_ref, q_ref, kv_ref, kvp.at[step], do_ref, o_ref, dq_ref, dkv_ref,
                back.at[slot], pt, ds, kvt, qm, dom, lambda: advance(1))

    @pl.when(jnp.logical_not(first))
    def _():
        back_copy(step).start()

    @pl.when(step == steps - 1)
    def _():
        for c in range(nchunk):
            mat, col, size, _ = chunks[c]
            if not ends[c]:
                (partw_ref, partr_ref)[mat][...] = recv[c][bits - 1][...]
            red.wait_sends(c, bits + ends[c])
        for c in range(nchunk):
            mat, col, size, _ = chunks[c]
            if ends[c] and mat == 0:
                totw_ref[...] = red.total(c)
            elif ends[c]:
                fold_rows(totr_ref, red.total(c))

        @pl.when(jnp.logical_not(last))
        def _():
            for i in range(half_steps, steps):
                onward_copy(i).wait_send()

        @pl.when(jnp.logical_not(first))
        def _():
            for i in range(max(0, steps - 2), steps):
                back_copy(i).wait_send()

        @pl.when(jnp.logical_not(last))
        def _():
            for i in range(steps):
                back_copy(i).wait_recv()


def attend(bits, parts, flag, q, kv, kvp, do, gw, gr):
    rows, width = q.shape
    steps = width // PAIR
    hidden = gr.shape[1]
    take = gw.shape[0] // (parts << bits)
    shaped = [g.reshape((2,) * bits + (parts, take, g.shape[1])) for g in (gw, gr)]
    plain, other = halving_orders(bits)
    chunks = [(0, 0, hidden // 2, plain), (1, 0, hidden // 2, other),
              (0, hidden // 2, hidden // 2, plain), (1, hidden // 2, hidden // 2, other)]
    npeer = bits + parts - 1
    tok = pl.BlockSpec((rows, PAIR), lambda i: (0, i))
    kvs = pl.BlockSpec((2, rows, PAIR), lambda i: (0, 0, i))
    hbm = pl.BlockSpec(memory_space=pl.ANY)
    tok_shape = jax.ShapeDtypeStruct((rows, width), BF16)
    kv_shape = jax.ShapeDtypeStruct((2, rows, width), BF16)
    ends = (1, 1, 0, 0)
    part = (parts, take, hidden // 2)
    totw, totr = (take, hidden // 2), (take * hidden // 2 // width, width)
    return pl.pallas_call(
        partial(attend_kernel, bits, parts, chunks, ends),
        grid=(steps,),
        out_shape=(tok_shape, tok_shape, kv_shape, kv_shape,
                   jax.ShapeDtypeStruct(part, BF16), jax.ShapeDtypeStruct(part, BF16),
                   jax.ShapeDtypeStruct(totw, F32), jax.ShapeDtypeStruct(totr, F32)),
        in_specs=[pl.BlockSpec(memory_space=pltpu.SMEM), tok, kvs, hbm, hbm, tok, hbm, hbm],
        out_specs=(tok, tok, kvs, hbm, whole(part), whole(part), whole(totw), whole(totr)),
        scratch_shapes=[
            pltpu.VMEM((2,) * (bits - 1) + (parts, take, size), BF16) for _, _, size, _ in chunks
        ] + halving_scratch(bits, parts, take, chunks, ends) + [
            pltpu.VMEM((2, 2 * rows, rows), BF16),
            pltpu.VMEM((2, 2 * rows, rows), BF16),
            pltpu.VMEM((2, PAIR, 2 * rows), BF16),
            pltpu.VMEM((2, rows, PAIR), BF16),
            pltpu.VMEM((2, rows, PAIR), BF16),
            pltpu.VMEM((2, 2, rows, PAIR), BF16),
            pltpu.VMEM((steps, 2, rows, PAIR), BF16),
            pltpu.SemaphoreType.DMA((len(chunks),)),
            pltpu.SemaphoreType.DMA((len(chunks), npeer)),
            pltpu.SemaphoreType.DMA((len(chunks), npeer)),
            pltpu.SemaphoreType.DMA((steps,)),
            pltpu.SemaphoreType.DMA((steps,)),
            pltpu.SemaphoreType.DMA((steps // 2,)),
            pltpu.SemaphoreType.DMA((steps - steps // 2,)),
            pltpu.SemaphoreType.DMA((steps - steps // 2,)),
        ],
        compiler_params=pltpu.CompilerParams(
            vmem_limit_bytes=63 << 20, collective_id=1, has_side_effects=True),
        cost_estimate=cost(60 * rows * rows * width, 20 * rows * width),
        name="attend",
    )(flag, q, kv, kv, kvp, do, *shaped)


def dense_kernel(o_ref, wd_ref, db_ref, rb_ref, mid_ref, x_ref, og_ref, out_ref, dwd_ref, ot):
    @pl.when(pl.program_id(0) == 0)
    def _():
        ot[...] = o_ref[...].T

    total = x_ref[...].astype(F32) + mid_ref[...] + (db_ref[...] + rb_ref[...])
    out_ref[...] = (total + dot(o_ref[...], wd_ref[...])).astype(BF16)
    dwd_ref[...] = dot(ot[...], og_ref[...]).astype(BF16)


def dense(o, wd, db, rb, mid, x, og):
    rows, width = x.shape
    blk = 256
    col = lambda r: pl.BlockSpec((r, blk), lambda i: (0, i))
    return pl.pallas_call(
        dense_kernel,
        grid=(width // blk,),
        out_shape=(jax.ShapeDtypeStruct((rows, width), BF16), jax.ShapeDtypeStruct((width, width), BF16)),
        in_specs=[whole(o.shape), col(width), col(1), col(1), col(rows), col(rows), col(rows)],
        out_specs=(col(rows), col(width)),
        scratch_shapes=[pltpu.VMEM((width, rows), BF16)],
        compiler_params=params(),
        cost_estimate=cost(4 * rows * width * width, 12 * rows * width),
        name="dense",
    )(o, wd, db, rb, mid, x, og)


def tail_kernel(bits, parts, chunks, x_ref, gain_ref, gain2_ref, norm_t, w_ref, ang_ref, dq_ref, dkv_ref,
                dkvn_ref, og_ref, sg_ref, dwd_ref, partw_ref, partr_ref, dog_ref, dbe_ref,
                ig_ref, dw_out, dwd_out, dwe_out, dwr_out, vec_out, *refs):
    nchunk = len(chunks)
    recv = [refs[c * (bits + 1):(c + 1) * (bits + 1)] for c in range(nchunk)]
    (tab, fg, dw, db, dgain, dshift, dgain2, dshift2, zw, zr, state, vrecv, send_sem, recv_sem) = refs[
        nchunk * (bits + 1):]
    red = Halving(bits, parts, chunks, (dw, dwd_ref), None, recv, send_sem, recv_sem)
    step = pl.program_id(0)
    steps = pl.num_programs(0)
    width = x_ref.shape[1]
    nstep = width // (STEP_PAIRS * PAIR)
    cols = 3 * STEP_PAIRS * PAIR

    done = set()

    def forward(c, stage):
        if (c, stage) not in done:
            done.add((c, stage))
            red.add(c, stage)
            red.start(c, stage + 1)

    def z_copies():
        return [red.copy(nchunk + 1 + m, bits + n, part.at[peer[1]], dst.at[n], peer)
                for m, (part, dst) in enumerate(((partw_ref, zw), (partr_ref, zr)))
                for n, peer in enumerate(red.others)]

    @pl.when(step == 0)
    def _():
        red.barrier()
        for copy in z_copies():
            copy.start()
        for c in range(nstep, nchunk):
            red.start(c, 0)
        build_tables(ang_ref, tab)
        fg[...] = jnp.zeros_like(fg)

    for c in range(1, nstep):
        @pl.when(step == c)
        def _(c=c):
            red.start(c - 1, 0)
            if c == 1:
                for extra in range(nstep, nchunk):
                    forward(extra, 0)
            else:
                forward(c - 2, 0)
            if c == nstep - 1:
                for extra in range(nstep, nchunk):
                    forward(extra, 1)

    blocks = []
    for n in range(STEP_PAIRS):
        mine = slice(n * PAIR, (n + 1) * PAIR)
        dq = turn(dq_ref[:, mine].astype(F32), tab, -1.0)
        dk = turn(dkv_ref[0, :, mine].astype(F32) + dkvn_ref[0, :, mine].astype(F32), tab, -1.0)
        dv = dkv_ref[1, :, mine].astype(F32) + dkvn_ref[1, :, mine].astype(F32)
        low = low_lanes(dq.shape)
        dk = pltpu.roll(dk, HEAD_DIM, 1)
        blocks += [jnp.where(low, dq, dk), jnp.where(low, dv, dq), jnp.where(low, dk, dv)]
    dm = jnp.concatenate(blocks, axis=1).astype(BF16)
    at = pl.ds(pl.multiple_of(step * cols, cols), cols)
    db[:, at] = jnp.sum(dm.astype(F32), axis=0, keepdims=True)
    dw[(slice(None),) * (bits + 2) + (at,)] = dot(norm_t[...], dm).reshape(
        dw.shape[:-1] + (cols,)).astype(BF16)
    fg[...] += dot_t(dm, w_ref[...])

    def vec_copies(stage):
        if stage < bits:
            return [red.copy(nchunk, stage, state.at[stage], vrecv.at[stage], red.mate[stage])]
        return [red.copy(nchunk, bits + n, state.at[bits], vrecv.at[bits + n], peer)
                for n, peer in enumerate(red.others)]

    def vec_start(stage):
        for copy in vec_copies(stage):
            copy.start()

    def vec_add(stage):
        copies = vec_copies(stage)
        for copy in copies:
            copy.wait_recv()
        total = state[stage]
        for n in range(len(copies)):
            total = total + vrecv[stage + n]
        if stage < bits:
            state[stage + 1] = total
            vec_start(stage + 1)
        else:
            vec_out[...] = total

    @pl.when(step == steps - 1)
    def _():
        red.start(nstep - 1, 0)
        forward(nstep - 2, 0)

        def emit(rows, part):
            ig_ref[rows, :] = (og_ref[rows, :].astype(F32) + part).astype(BF16)

        forward(nstep - 1, 0)
        forward(0, 1)
        norm_args = (x_ref, (gain_ref, gain2_ref), (fg, sg_ref), (dgain, dgain2), (dshift, dshift2), emit)
        row_blocks = x_ref.shape[0] // ROWS
        norm_back(*norm_args, 0, row_blocks // 2)
        forward(1, 1)
        for extra in range(nstep, nchunk):
            forward(extra, 2)
        norm_back(*norm_args, row_blocks // 2, row_blocks)
        begin = 0
        for ref in (dgain, dshift, db, dog_ref, dgain2, dshift2, dbe_ref):
            state[0, :, begin:begin + ref.shape[1]] = ref[...]
            begin += ref.shape[1]
        vec_start(0)
        order = list(range(nstep, nchunk)) + list(range(nstep))
        for stage in range(1, bits):
            for c in order:
                forward(c, stage)
            vec_add(stage - 1)
        copies = z_copies()
        for m, (part, got, out) in enumerate(((partw_ref, zw, dwe_out), (partr_ref, zr, dwr_out))):
            total = part[red.me_s].astype(F32)
            for n in range(parts - 1):
                copies[m * (parts - 1) + n].wait_recv()
                total = total + got[n].astype(F32)
            if m == 0:
                out[...] = total
            else:
                fold_rows(out, total)
        vec_add(bits - 1)
        for c in order:
            mat, col, size, _ = chunks[c]
            (dw_out, dwd_out)[mat][:, col:col + size] = red.total(c)
        vec_add(bits)
        for c in range(nchunk):
            red.wait_sends(c, bits + 1)
        for copy in copies:
            copy.wait_send()
        for stage in range(bits + 1):
            for copy in vec_copies(stage):
                copy.wait_send()


def tail(bits, parts, x, gain, gain2, norm_t, w, ang, dq, dkv, dkvn, og, sg, dwd, partw, partr, dog, dbe):
    rows, width = x.shape
    full, vec = whole((rows, width)), whole((1, width))
    wide = STEP_PAIRS * PAIR
    cols = 3 * wide
    nstep = width // wide
    hidden, part = dbe.shape[1], partw.shape[2]
    take = width // (parts << bits)
    total = 5 * width + 3 * width + hidden
    npeer = bits + parts - 1
    lead = (2,) * bits + (parts, take)
    plain, other = halving_orders(bits)
    chunks = [(0, n * cols, cols, other if n % 2 else plain) for n in range(nstep)]
    chunks += [(1, n * (width // 2), width // 2, other if n % 2 else plain) for n in range(2)]
    tok = pl.BlockSpec((rows, wide), lambda i: (0, i))
    kvs = pl.BlockSpec((2, rows, wide), lambda i: (0, 0, i))
    up = pl.BlockSpec((width, cols), lambda i: (0, i))
    dwd = dwd.reshape(lead + (width,))
    outs = [((rows, width), BF16), ((take, 3 * width), F32), ((take, width), F32), ((take, part), F32),
            ((take * part // width, width), F32), ((1, total), F32)]
    row_vec = pltpu.VMEM((1, width), F32)
    nsem = (len(chunks) + 3, npeer)
    return pl.pallas_call(
        partial(tail_kernel, bits, parts, chunks),
        grid=(nstep,),
        out_shape=tuple(jax.ShapeDtypeStruct(s, d) for s, d in outs),
        in_specs=[full, vec, vec, whole(norm_t.shape), up, whole(ang.shape), tok, kvs, kvs, full, full,
                  whole(dwd.shape), whole(partw.shape), whole(partr.shape), vec, whole(dbe.shape)],
        out_specs=tuple(whole(s) for s, _ in outs),
        scratch_shapes=halving_scratch(bits, parts, take, chunks, [1] * len(chunks)) + [
            pltpu.VMEM((3, rows, PAIR), F32), pltpu.VMEM((rows, width), F32),
            pltpu.VMEM(lead + (3 * width,), BF16), pltpu.VMEM((1, 3 * width), F32),
            row_vec, row_vec, row_vec, row_vec,
            pltpu.VMEM((parts - 1, take, part), BF16), pltpu.VMEM((parts - 1, take, part), BF16),
            pltpu.VMEM((bits + 1, 1, total), F32), pltpu.VMEM((npeer, 1, total), F32),
            pltpu.SemaphoreType.DMA(nsem), pltpu.SemaphoreType.DMA(nsem),
        ],
        compiler_params=pltpu.CompilerParams(
            vmem_limit_bytes=63 << 20, collective_id=0, has_side_effects=True),
        cost_estimate=cost(12 * rows * width * width, 8 * rows * width),
        name="tail",
    )(x, gain, gain2, norm_t, w, ang, dq, dkv, dkvn, og, sg, dwd, partw, partr, dog, dbe)


def finish_kernel(sizes, index_ref, ig_ref, dw_ref, dwd_ref, dwe0_ref, dwe1_ref, dwr0_ref, dwr1_ref, vec_ref,
                  ig_out, dw_out, dwd_out, dwe_out, dwr_out, *outs):
    for src, dst in ((ig_ref, ig_out), (dw_ref, dw_out), (dwd_ref, dwd_out)):
        dst[...] = src[...]
    half = dwe0_ref.shape[1]
    dwe_out[:, :half] = dwe0_ref[...]
    dwe_out[:, half:] = dwe1_ref[...]
    half = dwr0_ref.shape[0]
    dwr_out[:half, :] = dwr0_ref[...]
    dwr_out[half:, :] = dwr1_ref[...]
    at = 0
    for size, out in zip(sizes, outs):
        own = out.shape[1]
        row = jnp.broadcast_to(vec_ref[:, at:at + size], (8, size))
        out[...] = pltpu.roll(row, lax.rem(size - index_ref[0] * own, size), 1)[:1, :own]
        at += size


def finish(index, ndev, sizes, ig, dw, dwd, dwe0, dwe1, dwr0, dwr1, vec):
    mats = (ig, dw, dwd, dwe0, dwe1, dwr0, dwr1)
    outs = [(m.shape, m.dtype) for m in (ig, dw, dwd)] + [
        ((dwe0.shape[0], 2 * dwe0.shape[1]), F32), ((2 * dwr0.shape[0], dwr0.shape[1]), F32)]
    outs += [((1, n // ndev), F32) for n in sizes]
    return pl.pallas_call(
        partial(finish_kernel, sizes),
        out_shape=tuple(jax.ShapeDtypeStruct(s, d) for s, d in outs),
        grid=(1,),
        in_specs=[pl.BlockSpec(memory_space=pltpu.SMEM)] + [whole(m.shape) for m in mats] + [whole(vec.shape)],
        out_specs=tuple(whole(s) for s, _ in outs),
        compiler_params=params(),
        name="finish",
    )(index, *mats, vec)


def body(
    tokens,
    seq_lengths,
    attn_gain,
    attn_shift,
    qkv_weight,
    qkv_bias,
    dense_weight,
    dense_bias,
    mlp_gain,
    mlp_shift,
    expand_weight,
    expand_bias,
    reduce_weight,
    reduce_bias,
    out_grad,
):
    seq_parts = lax.axis_size("seq")
    place = lax.axis_index("seq")
    rows, width = tokens.shape
    lengths = seq_lengths[0]
    starts = jnp.cumsum(lengths) - lengths
    row0 = place * rows
    offset = row0 - jnp.max(jnp.where(starts <= row0, starts, 0))
    flag = (offset > 0).astype(jnp.int32).reshape(1)
    positions = (offset + jnp.arange(rows, dtype=jnp.int32)).astype(F32)
    frequency = jnp.exp(jnp.arange(ROT // 2, dtype=F32) * (-2.0 * math.log(10000.0) / ROT))
    phases = frequency[:, None] * positions[None, :]
    ang = jnp.concatenate([jnp.cos(phases), jnp.sin(phases)], axis=0)

    row = lambda v: v.reshape(1, -1)
    ag, ash, mg, msh = row(attn_gain), row(attn_shift), row(mlp_gain), row(mlp_shift)
    onward = [(i, i + 1) for i in range(seq_parts - 1)]

    batch_parts = lax.axis_size("batch")
    ndev = batch_parts * seq_parts
    bits = batch_parts.bit_length() - 1
    q, kv, kvh, do, n1t, n2, n2t = project(
        tokens, ag, ash, mg, msh, qkv_weight, row(qkv_bias), ang, out_grad, dense_weight)
    kvp = lax.ppermute(kvh, "seq", onward)
    mid, slope, dwr, dog = mlp_fwd(
        ndev, n2, expand_weight, row(expand_bias), reduce_weight, out_grad)
    sg, dwe, dbe = mlp_back(n2t, expand_weight, reduce_weight, out_grad, slope)

    o, dq, dkv, dkvn, partw, partr, totw, totr = attend(bits, seq_parts, flag, q, kv, kvp, do, dwe, dwr)
    layer_out, dwd = dense(o, dense_weight, row(dense_bias), row(reduce_bias), mid, tokens, out_grad)
    input_grad, dw, dwd, dwe, dwr, vsum = tail(
        bits, seq_parts, tokens, ag, mg, n1t, qkv_weight, ang, dq, dkv, dkvn, out_grad, sg, dwd,
        partw, partr, dog, dbe)
    index = lax.axis_index("batch") * seq_parts + place
    sizes = (width, width, 3 * width, width, width, width, dbe.shape[1])
    input_grad, dw, dwd, dwe, dwr, *vectors = finish(
        index.astype(jnp.int32).reshape(1), ndev, sizes, input_grad, dw, dwd, totw, dwe, totr, dwr, vsum)
    dag, das, dqb, dog, dmg, dms, dbe = [v.reshape(-1) for v in vectors]
    return (
        layer_out,
        input_grad,
        dag,
        das,
        dw,
        dqb,
        dwd,
        dog,
        dmg,
        dms,
        dwe,
        dbe,
        dwr,
        dog,
    )


def solution(mesh):
    tok = P(("batch", "seq"), None)
    vec = P(("batch", "seq"))
    in_specs = (tok, P("batch", None)) + (P(),) * 12 + (tok,)
    out_specs = (tok, tok, vec, vec, tok, vec, tok, vec, vec, vec, tok, vec, tok, vec)
    return jax.shard_map(body, mesh=mesh, in_specs=in_specs, out_specs=out_specs, check_vma=False)
```

```python
from functools import partial
import math

import jax
import jax.numpy as jnp
from jax import lax
from jax.experimental import pallas as pl
from jax.experimental.pallas import tpu as pltpu
from jax.sharding import PartitionSpec as P

HEAD_DIM = 64
ROT = 16
PAIR = 2 * HEAD_DIM
EPSILON = 1e-05
MASKED = -1e30
SCALE = 1.0 / math.sqrt(HEAD_DIM)
QB = 256
FB = 1024
STEP_PAIRS = 2
ROWS = 128
F32 = jnp.float32
BF16 = jnp.bfloat16
VMEM_LIMIT = 60 << 20
MESH = pl.DeviceIdType.MESH


def dot(left, right):
    return jnp.dot(left, right, preferred_element_type=F32)


def dot_t(left, right):
    return lax.dot_general(left, right, (((1,), (1,)), ((), ())), preferred_element_type=F32)


def params():
    return pltpu.CompilerParams(vmem_limit_bytes=VMEM_LIMIT)


def cost(flops, nbytes):
    return pl.CostEstimate(flops=int(flops), bytes_accessed=int(nbytes), transcendentals=0)


def whole(shape):
    return pl.BlockSpec(shape, lambda i: (0,) * len(shape), pipeline_mode=pl.Buffered(1))


def statistics(x):
    mean = jnp.mean(x, axis=-1, keepdims=True)
    centered = x - mean
    variance = jnp.mean(centered * centered, axis=-1, keepdims=True)
    rstd = lax.rsqrt(variance + EPSILON)
    return centered * rstd, rstd


def row_block(i):
    return pl.ds(pl.multiple_of(i * ROWS, ROWS), ROWS)


def norm_rows(x_ref, gains, outs):
    def step(i, carry):
        rows = row_block(i)
        xn, _ = statistics(x_ref[rows, :].astype(F32))
        for (gain_ref, shift_ref), out_ref in zip(gains, outs):
            out_ref[rows, :] = (xn * gain_ref[...] + shift_ref[...]).astype(BF16)
        return carry

    lax.fori_loop(0, x_ref.shape[0] // ROWS, step, 0)


def norm_back(x_ref, gains, grads, gain_grads, shift_grads, emit, begin, end):
    if begin == 0:
        for ref in gain_grads + shift_grads:
            ref[...] = jnp.zeros_like(ref)

    def step(i, carry):
        rows = row_block(i)
        xn, rstd = statistics(x_ref[rows, :].astype(F32))
        scaled = 0.0
        for gain_ref, grad_ref, dgain_ref, dshift_ref in zip(gains, grads, gain_grads, shift_grads):
            grad = grad_ref[rows, :]
            dgain_ref[...] += jnp.sum(grad * xn, axis=0, keepdims=True)
            dshift_ref[...] += jnp.sum(grad, axis=0, keepdims=True)
            scaled = scaled + grad * gain_ref[...]
        mean_s = jnp.mean(scaled, axis=-1, keepdims=True)
        mean_sx = jnp.mean(scaled * xn, axis=-1, keepdims=True)
        emit(rows, rstd * (scaled - mean_s - xn * mean_sx))
        return carry

    lax.fori_loop(begin, end, step, 0)


def build_tables(angle_ref, tab_ref):
    half = ROT // 2
    cos8, sin8 = angle_ref[0:half, :], angle_ref[half:ROT, :]
    rest = HEAD_DIM - ROT
    count = cos8.shape[1]
    ones = jnp.ones((rest, count), F32)
    zeros = jnp.zeros((rest, count), F32)
    z8 = jnp.zeros_like(sin8)
    tab_ref[0] = jnp.concatenate([cos8, cos8, ones] * 2, axis=0).T
    tab_ref[1] = jnp.concatenate([-sin8, z8, zeros] * 2, axis=0).T
    tab_ref[2] = jnp.concatenate([z8, sin8, zeros] * 2, axis=0).T


def turn(u, tab_ref, sign):
    half = ROT // 2
    ahead = pltpu.roll(u, PAIR - half, 1)
    behind = pltpu.roll(u, half, 1)
    return u * tab_ref[0] + sign * (ahead * tab_ref[1] + behind * tab_ref[2])


def low_lanes(shape):
    return lax.broadcasted_iota(jnp.int32, shape, 1) < HEAD_DIM


def project_kernel(x_ref, gain_ref, shift_ref, gain2_ref, shift2_ref, w_ref, b_ref, ang_ref, og_ref,
                   wd_ref, q_ref, kv_ref, kvh_ref, do_ref, n1t_ref, n2_ref, n2t_ref,
                   norm, n1t, n2, n2t, tab, sem):
    saves = [pltpu.make_async_copy(src, dst, sem.at[n]) for n, (src, dst) in enumerate(
        ((n1t, n1t_ref), (n2, n2_ref), (n2t, n2t_ref)))]

    @pl.when(pl.program_id(0) == 0)
    def _():
        norm_rows(x_ref, ((gain_ref, shift_ref), (gain2_ref, shift2_ref)), (norm, n2))
        saves[1].start()
        n1t[...] = norm[...].T
        saves[0].start()
        n2t[...] = n2[...].T
        saves[2].start()
        build_tables(ang_ref, tab)

    for n in range(STEP_PAIRS):
        cols = slice(n * 3 * PAIR, (n + 1) * 3 * PAIR)
        mine = slice(n * PAIR, (n + 1) * PAIR)
        mixed = dot(norm[...], w_ref[:, cols]) + b_ref[:, cols]
        t0, t1, t2 = mixed[:, :PAIR], mixed[:, PAIR:2 * PAIR], mixed[:, 2 * PAIR:]
        low = low_lanes(t0.shape)
        q = jnp.where(low, t0, t1)
        k = pltpu.roll(jnp.where(low, t2, t0), HEAD_DIM, 1)
        v = jnp.where(low, t1, t2)
        q_ref[:, mine] = turn(q, tab, 1.0).astype(BF16)
        kv_ref[0, :, mine] = turn(k, tab, 1.0).astype(BF16)
        kv_ref[1, :, mine] = v.astype(BF16)
    do_ref[...] = dot_t(og_ref[...], wd_ref[...]).astype(BF16)

    @pl.when(pl.program_id(0) < pl.num_programs(0) // 2)
    def _():
        kvh_ref[...] = kv_ref[...]

    @pl.when(pl.program_id(0) == pl.num_programs(0) - 1)
    def _():
        for save in saves:
            save.wait()


def project(x, gain, shift, gain2, shift2, w, b, ang, og, wd):
    rows, width = x.shape
    wide = STEP_PAIRS * PAIR
    tok = pl.BlockSpec((rows, wide), lambda i: (0, i))
    return pl.pallas_call(
        project_kernel,
        grid=(width // wide,),
        out_shape=(
            jax.ShapeDtypeStruct((rows, width), BF16),
            jax.ShapeDtypeStruct((2, rows, width), BF16),
            jax.ShapeDtypeStruct((2, rows, width // 2), BF16),
            jax.ShapeDtypeStruct((rows, width), BF16),
            jax.ShapeDtypeStruct((width, rows), BF16),
            jax.ShapeDtypeStruct((rows, width), BF16),
            jax.ShapeDtypeStruct((width, rows), BF16),
        ),
        in_specs=[
            whole((rows, width)), *[whole((1, width))] * 4,
            pl.BlockSpec((width, 3 * wide), lambda i: (0, i)),
            pl.BlockSpec((1, 3 * wide), lambda i: (0, i)),
            whole(ang.shape), whole((rows, width)),
            pl.BlockSpec((wide, width), lambda i: (i, 0)),
        ],
        out_specs=(tok, pl.BlockSpec((2, rows, wide), lambda i: (0, 0, i)),
                   pl.BlockSpec((2, rows, wide), lambda i: (0, 0, jnp.minimum(i, width // wide // 2 - 1))), tok,
                   *[pl.BlockSpec(memory_space=pl.ANY)] * 3),
        scratch_shapes=[pltpu.VMEM((rows, width), BF16), pltpu.VMEM((width, rows), BF16),
                        pltpu.VMEM((rows, width), BF16), pltpu.VMEM((width, rows), BF16),
                        pltpu.VMEM((3, rows, PAIR), F32), pltpu.SemaphoreType.DMA((3,))],
        compiler_params=params(),
        cost_estimate=cost(8 * rows * width * width, 24 * rows * width),
        name="project",
    )(x, gain, shift, gain2, shift2, w, b, ang, og, wd)


def gelu_parts(h):
    z = jnp.abs(h) * math.sqrt(0.5)
    t = 1.0 / (1.0 + 0.5 * z)
    poly = jnp.full_like(t, 0.17087277)
    for c in (-0.82215223, 1.48851587, -1.13520398, 0.27886807, -0.18628806, 0.09678418,
              0.37409196, 1.00002368, -1.26551223):
        poly = poly * t + c
    zz = z * z
    tail = 0.5 * t * jnp.exp(poly - zz)
    cdf = jnp.where(h >= 0, 1.0 - tail, tail)
    slope = cdf + h * (jnp.exp(-zz) * (1.0 / math.sqrt(2.0 * math.pi)))
    return h * cdf, slope


def mlp_kernel(take, parts, n2_ref, n2t_ref, we_ref, be_ref, wr_ref, og_ref, kv_ref,
               mid_ref, dwr_ref, dog_ref, sg_ref, dwe_ref, dbe_ref, kvp_ref, slope, send_sem, recv_sem, fill_sem):
    step = pl.program_id(0)
    blocks = pl.num_programs(0) // 2
    width = n2_ref.shape[1]
    me_b, me_s = lax.axis_index("batch"), lax.axis_index("seq")
    first, last = me_s == 0, me_s == parts - 1
    onward = pltpu.make_async_remote_copy(
        src_ref=kv_ref, dst_ref=kvp_ref, send_sem=send_sem, recv_sem=recv_sem,
        device_id=(me_b, lax.rem(me_s + 1, parts)), device_id_type=MESH)

    @pl.when(step == 0)
    def _():
        sem = pltpu.get_barrier_semaphore()
        for d in range(1, parts):
            pl.semaphore_signal(sem, inc=1, device_id=(me_b, lax.rem(me_s + d, parts)), device_id_type=MESH)
        pl.semaphore_wait(sem, parts - 1)

        @pl.when(jnp.logical_not(last))
        def _():
            onward.start()

        @pl.when(first)
        def _():
            slope[0] = jnp.zeros(slope.shape[1:], BF16)
            fills = [pltpu.make_async_copy(slope.at[0, :, :kvp_ref.shape[2]], kvp_ref.at[n], fill_sem.at[n]) for n in range(2)]
            for fill in fills:
                fill.start()
            for fill in fills:
                fill.wait()

        mid_ref[...] = jnp.zeros_like(mid_ref)
        sg_ref[...] = jnp.zeros_like(sg_ref)
        dog_ref[...] = jnp.sum(og_ref[...].astype(F32), axis=0, keepdims=True)

    @pl.when(step < blocks)
    def _():
        h = dot(n2_ref[...], we_ref[...]) + be_ref[...]
        active, bend = gelu_parts(h)
        active = active.astype(BF16)
        slope[step] = bend.astype(BF16)
        mid_ref[...] += dot(active, wr_ref[...])
        dwr = dot(active.T, og_ref[...]).astype(BF16)
        ratio = dwr_ref.shape[1] // width
        for piece in range(FB // take):
            group, j = piece // ratio, piece % ratio
            dwr_ref[group * take:(group + 1) * take, j * width:(j + 1) * width] = (
                dwr[piece * take:(piece + 1) * take, :])

    @pl.when(step >= blocks)
    def _():
        hidden = (dot_t(og_ref[...], wr_ref[...]) * slope[step - blocks].astype(F32)).astype(BF16)
        dwe_ref[...] = dot(n2t_ref[...], hidden).astype(BF16)
        dbe_ref[...] = jnp.sum(hidden.astype(F32), axis=0, keepdims=True)
        sg_ref[...] += dot_t(hidden, we_ref[...])

    @pl.when(step == 2 * blocks - 1)
    def _():
        @pl.when(jnp.logical_not(last))
        def _():
            onward.wait_send()

        @pl.when(jnp.logical_not(first))
        def _():
            onward.wait_recv()


def mlp(ndev, parts, n2, n2t, we, be, wr, og, kv):
    rows, width = n2.shape
    hidden = we.shape[1]
    blocks = hidden // FB
    full, vec = whole((rows, width)), whole((1, width))
    gate = FB * width // hidden
    fshape, hbm = jax.ShapeDtypeStruct((rows, width), F32), pl.BlockSpec(memory_space=pl.ANY)
    early = lambda i: jnp.minimum(i, blocks - 1)
    late = lambda i: jnp.maximum(i - blocks, 0)
    return pl.pallas_call(
        partial(mlp_kernel, width // ndev, parts),
        grid=(2 * blocks,),
        out_shape=(fshape, jax.ShapeDtypeStruct((width, hidden), BF16), jax.ShapeDtypeStruct((1, width), F32),
                   fshape, jax.ShapeDtypeStruct((width, hidden), BF16), jax.ShapeDtypeStruct((1, hidden), F32),
                   jax.ShapeDtypeStruct(kv.shape, BF16)),
        in_specs=[full, whole(n2t.shape),
                  pl.BlockSpec((width, FB), lambda i: (0, lax.rem(i, blocks))),
                  pl.BlockSpec((1, FB), lambda i: (0, early(i))),
                  pl.BlockSpec((FB, width), lambda i: (lax.rem(i, blocks), 0)),
                  full, hbm],
        out_specs=(full, pl.BlockSpec((gate, hidden), lambda i: (early(i), 0)), vec, full,
                   pl.BlockSpec((width, FB), lambda i: (0, late(i))),
                   pl.BlockSpec((1, FB), lambda i: (0, late(i))), hbm),
        scratch_shapes=[pltpu.VMEM((blocks, rows, FB), BF16), pltpu.SemaphoreType.DMA,
                        pltpu.SemaphoreType.DMA, pltpu.SemaphoreType.DMA((2,))],
        compiler_params=pltpu.CompilerParams(
            vmem_limit_bytes=63 << 20, collective_id=2, has_side_effects=True),
        cost_estimate=cost(12 * rows * width * hidden, 8 * width * hidden),
        name="mlp",
    )(n2, n2t, we, be, wr, og, kv)


class Halving:
    def __init__(self, bits, parts, chunks, mats, own, recv, send_sem, recv_sem):
        self.bits, self.parts, self.chunks = bits, parts, chunks
        self.mats, self.own, self.recv = mats, own, recv
        self.send_sem, self.recv_sem = send_sem, recv_sem
        self.me_b, self.me_s = lax.axis_index("batch"), lax.axis_index("seq")
        self.bit = [lax.rem(self.me_b // (1 << k), 2) for k in range(bits)]
        self.mate = [
            (self.me_b + (1 << k) - 2 * (1 << k) * self.bit[k], self.me_s) for k in range(bits)]
        self.others = [(self.me_b, lax.rem(self.me_s + d, parts)) for d in range(1, parts)]
        self.peers = self.mate + self.others

    def barrier(self):
        sem = pltpu.get_barrier_semaphore()
        for peer in self.peers:
            pl.semaphore_signal(sem, inc=1, device_id=peer, device_id_type=MESH)
        pl.semaphore_wait(sem, len(self.peers))

    def copy(self, slot, n, src, dst, peer):
        return pltpu.make_async_remote_copy(
            src_ref=src, dst_ref=dst, send_sem=self.send_sem.at[slot, n],
            recv_sem=self.recv_sem.at[slot, n], device_id=peer, device_id_type=MESH)

    def dims(self, order, stage):
        return [d for d in range(self.bits - 1, -1, -1) if d not in order[:stage]]

    def part(self, c, value):
        mat, col, size, order = self.chunks[c]
        index = tuple(value if d == order[0] else slice(None) for d in self.dims(order, 0))
        return self.mats[mat].at[index + (slice(None), slice(None), pl.ds(col, size))]

    def copies(self, c, stage):
        order = self.chunks[c][3]
        if stage == self.bits:
            return [
                self.copy(c, self.bits + n, self.recv[c][stage - 1].at[peer[1]], self.recv[c][stage].at[n], peer)
                for n, peer in enumerate(self.others)]
        k = order[stage]
        if stage == 0:
            src = self.part(c, 1 - self.bit[k])
        else:
            index = tuple(1 - self.bit[k] if d == k else slice(None) for d in self.dims(order, stage))
            src = self.recv[c][stage - 1].at[index]
        return [self.copy(c, stage, src, self.recv[c][stage], self.mate[k])]

    def start(self, c, stage):
        for copy in self.copies(c, stage):
            copy.start()

    def wait_sends(self, c, stages):
        for stage in range(stages):
            for copy in self.copies(c, stage):
                copy.wait_send()

    def add(self, c, stage):
        mat, col, size, order = self.chunks[c]
        k = order[stage]
        dims = self.dims(order, stage)
        self.copies(c, stage)[0].wait_recv()
        dst = self.recv[c][stage]
        lead = self.bits - 1 - stage

        def one(i, carry):
            part = lax.rem(i, self.parts)
            rest = i // self.parts
            sub = tuple(lax.rem(rest // (1 << (lead - 1 - n)), 2) for n in range(lead))
            at = sub + (part,)
            left = list(sub)
            own_at = tuple(self.bit[k] if d == k else left.pop(0) for d in dims) + (part,)
            if stage > 0:
                own = self.recv[c][stage - 1][own_at]
            elif self.own is None:
                own = self.mats[mat][own_at + (slice(None), pl.ds(col, size))]
            else:
                own = self.own[c][at]
            dst[at] = own + dst[at]
            return carry

        lax.fori_loop(0, self.parts << lead, one, 0)

    def total(self, c):
        total = self.recv[c][self.bits - 1][self.me_s].astype(F32)
        for n, copy in enumerate(self.copies(c, self.bits)):
            copy.wait_recv()
            total = total + self.recv[c][self.bits][n].astype(F32)
        return total


def halving_orders(bits):
    plain = list(range(bits))
    other = [0] + [k for i in range(1, bits, 2) for k in reversed(range(i, min(i + 2, bits)))]
    return plain, other


def halving_scratch(bits, parts, rows, chunks, ends):
    scratch = []
    for (_, _, size, _), end in zip(chunks, ends):
        for stage in range(bits):
            scratch.append(pltpu.VMEM((2,) * (bits - 1 - stage) + (parts, rows, size), BF16))
        if end:
            scratch.append(pltpu.VMEM((parts - 1, rows, size), BF16))
    return scratch


def attend_pair(flag_ref, q_ref, kv_ref, kvp_ref, do_ref, o_ref, dq_ref, dkv_ref, dkvp_ref,
                pt, ds, kvt, qm, dom, midway):
    rows_all = q_ref.shape[0]
    nq = rows_all // QB
    away = (flag_ref[0] - 1).astype(F32) * (-MASKED)
    sources = [(kvp_ref, i) for i in range(nq)] + [(kv_ref, i) for i in range(nq)]

    def block(which, b):
        ref, i = sources[b]
        return ref[which, i * QB:(i + 1) * QB, :]

    for which in range(2):
        kvt[which, :, :rows_all] = kvp_ref[which].T
        kvt[which, :, rows_all:] = kv_ref[which].T
    lane = lax.broadcasted_iota(jnp.int32, (QB, PAIR), 1)
    sub = lax.broadcasted_iota(jnp.int32, (PAIR, QB), 0)
    causal = lax.broadcasted_iota(jnp.int32, (QB, QB), 0) <= lax.broadcasted_iota(
        jnp.int32, (QB, QB), 1)
    for j in range(nq):
        if j == nq // 2:
            midway()
        rows = slice(j * QB, (j + 1) * QB)
        q = q_ref[rows, :] * jnp.asarray(SCALE, BF16)
        qt = q.T
        dot_rows = do_ref[rows, :].astype(F32).T
        blocks = range(nq + j + 1)
        k1 = (nq + j + 1) * QB
        outs, scaled, dqs = [], [], []
        for h in range(2):
            hs = slice(h * HEAD_DIM, (h + 1) * HEAD_DIM)
            qm[h, rows, :] = jnp.where((lane < HEAD_DIM) == (h == 0), q, jnp.zeros_like(q))
            qtm = jnp.where((sub < HEAD_DIM) == (h == 0), qt, jnp.zeros_like(qt))
            scores, tops = [], [None, None]
            for b in blocks:
                s = dot(block(0, b), qtm)
                if b == nq + j:
                    s = jnp.where(causal, s, MASKED)
                scores.append(s)
                part = jnp.max(s.reshape(QB // 8, 8, QB), axis=0)
                side = int(b >= nq)
                tops[side] = part if tops[side] is None else jnp.maximum(tops[side], part)
            top = jnp.max(jnp.maximum(tops[0] + away, tops[1]), axis=0, keepdims=True)
            shift = (top - away, top)
            total = None
            for b, s in zip(blocks, scores):
                p = jnp.exp(s - shift[int(b >= nq)])
                part = jnp.sum(p.reshape(QB // 8, 8, QB), axis=0)
                total = part if total is None else total + part
                pt[h, b * QB:(b + 1) * QB, rows] = p.astype(BF16)
            inv = 1.0 / jnp.sum(total, axis=0, keepdims=True)
            out_t = dot(kvt[1, hs, :k1], pt[h, :k1, rows]) * inv
            dol_t = dot_rows[hs] * inv
            delta = jnp.sum(dol_t * out_t, axis=0, keepdims=True)
            outs.append(out_t)
            scaled.append(dol_t)
            zero = jnp.zeros((HEAD_DIM, QB), BF16)
            dol_b = dol_t.astype(BF16)
            dol_m = jnp.concatenate([dol_b, zero] if h == 0 else [zero, dol_b], axis=0)
            for b in blocks:
                dp = dot(block(1, b), dol_m)
                d = pt[h, b * QB:(b + 1) * QB, rows].astype(F32) * (dp - delta)
                ds[h, b * QB:(b + 1) * QB, rows] = d.astype(BF16)
            dqs.append(dot(kvt[0, hs, :k1], ds[h, :k1, rows]) * SCALE)
        o_ref[rows, :] = jnp.concatenate(outs, 0).T.astype(BF16)
        dq_ref[rows, :] = jnp.concatenate(dqs, 0).T.astype(BF16)
        dol = jnp.concatenate(scaled, 0).T.astype(BF16)
        for h in range(2):
            dom[h, rows, :] = jnp.where((lane < HEAD_DIM) == (h == 0), dol, jnp.zeros_like(dol))
    for b in range(2 * nq):
        q0 = max(0, b - nq) * QB
        br = slice(b * QB, (b + 1) * QB)
        dk = dot(ds[0, br, q0:], qm[0, q0:, :]) + dot(ds[1, br, q0:], qm[1, q0:, :])
        dv = dot(pt[0, br, q0:], dom[0, q0:, :]) + dot(pt[1, br, q0:], dom[1, q0:, :])
        ref, i = (dkvp_ref, b) if b < nq else (dkv_ref, b - nq)
        ref[0, i * QB:(i + 1) * QB, :] = dk.astype(BF16)
        ref[1, i * QB:(i + 1) * QB, :] = dv.astype(BF16)


def fold_rows(out_ref, total):
    take, width = total.shape[0], out_ref.shape[1]
    for j in range(total.shape[1] // width):
        out_ref[j * take:(j + 1) * take, :] = total[:, j * width:(j + 1) * width]


def attend_kernel(bits, parts, chunks, ends, flag_ref, q_ref, kv_ref, kv_hbm, kvp_hbm, do_ref, gw_ref, gr_ref,
                  o_ref, dq_ref, dkv_ref, dkvn_ref, partw_ref, partr_ref, totw_ref, totr_ref, *refs):
    nchunk = len(chunks)
    own, refs = refs[:nchunk], refs[nchunk:]
    recv = []
    for end in ends:
        recv.append(refs[:bits + end])
        refs = refs[bits + end:]
    (pt, ds, kvt, qm, dom, back, kvp, own_sem, send_sem, recv_sem, back_send, back_recv,
     kv_load, kv_send, kv_recv) = refs
    red = Halving(bits, parts, chunks, (gw_ref, gr_ref), own, recv, send_sem, recv_sem)
    step = pl.program_id(0)
    steps = dkvn_ref.shape[2] // PAIR

    def own_copy(c):
        return pltpu.make_async_copy(red.part(c, red.bit[chunks[c][3][0]]), own[c], own_sem.at[c])

    def back_copy(i):
        cols = pl.ds(pl.multiple_of(i * PAIR, PAIR), PAIR)
        return pltpu.make_async_remote_copy(
            src_ref=back.at[lax.rem(i, 2)], dst_ref=dkvn_ref.at[:, :, cols],
            send_sem=back_send.at[i], recv_sem=back_recv.at[i],
            device_id=red.others[parts - 2], device_id_type=MESH)

    first, last = red.me_s == 0, red.me_s == parts - 1
    half_steps = steps // 2

    def pair_cols(i):
        return pl.ds(pl.multiple_of(i * PAIR, PAIR), PAIR)

    def load_copy(i):
        return pltpu.make_async_copy(kvp_hbm.at[:, :, pair_cols(i)], kvp.at[i], kv_load.at[i])

    def onward_copy(i):
        return pltpu.make_async_remote_copy(
            src_ref=kv_hbm.at[:, :, pair_cols(i)], dst_ref=kvp.at[i],
            send_sem=kv_send.at[i - half_steps], recv_sem=kv_recv.at[i - half_steps],
            device_id=red.others[0], device_id_type=MESH)

    @pl.when(step == 0)
    def _():
        red.barrier()
        for i in range(half_steps):
            load_copy(i).start()
        for c in range(nchunk):
            red.start(c, 0)
            own_copy(c).start()

    @pl.when(jnp.logical_and(step == 0, jnp.logical_not(last)))
    def _():
        for i in range(half_steps, steps):
            onward_copy(i).start()

    @pl.when(jnp.logical_and(step == 0, first))
    def _():
        kvp[half_steps:] = jnp.zeros((steps - half_steps,) + kvp.shape[1:], BF16)

    moments = {}
    for c in range(nchunk):
        times = (2, 5, 7) if ends[c] else (5, 10, 13)
        for stage in range(bits):
            at = times[min(stage, 2)] + max(0, stage - 2)
            moments.setdefault(min(at * steps // 8, 2 * steps - 1), []).append((c, stage))

    def advance(half):
        for at, work in moments.items():
            if at % 2 == half:
                @pl.when(step == at // 2)
                def _(work=work):
                    for c, stage in work:
                        if stage == 0:
                            own_copy(c).wait()
                        red.add(c, stage)
                        if stage + 1 < bits + ends[c]:
                            red.start(c, stage + 1)

    slot = lax.rem(step, 2)

    @pl.when(jnp.logical_and(step == 0, last))
    def _():
        back[1] = jnp.zeros(back.shape[1:], BF16)
        fills = [pltpu.make_async_copy(back.at[1], dkvn_ref.at[:, :, pl.ds(i * PAIR, PAIR)], back_recv.at[i])
                 for i in range(steps)]
        for fill in fills:
            fill.start()
        for fill in fills:
            fill.wait()

    advance(0)

    @pl.when(jnp.logical_and(step >= 2, jnp.logical_not(first)))
    def _():
        back_copy(step - 2).wait_send()

    @pl.when(step < half_steps)
    def _():
        load_copy(step).wait()

    @pl.when(jnp.logical_and(step >= half_steps, jnp.logical_not(first)))
    def _():
        onward_copy(step).wait_recv()

    attend_pair(flag_ref, q_ref, kv_ref, kvp.at[step], do_ref, o_ref, dq_ref, dkv_ref,
                back.at[slot], pt, ds, kvt, qm, dom, lambda: advance(1))

    @pl.when(jnp.logical_not(first))
    def _():
        back_copy(step).start()

    @pl.when(step == steps - 1)
    def _():
        for c in range(nchunk):
            mat, col, size, _ = chunks[c]
            if not ends[c]:
                (partw_ref, partr_ref)[mat][...] = recv[c][bits - 1][...]
            red.wait_sends(c, bits + ends[c])
        for c in range(nchunk):
            mat, col, size, _ = chunks[c]
            if ends[c] and mat == 0:
                totw_ref[...] = red.total(c)
            elif ends[c]:
                fold_rows(totr_ref, red.total(c))

        @pl.when(jnp.logical_not(last))
        def _():
            for i in range(half_steps, steps):
                onward_copy(i).wait_send()

        @pl.when(jnp.logical_not(first))
        def _():
            for i in range(max(0, steps - 2), steps):
                back_copy(i).wait_send()

        @pl.when(jnp.logical_not(last))
        def _():
            for i in range(steps):
                back_copy(i).wait_recv()


def attend(bits, parts, flag, q, kv, kvp, do, gw, gr):
    rows, width = q.shape
    steps = width // PAIR
    hidden = gr.shape[1]
    take = gw.shape[0] // (parts << bits)
    shaped = [g.reshape((2,) * bits + (parts, take, g.shape[1])) for g in (gw, gr)]
    plain, other = halving_orders(bits)
    chunks = [(0, 0, hidden // 2, plain), (1, 0, hidden // 2, other),
              (0, hidden // 2, hidden // 2, plain), (1, hidden // 2, hidden // 2, other)]
    npeer = bits + parts - 1
    tok = pl.BlockSpec((rows, PAIR), lambda i: (0, i))
    kvs = pl.BlockSpec((2, rows, PAIR), lambda i: (0, 0, i))
    hbm = pl.BlockSpec(memory_space=pl.ANY)
    tok_shape = jax.ShapeDtypeStruct((rows, width), BF16)
    kv_shape = jax.ShapeDtypeStruct((2, rows, width), BF16)
    ends = (1, 1, 0, 0)
    part = (parts, take, hidden // 2)
    totw, totr = (take, hidden // 2), (take * hidden // 2 // width, width)
    return pl.pallas_call(
        partial(attend_kernel, bits, parts, chunks, ends),
        grid=(steps,),
        out_shape=(tok_shape, tok_shape, kv_shape, kv_shape,
                   jax.ShapeDtypeStruct(part, BF16), jax.ShapeDtypeStruct(part, BF16),
                   jax.ShapeDtypeStruct(totw, F32), jax.ShapeDtypeStruct(totr, F32)),
        in_specs=[pl.BlockSpec(memory_space=pltpu.SMEM), tok, kvs, hbm, hbm, tok, hbm, hbm],
        out_specs=(tok, tok, kvs, hbm, whole(part), whole(part), whole(totw), whole(totr)),
        scratch_shapes=[
            pltpu.VMEM((2,) * (bits - 1) + (parts, take, size), BF16) for _, _, size, _ in chunks
        ] + halving_scratch(bits, parts, take, chunks, ends) + [
            pltpu.VMEM((2, 2 * rows, rows), BF16),
            pltpu.VMEM((2, 2 * rows, rows), BF16),
            pltpu.VMEM((2, PAIR, 2 * rows), BF16),
            pltpu.VMEM((2, rows, PAIR), BF16),
            pltpu.VMEM((2, rows, PAIR), BF16),
            pltpu.VMEM((2, 2, rows, PAIR), BF16),
            pltpu.VMEM((steps, 2, rows, PAIR), BF16),
            pltpu.SemaphoreType.DMA((len(chunks),)),
            pltpu.SemaphoreType.DMA((len(chunks), npeer)),
            pltpu.SemaphoreType.DMA((len(chunks), npeer)),
            pltpu.SemaphoreType.DMA((steps,)),
            pltpu.SemaphoreType.DMA((steps,)),
            pltpu.SemaphoreType.DMA((steps // 2,)),
            pltpu.SemaphoreType.DMA((steps - steps // 2,)),
            pltpu.SemaphoreType.DMA((steps - steps // 2,)),
        ],
        compiler_params=pltpu.CompilerParams(
            vmem_limit_bytes=63 << 20, collective_id=1, has_side_effects=True),
        cost_estimate=cost(60 * rows * rows * width, 20 * rows * width),
        name="attend",
    )(flag, q, kv, kv, kvp, do, *shaped)


def dense_kernel(o_ref, wd_ref, db_ref, rb_ref, mid_ref, x_ref, og_ref, out_ref, dwd_ref, ot):
    @pl.when(pl.program_id(0) == 0)
    def _():
        ot[...] = o_ref[...].T

    total = x_ref[...].astype(F32) + mid_ref[...] + (db_ref[...] + rb_ref[...])
    out_ref[...] = (total + dot(o_ref[...], wd_ref[...])).astype(BF16)
    dwd_ref[...] = dot(ot[...], og_ref[...]).astype(BF16)


def dense(o, wd, db, rb, mid, x, og):
    rows, width = x.shape
    blk = 256
    col = lambda r: pl.BlockSpec((r, blk), lambda i: (0, i))
    return pl.pallas_call(
        dense_kernel,
        grid=(width // blk,),
        out_shape=(jax.ShapeDtypeStruct((rows, width), BF16), jax.ShapeDtypeStruct((width, width), BF16)),
        in_specs=[whole(o.shape), col(width), col(1), col(1), col(rows), col(rows), col(rows)],
        out_specs=(col(rows), col(width)),
        scratch_shapes=[pltpu.VMEM((width, rows), BF16)],
        compiler_params=params(),
        cost_estimate=cost(4 * rows * width * width, 12 * rows * width),
        name="dense",
    )(o, wd, db, rb, mid, x, og)


def tail_kernel(bits, parts, chunks, x_ref, gain_ref, gain2_ref, norm_t, w_ref, ang_ref, dq_ref, dkv_ref,
                dkvn_ref, og_ref, sg_ref, dwd_ref, partw_ref, partr_ref, dog_ref, dbe_ref,
                ig_ref, dw_out, dwd_out, dwe_out, dwr_out, vec_out, *refs):
    nchunk = len(chunks)
    recv = [refs[c * (bits + 1):(c + 1) * (bits + 1)] for c in range(nchunk)]
    (tab, fg, dw, db, dgain, dshift, dgain2, dshift2, zw, zr, state, vrecv, send_sem, recv_sem) = refs[
        nchunk * (bits + 1):]
    red = Halving(bits, parts, chunks, (dw, dwd_ref), None, recv, send_sem, recv_sem)
    step = pl.program_id(0)
    steps = pl.num_programs(0)
    width = x_ref.shape[1]
    nstep = width // (STEP_PAIRS * PAIR)
    cols = 3 * STEP_PAIRS * PAIR

    done = set()

    def forward(c, stage):
        if (c, stage) not in done:
            done.add((c, stage))
            red.add(c, stage)
            red.start(c, stage + 1)

    def z_copies():
        return [red.copy(nchunk + 1 + m, bits + n, part.at[peer[1]], dst.at[n], peer)
                for m, (part, dst) in enumerate(((partw_ref, zw), (partr_ref, zr)))
                for n, peer in enumerate(red.others)]

    @pl.when(step == 0)
    def _():
        red.barrier()
        for copy in z_copies():
            copy.start()
        for c in range(nstep, nchunk):
            red.start(c, 0)
        build_tables(ang_ref, tab)
        fg[...] = jnp.zeros_like(fg)

    for c in range(1, nstep):
        @pl.when(step == c)
        def _(c=c):
            red.start(c - 1, 0)
            if c == 1:
                for extra in range(nstep, nchunk):
                    forward(extra, 0)
            else:
                forward(c - 2, 0)
            if c == nstep - 1:
                for extra in range(nstep, nchunk):
                    forward(extra, 1)

    blocks = []
    for n in range(STEP_PAIRS):
        mine = slice(n * PAIR, (n + 1) * PAIR)
        dq = turn(dq_ref[:, mine].astype(F32), tab, -1.0)
        dk = turn(dkv_ref[0, :, mine].astype(F32) + dkvn_ref[0, :, mine].astype(F32), tab, -1.0)
        dv = dkv_ref[1, :, mine].astype(F32) + dkvn_ref[1, :, mine].astype(F32)
        low = low_lanes(dq.shape)
        dk = pltpu.roll(dk, HEAD_DIM, 1)
        blocks += [jnp.where(low, dq, dk), jnp.where(low, dv, dq), jnp.where(low, dk, dv)]
    dm = jnp.concatenate(blocks, axis=1).astype(BF16)
    at = pl.ds(pl.multiple_of(step * cols, cols), cols)
    db[:, at] = jnp.sum(dm.astype(F32), axis=0, keepdims=True)
    dw[(slice(None),) * (bits + 2) + (at,)] = dot(norm_t[...], dm).reshape(
        dw.shape[:-1] + (cols,)).astype(BF16)
    fg[...] += dot_t(dm, w_ref[...])

    def vec_copies(stage):
        if stage < bits:
            return [red.copy(nchunk, stage, state.at[stage], vrecv.at[stage], red.mate[stage])]
        return [red.copy(nchunk, bits + n, state.at[bits], vrecv.at[bits + n], peer)
                for n, peer in enumerate(red.others)]

    def vec_start(stage):
        for copy in vec_copies(stage):
            copy.start()

    def vec_add(stage):
        copies = vec_copies(stage)
        for copy in copies:
            copy.wait_recv()
        total = state[stage]
        for n in range(len(copies)):
            total = total + vrecv[stage + n]
        if stage < bits:
            state[stage + 1] = total
            vec_start(stage + 1)
        else:
            vec_out[...] = total

    @pl.when(step == steps - 1)
    def _():
        red.start(nstep - 1, 0)
        forward(nstep - 2, 0)

        def emit(rows, part):
            ig_ref[rows, :] = (og_ref[rows, :].astype(F32) + part).astype(BF16)

        forward(nstep - 1, 0)
        forward(0, 1)
        norm_args = (x_ref, (gain_ref, gain2_ref), (fg, sg_ref), (dgain, dgain2), (dshift, dshift2), emit)
        row_blocks = x_ref.shape[0] // ROWS
        norm_back(*norm_args, 0, row_blocks // 2)
        forward(1, 1)
        for extra in range(nstep, nchunk):
            forward(extra, 2)
        norm_back(*norm_args, row_blocks // 2, row_blocks)
        begin = 0
        for ref in (dgain, dshift, db, dog_ref, dgain2, dshift2, dbe_ref):
            state[0, :, begin:begin + ref.shape[1]] = ref[...]
            begin += ref.shape[1]
        vec_start(0)
        order = list(range(nstep, nchunk)) + list(range(nstep))
        for stage in range(1, bits):
            for c in order:
                forward(c, stage)
            vec_add(stage - 1)
        copies = z_copies()
        for m, (part, got, out) in enumerate(((partw_ref, zw, dwe_out), (partr_ref, zr, dwr_out))):
            total = part[red.me_s].astype(F32)
            for n in range(parts - 1):
                copies[m * (parts - 1) + n].wait_recv()
                total = total + got[n].astype(F32)
            if m == 0:
                out[...] = total
            else:
                fold_rows(out, total)
        vec_add(bits - 1)
        for c in order:
            mat, col, size, _ = chunks[c]
            (dw_out, dwd_out)[mat][:, col:col + size] = red.total(c)
        vec_add(bits)
        for c in range(nchunk):
            red.wait_sends(c, bits + 1)
        for copy in copies:
            copy.wait_send()
        for stage in range(bits + 1):
            for copy in vec_copies(stage):
                copy.wait_send()


def tail(bits, parts, x, gain, gain2, norm_t, w, ang, dq, dkv, dkvn, og, sg, dwd, partw, partr, dog, dbe):
    rows, width = x.shape
    full, vec = whole((rows, width)), whole((1, width))
    wide = STEP_PAIRS * PAIR
    cols = 3 * wide
    nstep = width // wide
    hidden, part = dbe.shape[1], partw.shape[2]
    take = width // (parts << bits)
    total = 5 * width + 3 * width + hidden
    npeer = bits + parts - 1
    lead = (2,) * bits + (parts, take)
    plain, other = halving_orders(bits)
    chunks = [(0, n * cols, cols, other if n % 2 else plain) for n in range(nstep)]
    chunks += [(1, n * (width // 2), width // 2, other if n % 2 else plain) for n in range(2)]
    tok = pl.BlockSpec((rows, wide), lambda i: (0, i))
    kvs = pl.BlockSpec((2, rows, wide), lambda i: (0, 0, i))
    up = pl.BlockSpec((width, cols), lambda i: (0, i))
    dwd = dwd.reshape(lead + (width,))
    outs = [((rows, width), BF16), ((take, 3 * width), F32), ((take, width), F32), ((take, part), F32),
            ((take * part // width, width), F32), ((1, total), F32)]
    row_vec = pltpu.VMEM((1, width), F32)
    nsem = (len(chunks) + 3, npeer)
    return pl.pallas_call(
        partial(tail_kernel, bits, parts, chunks),
        grid=(nstep,),
        out_shape=tuple(jax.ShapeDtypeStruct(s, d) for s, d in outs),
        in_specs=[full, vec, vec, whole(norm_t.shape), up, whole(ang.shape), tok, kvs, kvs, full, full,
                  whole(dwd.shape), whole(partw.shape), whole(partr.shape), vec, whole(dbe.shape)],
        out_specs=tuple(whole(s) for s, _ in outs),
        scratch_shapes=halving_scratch(bits, parts, take, chunks, [1] * len(chunks)) + [
            pltpu.VMEM((3, rows, PAIR), F32), pltpu.VMEM((rows, width), F32),
            pltpu.VMEM(lead + (3 * width,), BF16), pltpu.VMEM((1, 3 * width), F32),
            row_vec, row_vec, row_vec, row_vec,
            pltpu.VMEM((parts - 1, take, part), BF16), pltpu.VMEM((parts - 1, take, part), BF16),
            pltpu.VMEM((bits + 1, 1, total), F32), pltpu.VMEM((npeer, 1, total), F32),
            pltpu.SemaphoreType.DMA(nsem), pltpu.SemaphoreType.DMA(nsem),
        ],
        compiler_params=pltpu.CompilerParams(
            vmem_limit_bytes=63 << 20, collective_id=0, has_side_effects=True),
        cost_estimate=cost(12 * rows * width * width, 8 * rows * width),
        name="tail",
    )(x, gain, gain2, norm_t, w, ang, dq, dkv, dkvn, og, sg, dwd, partw, partr, dog, dbe)


def finish_kernel(sizes, index_ref, ig_ref, dw_ref, dwd_ref, dwe0_ref, dwe1_ref, dwr0_ref, dwr1_ref, vec_ref,
                  ig_out, dw_out, dwd_out, dwe_out, dwr_out, *outs):
    for src, dst in ((ig_ref, ig_out), (dw_ref, dw_out), (dwd_ref, dwd_out)):
        dst[...] = src[...]
    half = dwe0_ref.shape[1]
    dwe_out[:, :half] = dwe0_ref[...]
    dwe_out[:, half:] = dwe1_ref[...]
    half = dwr0_ref.shape[0]
    dwr_out[:half, :] = dwr0_ref[...]
    dwr_out[half:, :] = dwr1_ref[...]
    at = 0
    for size, out in zip(sizes, outs):
        own = out.shape[1]
        row = jnp.broadcast_to(vec_ref[:, at:at + size], (8, size))
        out[...] = pltpu.roll(row, lax.rem(size - index_ref[0] * own, size), 1)[:1, :own]
        at += size


def finish(index, ndev, sizes, ig, dw, dwd, dwe0, dwe1, dwr0, dwr1, vec):
    mats = (ig, dw, dwd, dwe0, dwe1, dwr0, dwr1)
    outs = [(m.shape, m.dtype) for m in (ig, dw, dwd)] + [
        ((dwe0.shape[0], 2 * dwe0.shape[1]), F32), ((2 * dwr0.shape[0], dwr0.shape[1]), F32)]
    outs += [((1, n // ndev), F32) for n in sizes]
    return pl.pallas_call(
        partial(finish_kernel, sizes),
        out_shape=tuple(jax.ShapeDtypeStruct(s, d) for s, d in outs),
        grid=(1,),
        in_specs=[pl.BlockSpec(memory_space=pltpu.SMEM)] + [whole(m.shape) for m in mats] + [whole(vec.shape)],
        out_specs=tuple(whole(s) for s, _ in outs),
        compiler_params=params(),
        name="finish",
    )(index, *mats, vec)


def body(
    tokens,
    seq_lengths,
    attn_gain,
    attn_shift,
    qkv_weight,
    qkv_bias,
    dense_weight,
    dense_bias,
    mlp_gain,
    mlp_shift,
    expand_weight,
    expand_bias,
    reduce_weight,
    reduce_bias,
    out_grad,
):
    seq_parts = lax.axis_size("seq")
    place = lax.axis_index("seq")
    rows, width = tokens.shape
    lengths = seq_lengths[0]
    starts = jnp.cumsum(lengths) - lengths
    row0 = place * rows
    offset = row0 - jnp.max(jnp.where(starts <= row0, starts, 0))
    flag = (offset > 0).astype(jnp.int32).reshape(1)
    positions = (offset + jnp.arange(rows, dtype=jnp.int32)).astype(F32)
    frequency = jnp.exp(jnp.arange(ROT // 2, dtype=F32) * (-2.0 * math.log(10000.0) / ROT))
    phases = frequency[:, None] * positions[None, :]
    ang = jnp.concatenate([jnp.cos(phases), jnp.sin(phases)], axis=0)

    row = lambda v: v.reshape(1, -1)
    ag, ash, mg, msh = row(attn_gain), row(attn_shift), row(mlp_gain), row(mlp_shift)

    batch_parts = lax.axis_size("batch")
    ndev = batch_parts * seq_parts
    bits = batch_parts.bit_length() - 1
    q, kv, kvh, do, n1t, n2, n2t = project(
        tokens, ag, ash, mg, msh, qkv_weight, row(qkv_bias), ang, out_grad, dense_weight)
    mid, dwr, dog, sg, dwe, dbe, kvp = mlp(
        ndev, seq_parts, n2, n2t, expand_weight, row(expand_bias), reduce_weight, out_grad, kvh)
    o, dq, dkv, dkvn, partw, partr, totw, totr = attend(bits, seq_parts, flag, q, kv, kvp, do, dwe, dwr)
    layer_out, dwd = dense(o, dense_weight, row(dense_bias), row(reduce_bias), mid, tokens, out_grad)
    input_grad, dw, dwd, dwe, dwr, vsum = tail(
        bits, seq_parts, tokens, ag, mg, n1t, qkv_weight, ang, dq, dkv, dkvn, out_grad, sg, dwd,
        partw, partr, dog, dbe)
    index = lax.axis_index("batch") * seq_parts + place
    sizes = (width, width, 3 * width, width, width, width, dbe.shape[1])
    input_grad, dw, dwd, dwe, dwr, *vectors = finish(
        index.astype(jnp.int32).reshape(1), ndev, sizes, input_grad, dw, dwd, totw, dwe, totr, dwr, vsum)
    dag, das, dqb, dog, dmg, dms, dbe = [v.reshape(-1) for v in vectors]
    return (
        layer_out,
        input_grad,
        dag,
        das,
        dw,
        dqb,
        dwd,
        dog,
        dmg,
        dms,
        dwe,
        dbe,
        dwr,
        dog,
    )


def solution(mesh):
    tok = P(("batch", "seq"), None)
    vec = P(("batch", "seq"))
    in_specs = (tok, P("batch", None)) + (P(),) * 12 + (tok,)
    out_specs = (tok, tok, vec, vec, tok, vec, tok, vec, vec, vec, tok, vec, tok, vec)
    return jax.shard_map(body, mesh=mesh, in_specs=in_specs, out_specs=out_specs, check_vma=False)
```

```python
from functools import partial
import math

import jax
import jax.numpy as jnp
from jax import lax
from jax.experimental import pallas as pl
from jax.experimental.pallas import tpu as pltpu
from jax.sharding import PartitionSpec as P

HEAD_DIM = 64
ROT = 16
PAIR = 2 * HEAD_DIM
EPSILON = 1e-05
MASKED = -1e30
SCALE = 1.0 / math.sqrt(HEAD_DIM)
QB = 256
FB = 1024
STEP_PAIRS = 2
ROWS = 128
F32 = jnp.float32
BF16 = jnp.bfloat16
VMEM_LIMIT = 60 << 20
MESH = pl.DeviceIdType.MESH


def dot(left, right):
    return jnp.dot(left, right, preferred_element_type=F32)


def dot_t(left, right):
    return lax.dot_general(left, right, (((1,), (1,)), ((), ())), preferred_element_type=F32)


def params():
    return pltpu.CompilerParams(vmem_limit_bytes=VMEM_LIMIT)


def cost(flops, nbytes):
    return pl.CostEstimate(flops=int(flops), bytes_accessed=int(nbytes), transcendentals=0)


def whole(shape):
    return pl.BlockSpec(shape, lambda i: (0,) * len(shape), pipeline_mode=pl.Buffered(1))


def statistics(x):
    mean = jnp.mean(x, axis=-1, keepdims=True)
    centered = x - mean
    variance = jnp.mean(centered * centered, axis=-1, keepdims=True)
    rstd = lax.rsqrt(variance + EPSILON)
    return centered * rstd, rstd


def row_block(i):
    return pl.ds(pl.multiple_of(i * ROWS, ROWS), ROWS)


def norm_rows(x_ref, gains, outs):
    def step(i, carry):
        rows = row_block(i)
        xn, _ = statistics(x_ref[rows, :].astype(F32))
        for (gain_ref, shift_ref), out_ref in zip(gains, outs):
            out_ref[rows, :] = (xn * gain_ref[...] + shift_ref[...]).astype(BF16)
        return carry

    lax.fori_loop(0, x_ref.shape[0] // ROWS, step, 0)


def norm_back(x_ref, gains, grads, gain_grads, shift_grads, emit, begin, end):
    if begin == 0:
        for ref in gain_grads + shift_grads:
            ref[...] = jnp.zeros_like(ref)

    def step(i, carry):
        rows = row_block(i)
        xn, rstd = statistics(x_ref[rows, :].astype(F32))
        scaled = 0.0
        for gain_ref, grad_ref, dgain_ref, dshift_ref in zip(gains, grads, gain_grads, shift_grads):
            grad = grad_ref[rows, :]
            dgain_ref[...] += jnp.sum(grad * xn, axis=0, keepdims=True)
            dshift_ref[...] += jnp.sum(grad, axis=0, keepdims=True)
            scaled = scaled + grad * gain_ref[...]
        mean_s = jnp.mean(scaled, axis=-1, keepdims=True)
        mean_sx = jnp.mean(scaled * xn, axis=-1, keepdims=True)
        emit(rows, rstd * (scaled - mean_s - xn * mean_sx))
        return carry

    lax.fori_loop(begin, end, step, 0)


def build_tables(angle_ref, tab_ref):
    half = ROT // 2
    cos8, sin8 = angle_ref[0:half, :], angle_ref[half:ROT, :]
    rest = HEAD_DIM - ROT
    count = cos8.shape[1]
    ones = jnp.ones((rest, count), F32)
    zeros = jnp.zeros((rest, count), F32)
    z8 = jnp.zeros_like(sin8)
    tab_ref[0] = jnp.concatenate([cos8, cos8, ones] * 2, axis=0).T
    tab_ref[1] = jnp.concatenate([-sin8, z8, zeros] * 2, axis=0).T
    tab_ref[2] = jnp.concatenate([z8, sin8, zeros] * 2, axis=0).T


def turn(u, tab_ref, sign):
    half = ROT // 2
    ahead = pltpu.roll(u, PAIR - half, 1)
    behind = pltpu.roll(u, half, 1)
    return u * tab_ref[0] + sign * (ahead * tab_ref[1] + behind * tab_ref[2])


def low_lanes(shape):
    return lax.broadcasted_iota(jnp.int32, shape, 1) < HEAD_DIM


def project_kernel(x_ref, gain_ref, shift_ref, gain2_ref, shift2_ref, w_ref, b_ref, ang_ref, og_ref,
                   wd_ref, q_ref, kv_ref, kvh_ref, do_ref, n1t_ref, n2_ref, n2t_ref,
                   norm, n1t, n2, n2t, tab, sem):
    saves = [pltpu.make_async_copy(src, dst, sem.at[n]) for n, (src, dst) in enumerate(
        ((n1t, n1t_ref), (n2, n2_ref), (n2t, n2t_ref)))]

    @pl.when(pl.program_id(0) == 0)
    def _():
        norm_rows(x_ref, ((gain_ref, shift_ref), (gain2_ref, shift2_ref)), (norm, n2))
        saves[1].start()
        n1t[...] = norm[...].T
        saves[0].start()
        n2t[...] = n2[...].T
        saves[2].start()
        build_tables(ang_ref, tab)

    for n in range(STEP_PAIRS):
        cols = slice(n * 3 * PAIR, (n + 1) * 3 * PAIR)
        mine = slice(n * PAIR, (n + 1) * PAIR)
        mixed = dot(norm[...], w_ref[:, cols]) + b_ref[:, cols]
        t0, t1, t2 = mixed[:, :PAIR], mixed[:, PAIR:2 * PAIR], mixed[:, 2 * PAIR:]
        low = low_lanes(t0.shape)
        q = jnp.where(low, t0, t1)
        k = pltpu.roll(jnp.where(low, t2, t0), HEAD_DIM, 1)
        v = jnp.where(low, t1, t2)
        q_ref[:, mine] = turn(q, tab, 1.0).astype(BF16)
        kv_ref[0, :, mine] = turn(k, tab, 1.0).astype(BF16)
        kv_ref[1, :, mine] = v.astype(BF16)
    do_ref[...] = dot_t(og_ref[...], wd_ref[...]).astype(BF16)

    @pl.when(pl.program_id(0) < pl.num_programs(0) // 2)
    def _():
        kvh_ref[...] = kv_ref[...]

    @pl.when(pl.program_id(0) == pl.num_programs(0) - 1)
    def _():
        for save in saves:
            save.wait()


def project(x, gain, shift, gain2, shift2, w, b, ang, og, wd):
    rows, width = x.shape
    wide = STEP_PAIRS * PAIR
    tok = pl.BlockSpec((rows, wide), lambda i: (0, i))
    return pl.pallas_call(
        project_kernel,
        grid=(width // wide,),
        out_shape=(
            jax.ShapeDtypeStruct((rows, width), BF16),
            jax.ShapeDtypeStruct((2, rows, width), BF16),
            jax.ShapeDtypeStruct((2, rows, width // 2), BF16),
            jax.ShapeDtypeStruct((rows, width), BF16),
            jax.ShapeDtypeStruct((width, rows), BF16),
            jax.ShapeDtypeStruct((rows, width), BF16),
            jax.ShapeDtypeStruct((width, rows), BF16),
        ),
        in_specs=[
            whole((rows, width)), *[whole((1, width))] * 4,
            pl.BlockSpec((width, 3 * wide), lambda i: (0, i)),
            pl.BlockSpec((1, 3 * wide), lambda i: (0, i)),
            whole(ang.shape), whole((rows, width)),
            pl.BlockSpec((wide, width), lambda i: (i, 0)),
        ],
        out_specs=(tok, pl.BlockSpec((2, rows, wide), lambda i: (0, 0, i)),
                   pl.BlockSpec((2, rows, wide), lambda i: (0, 0, jnp.minimum(i, width // wide // 2 - 1))), tok,
                   *[pl.BlockSpec(memory_space=pl.ANY)] * 3),
        scratch_shapes=[pltpu.VMEM((rows, width), BF16), pltpu.VMEM((width, rows), BF16),
                        pltpu.VMEM((rows, width), BF16), pltpu.VMEM((width, rows), BF16),
                        pltpu.VMEM((3, rows, PAIR), F32), pltpu.SemaphoreType.DMA((3,))],
        compiler_params=params(),
        cost_estimate=cost(8 * rows * width * width, 24 * rows * width),
        name="project",
    )(x, gain, shift, gain2, shift2, w, b, ang, og, wd)


LOG2E = 1.0 / math.log(2.0)
TAIL = (0.17087277, -0.82215223, 1.48851587, -1.13520398, 0.27886807, -0.18628806, 0.09678418,
        0.37409196, 1.00002368, -1.26551223 - math.log(2.0))


def gelu_parts(h):
    t = 1.0 / (1.0 + (0.5 * math.sqrt(0.5)) * jnp.abs(h))
    poly = TAIL[0] * LOG2E
    for c in TAIL[1:]:
        poly = poly * t + c * LOG2E
    fall = (h * h) * (-0.5 * LOG2E)
    tail = t * jnp.exp2(poly + fall)
    cdf = jnp.where(h >= 0, 1.0 - tail, tail)
    slope = cdf + (h * (1.0 / math.sqrt(2.0 * math.pi))) * jnp.exp2(fall)
    return h * cdf, slope


def mlp_kernel(take, parts, n2_ref, n2t_ref, we_ref, be_ref, wr_ref, og_ref, kv_ref,
               mid_ref, dwr_ref, dog_ref, sg_ref, dwe_ref, dbe_ref, kvp_ref, slope, send_sem, recv_sem, fill_sem):
    step = pl.program_id(0)
    blocks = pl.num_programs(0) // 2
    width = n2_ref.shape[1]
    me_b, me_s = lax.axis_index("batch"), lax.axis_index("seq")
    first, last = me_s == 0, me_s == parts - 1
    onward = pltpu.make_async_remote_copy(
        src_ref=kv_ref, dst_ref=kvp_ref, send_sem=send_sem, recv_sem=recv_sem,
        device_id=(me_b, lax.rem(me_s + 1, parts)), device_id_type=MESH)

    @pl.when(step == 0)
    def _():
        sem = pltpu.get_barrier_semaphore()
        for d in range(1, parts):
            pl.semaphore_signal(sem, inc=1, device_id=(me_b, lax.rem(me_s + d, parts)), device_id_type=MESH)
        pl.semaphore_wait(sem, parts - 1)

        @pl.when(jnp.logical_not(last))
        def _():
            onward.start()

        @pl.when(first)
        def _():
            slope[0] = jnp.zeros(slope.shape[1:], BF16)
            fills = [pltpu.make_async_copy(slope.at[0, :, :kvp_ref.shape[2]], kvp_ref.at[n], fill_sem.at[n]) for n in range(2)]
            for fill in fills:
                fill.start()
            for fill in fills:
                fill.wait()

        mid_ref[...] = jnp.zeros_like(mid_ref)
        sg_ref[...] = jnp.zeros_like(sg_ref)
        dog_ref[...] = jnp.sum(og_ref[...].astype(F32), axis=0, keepdims=True)

    @pl.when(step < blocks)
    def _():
        h = dot(n2_ref[...], we_ref[...]) + be_ref[...]
        active, bend = gelu_parts(h)
        active = active.astype(BF16)
        slope[step] = bend.astype(BF16)
        mid_ref[...] += dot(active, wr_ref[...])
        dwr = dot(active.T, og_ref[...]).astype(BF16)
        ratio = dwr_ref.shape[1] // width
        for piece in range(FB // take):
            group, j = piece // ratio, piece % ratio
            dwr_ref[group * take:(group + 1) * take, j * width:(j + 1) * width] = (
                dwr[piece * take:(piece + 1) * take, :])

    @pl.when(step >= blocks)
    def _():
        hidden = (dot_t(og_ref[...], wr_ref[...]) * slope[step - blocks].astype(F32)).astype(BF16)
        dwe_ref[...] = dot(n2t_ref[...], hidden).astype(BF16)
        dbe_ref[...] = jnp.sum(hidden.astype(F32), axis=0, keepdims=True)
        sg_ref[...] += dot_t(hidden, we_ref[...])

    @pl.when(step == 2 * blocks - 1)
    def _():
        @pl.when(jnp.logical_not(last))
        def _():
            onward.wait_send()

        @pl.when(jnp.logical_not(first))
        def _():
            onward.wait_recv()


def mlp(ndev, parts, n2, n2t, we, be, wr, og, kv):
    rows, width = n2.shape
    hidden = we.shape[1]
    blocks = hidden // FB
    full, vec = whole((rows, width)), whole((1, width))
    gate = FB * width // hidden
    fshape, hbm = jax.ShapeDtypeStruct((rows, width), F32), pl.BlockSpec(memory_space=pl.ANY)
    early = lambda i: jnp.minimum(i, blocks - 1)
    late = lambda i: jnp.maximum(i - blocks, 0)
    return pl.pallas_call(
        partial(mlp_kernel, width // ndev, parts),
        grid=(2 * blocks,),
        out_shape=(fshape, jax.ShapeDtypeStruct((width, hidden), BF16), jax.ShapeDtypeStruct((1, width), F32),
                   fshape, jax.ShapeDtypeStruct((width, hidden), BF16), jax.ShapeDtypeStruct((1, hidden), F32),
                   jax.ShapeDtypeStruct(kv.shape, BF16)),
        in_specs=[full, whole(n2t.shape),
                  pl.BlockSpec((width, FB), lambda i: (0, lax.rem(i, blocks))),
                  pl.BlockSpec((1, FB), lambda i: (0, early(i))),
                  pl.BlockSpec((FB, width), lambda i: (lax.rem(i, blocks), 0)),
                  full, hbm],
        out_specs=(full, pl.BlockSpec((gate, hidden), lambda i: (early(i), 0)), vec, full,
                   pl.BlockSpec((width, FB), lambda i: (0, late(i))),
                   pl.BlockSpec((1, FB), lambda i: (0, late(i))), hbm),
        scratch_shapes=[pltpu.VMEM((blocks, rows, FB), BF16), pltpu.SemaphoreType.DMA,
                        pltpu.SemaphoreType.DMA, pltpu.SemaphoreType.DMA((2,))],
        compiler_params=pltpu.CompilerParams(
            vmem_limit_bytes=63 << 20, collective_id=2, has_side_effects=True),
        cost_estimate=cost(12 * rows * width * hidden, 8 * width * hidden),
        name="mlp",
    )(n2, n2t, we, be, wr, og, kv)


class Halving:
    def __init__(self, bits, parts, chunks, mats, own, recv, send_sem, recv_sem):
        self.bits, self.parts, self.chunks = bits, parts, chunks
        self.mats, self.own, self.recv = mats, own, recv
        self.send_sem, self.recv_sem = send_sem, recv_sem
        self.me_b, self.me_s = lax.axis_index("batch"), lax.axis_index("seq")
        self.bit = [lax.rem(self.me_b // (1 << k), 2) for k in range(bits)]
        self.mate = [
            (self.me_b + (1 << k) - 2 * (1 << k) * self.bit[k], self.me_s) for k in range(bits)]
        self.others = [(self.me_b, lax.rem(self.me_s + d, parts)) for d in range(1, parts)]
        self.peers = self.mate + self.others

    def barrier(self):
        sem = pltpu.get_barrier_semaphore()
        for peer in self.peers:
            pl.semaphore_signal(sem, inc=1, device_id=peer, device_id_type=MESH)
        pl.semaphore_wait(sem, len(self.peers))

    def copy(self, slot, n, src, dst, peer):
        return pltpu.make_async_remote_copy(
            src_ref=src, dst_ref=dst, send_sem=self.send_sem.at[slot, n],
            recv_sem=self.recv_sem.at[slot, n], device_id=peer, device_id_type=MESH)

    def dims(self, order, stage):
        return [d for d in range(self.bits - 1, -1, -1) if d not in order[:stage]]

    def part(self, c, value):
        mat, col, size, order = self.chunks[c]
        index = tuple(value if d == order[0] else slice(None) for d in self.dims(order, 0))
        return self.mats[mat].at[index + (slice(None), slice(None), pl.ds(col, size))]

    def copies(self, c, stage):
        order = self.chunks[c][3]
        if stage == self.bits:
            return [
                self.copy(c, self.bits + n, self.recv[c][stage - 1].at[peer[1]], self.recv[c][stage].at[n], peer)
                for n, peer in enumerate(self.others)]
        k = order[stage]
        if stage == 0:
            src = self.part(c, 1 - self.bit[k])
        else:
            index = tuple(1 - self.bit[k] if d == k else slice(None) for d in self.dims(order, stage))
            src = self.recv[c][stage - 1].at[index]
        return [self.copy(c, stage, src, self.recv[c][stage], self.mate[k])]

    def start(self, c, stage):
        for copy in self.copies(c, stage):
            copy.start()

    def wait_sends(self, c, stages):
        for stage in range(stages):
            for copy in self.copies(c, stage):
                copy.wait_send()

    def add(self, c, stage):
        mat, col, size, order = self.chunks[c]
        k = order[stage]
        dims = self.dims(order, stage)
        self.copies(c, stage)[0].wait_recv()
        dst = self.recv[c][stage]
        lead = self.bits - 1 - stage

        def one(i, carry):
            part = lax.rem(i, self.parts)
            rest = i // self.parts
            sub = tuple(lax.rem(rest // (1 << (lead - 1 - n)), 2) for n in range(lead))
            at = sub + (part,)
            left = list(sub)
            own_at = tuple(self.bit[k] if d == k else left.pop(0) for d in dims) + (part,)
            if stage > 0:
                own = self.recv[c][stage - 1][own_at]
            elif self.own is None:
                own = self.mats[mat][own_at + (slice(None), pl.ds(col, size))]
            else:
                own = self.own[c][at]
            dst[at] = own + dst[at]
            return carry

        lax.fori_loop(0, self.parts << lead, one, 0)

    def total(self, c):
        total = self.recv[c][self.bits - 1][self.me_s].astype(F32)
        for n, copy in enumerate(self.copies(c, self.bits)):
            copy.wait_recv()
            total = total + self.recv[c][self.bits][n].astype(F32)
        return total


def halving_orders(bits):
    plain = list(range(bits))
    other = [0] + [k for i in range(1, bits, 2) for k in reversed(range(i, min(i + 2, bits)))]
    return plain, other


def halving_scratch(bits, parts, rows, chunks, ends):
    scratch = []
    for (_, _, size, _), end in zip(chunks, ends):
        for stage in range(bits):
            scratch.append(pltpu.VMEM((2,) * (bits - 1 - stage) + (parts, rows, size), BF16))
        if end:
            scratch.append(pltpu.VMEM((parts - 1, rows, size), BF16))
    return scratch


def attend_pair(flag_ref, q_ref, kv_ref, kvp_ref, do_ref, o_ref, dq_ref, dkv_ref, dkvp_ref,
                pt, ds, kvt, qm, dom, midway):
    rows_all = q_ref.shape[0]
    nq = rows_all // QB
    away = (flag_ref[0] - 1).astype(F32) * (-MASKED)
    sources = [(kvp_ref, i) for i in range(nq)] + [(kv_ref, i) for i in range(nq)]

    def block(which, b):
        ref, i = sources[b]
        return ref[which, i * QB:(i + 1) * QB, :]

    for which in range(2):
        kvt[which, :, :rows_all] = kvp_ref[which].T
        kvt[which, :, rows_all:] = kv_ref[which].T
    lane = lax.broadcasted_iota(jnp.int32, (QB, PAIR), 1)
    sub = lax.broadcasted_iota(jnp.int32, (PAIR, QB), 0)
    causal = lax.broadcasted_iota(jnp.int32, (QB, QB), 0) <= lax.broadcasted_iota(
        jnp.int32, (QB, QB), 1)
    for j in range(nq):
        if j == nq // 2:
            midway()
        rows = slice(j * QB, (j + 1) * QB)
        q = q_ref[rows, :] * jnp.asarray(SCALE, BF16)
        qt = q.T
        dot_rows = do_ref[rows, :].astype(F32).T
        blocks = range(nq + j + 1)
        k1 = (nq + j + 1) * QB
        outs, scaled, dqs = [], [], []
        for h in range(2):
            hs = slice(h * HEAD_DIM, (h + 1) * HEAD_DIM)
            qm[h, rows, :] = jnp.where((lane < HEAD_DIM) == (h == 0), q, jnp.zeros_like(q))
            qtm = jnp.where((sub < HEAD_DIM) == (h == 0), qt, jnp.zeros_like(qt))
            scores, tops = [], [None, None]
            for b in blocks:
                s = dot(block(0, b), qtm)
                if b == nq + j:
                    s = jnp.where(causal, s, MASKED)
                scores.append(s)
                part = jnp.max(s.reshape(QB // 8, 8, QB), axis=0)
                side = int(b >= nq)
                tops[side] = part if tops[side] is None else jnp.maximum(tops[side], part)
            top = jnp.max(jnp.maximum(tops[0] + away, tops[1]), axis=0, keepdims=True)
            shift = (top - away, top)
            total = None
            for b, s in zip(blocks, scores):
                p = jnp.exp(s - shift[int(b >= nq)])
                part = jnp.sum(p.reshape(QB // 8, 8, QB), axis=0)
                total = part if total is None else total + part
                pt[h, b * QB:(b + 1) * QB, rows] = p.astype(BF16)
            inv = 1.0 / jnp.sum(total, axis=0, keepdims=True)
            out_t = dot(kvt[1, hs, :k1], pt[h, :k1, rows]) * inv
            dol_t = dot_rows[hs] * inv
            delta = jnp.sum(dol_t * out_t, axis=0, keepdims=True)
            outs.append(out_t)
            scaled.append(dol_t)
            zero = jnp.zeros((HEAD_DIM, QB), BF16)
            dol_b = dol_t.astype(BF16)
            dol_m = jnp.concatenate([dol_b, zero] if h == 0 else [zero, dol_b], axis=0)
            for b in blocks:
                dp = dot(block(1, b), dol_m)
                d = pt[h, b * QB:(b + 1) * QB, rows].astype(F32) * (dp - delta)
                ds[h, b * QB:(b + 1) * QB, rows] = d.astype(BF16)
            dqs.append(dot(kvt[0, hs, :k1], ds[h, :k1, rows]) * SCALE)
        o_ref[rows, :] = jnp.concatenate(outs, 0).T.astype(BF16)
        dq_ref[rows, :] = jnp.concatenate(dqs, 0).T.astype(BF16)
        dol = jnp.concatenate(scaled, 0).T.astype(BF16)
        for h in range(2):
            dom[h, rows, :] = jnp.where((lane < HEAD_DIM) == (h == 0), dol, jnp.zeros_like(dol))
    for b in range(2 * nq):
        q0 = max(0, b - nq) * QB
        br = slice(b * QB, (b + 1) * QB)
        dk = dot(ds[0, br, q0:], qm[0, q0:, :]) + dot(ds[1, br, q0:], qm[1, q0:, :])
        dv = dot(pt[0, br, q0:], dom[0, q0:, :]) + dot(pt[1, br, q0:], dom[1, q0:, :])
        ref, i = (dkvp_ref, b) if b < nq else (dkv_ref, b - nq)
        ref[0, i * QB:(i + 1) * QB, :] = dk.astype(BF16)
        ref[1, i * QB:(i + 1) * QB, :] = dv.astype(BF16)


def fold_rows(out_ref, total):
    take, width = total.shape[0], out_ref.shape[1]
    for j in range(total.shape[1] // width):
        out_ref[j * take:(j + 1) * take, :] = total[:, j * width:(j + 1) * width]


def attend_kernel(bits, parts, chunks, ends, flag_ref, q_ref, kv_ref, kv_hbm, kvp_hbm, do_ref, gw_ref, gr_ref,
                  o_ref, dq_ref, dkv_ref, dkvn_ref, partw_ref, partr_ref, totw_ref, totr_ref, *refs):
    nchunk = len(chunks)
    own, refs = refs[:nchunk], refs[nchunk:]
    recv = []
    for end in ends:
        recv.append(refs[:bits + end])
        refs = refs[bits + end:]
    (pt, ds, kvt, qm, dom, back, kvp, own_sem, send_sem, recv_sem, back_send, back_recv,
     kv_load, kv_send, kv_recv) = refs
    red = Halving(bits, parts, chunks, (gw_ref, gr_ref), own, recv, send_sem, recv_sem)
    step = pl.program_id(0)
    steps = dkvn_ref.shape[2] // PAIR

    def own_copy(c):
        return pltpu.make_async_copy(red.part(c, red.bit[chunks[c][3][0]]), own[c], own_sem.at[c])

    def back_copy(i):
        cols = pl.ds(pl.multiple_of(i * PAIR, PAIR), PAIR)
        return pltpu.make_async_remote_copy(
            src_ref=back.at[lax.rem(i, 2)], dst_ref=dkvn_ref.at[:, :, cols],
            send_sem=back_send.at[i], recv_sem=back_recv.at[i],
            device_id=red.others[parts - 2], device_id_type=MESH)

    first, last = red.me_s == 0, red.me_s == parts - 1
    half_steps = steps // 2

    def pair_cols(i):
        return pl.ds(pl.multiple_of(i * PAIR, PAIR), PAIR)

    def load_copy(i):
        return pltpu.make_async_copy(kvp_hbm.at[:, :, pair_cols(i)], kvp.at[i], kv_load.at[i])

    def onward_copy(i):
        return pltpu.make_async_remote_copy(
            src_ref=kv_hbm.at[:, :, pair_cols(i)], dst_ref=kvp.at[i],
            send_sem=kv_send.at[i - half_steps], recv_sem=kv_recv.at[i - half_steps],
            device_id=red.others[0], device_id_type=MESH)

    @pl.when(step == 0)
    def _():
        red.barrier()
        for i in range(half_steps):
            load_copy(i).start()
        for c in range(nchunk):
            red.start(c, 0)
            own_copy(c).start()

    @pl.when(jnp.logical_and(step == 0, jnp.logical_not(last)))
    def _():
        for i in range(half_steps, steps):
            onward_copy(i).start()

    @pl.when(jnp.logical_and(step == 0, first))
    def _():
        kvp[half_steps:] = jnp.zeros((steps - half_steps,) + kvp.shape[1:], BF16)

    moments = {}
    for c in range(nchunk):
        times = (2, 5, 7) if ends[c] else (5, 10, 13)
        for stage in range(bits):
            at = times[min(stage, 2)] + max(0, stage - 2)
            moments.setdefault(min(at * steps // 8, 2 * steps - 1), []).append((c, stage))

    def advance(half):
        for at, work in moments.items():
            if at % 2 == half:
                @pl.when(step == at // 2)
                def _(work=work):
                    for c, stage in work:
                        if stage == 0:
                            own_copy(c).wait()
                        red.add(c, stage)
                        if stage + 1 < bits + ends[c]:
                            red.start(c, stage + 1)

    slot = lax.rem(step, 2)

    @pl.when(jnp.logical_and(step == 0, last))
    def _():
        back[1] = jnp.zeros(back.shape[1:], BF16)
        fills = [pltpu.make_async_copy(back.at[1], dkvn_ref.at[:, :, pl.ds(i * PAIR, PAIR)], back_recv.at[i])
                 for i in range(steps)]
        for fill in fills:
            fill.start()
        for fill in fills:
            fill.wait()

    advance(0)

    @pl.when(jnp.logical_and(step >= 2, jnp.logical_not(first)))
    def _():
        back_copy(step - 2).wait_send()

    @pl.when(step < half_steps)
    def _():
        load_copy(step).wait()

    @pl.when(jnp.logical_and(step >= half_steps, jnp.logical_not(first)))
    def _():
        onward_copy(step).wait_recv()

    attend_pair(flag_ref, q_ref, kv_ref, kvp.at[step], do_ref, o_ref, dq_ref, dkv_ref,
                back.at[slot], pt, ds, kvt, qm, dom, lambda: advance(1))

    @pl.when(jnp.logical_not(first))
    def _():
        back_copy(step).start()

    @pl.when(step == steps - 1)
    def _():
        for c in range(nchunk):
            mat, col, size, _ = chunks[c]
            if not ends[c]:
                (partw_ref, partr_ref)[mat][...] = recv[c][bits - 1][...]
            red.wait_sends(c, bits + ends[c])
        for c in range(nchunk):
            mat, col, size, _ = chunks[c]
            if ends[c] and mat == 0:
                totw_ref[...] = red.total(c)
            elif ends[c]:
                fold_rows(totr_ref, red.total(c))

        @pl.when(jnp.logical_not(last))
        def _():
            for i in range(half_steps, steps):
                onward_copy(i).wait_send()

        @pl.when(jnp.logical_not(first))
        def _():
            for i in range(max(0, steps - 2), steps):
                back_copy(i).wait_send()

        @pl.when(jnp.logical_not(last))
        def _():
            for i in range(steps):
                back_copy(i).wait_recv()


def attend(bits, parts, flag, q, kv, kvp, do, gw, gr):
    rows, width = q.shape
    steps = width // PAIR
    hidden = gr.shape[1]
    take = gw.shape[0] // (parts << bits)
    shaped = [g.reshape((2,) * bits + (parts, take, g.shape[1])) for g in (gw, gr)]
    plain, other = halving_orders(bits)
    chunks = [(0, 0, hidden // 2, plain), (1, 0, hidden // 2, other),
              (0, hidden // 2, hidden // 2, plain), (1, hidden // 2, hidden // 2, other)]
    npeer = bits + parts - 1
    tok = pl.BlockSpec((rows, PAIR), lambda i: (0, i))
    kvs = pl.BlockSpec((2, rows, PAIR), lambda i: (0, 0, i))
    hbm = pl.BlockSpec(memory_space=pl.ANY)
    tok_shape = jax.ShapeDtypeStruct((rows, width), BF16)
    kv_shape = jax.ShapeDtypeStruct((2, rows, width), BF16)
    ends = (1, 1, 0, 0)
    part = (parts, take, hidden // 2)
    totw, totr = (take, hidden // 2), (take * hidden // 2 // width, width)
    return pl.pallas_call(
        partial(attend_kernel, bits, parts, chunks, ends),
        grid=(steps,),
        out_shape=(tok_shape, tok_shape, kv_shape, kv_shape,
                   jax.ShapeDtypeStruct(part, BF16), jax.ShapeDtypeStruct(part, BF16),
                   jax.ShapeDtypeStruct(totw, F32), jax.ShapeDtypeStruct(totr, F32)),
        in_specs=[pl.BlockSpec(memory_space=pltpu.SMEM), tok, kvs, hbm, hbm, tok, hbm, hbm],
        out_specs=(tok, tok, kvs, hbm, whole(part), whole(part), whole(totw), whole(totr)),
        scratch_shapes=[
            pltpu.VMEM((2,) * (bits - 1) + (parts, take, size), BF16) for _, _, size, _ in chunks
        ] + halving_scratch(bits, parts, take, chunks, ends) + [
            pltpu.VMEM((2, 2 * rows, rows), BF16),
            pltpu.VMEM((2, 2 * rows, rows), BF16),
            pltpu.VMEM((2, PAIR, 2 * rows), BF16),
            pltpu.VMEM((2, rows, PAIR), BF16),
            pltpu.VMEM((2, rows, PAIR), BF16),
            pltpu.VMEM((2, 2, rows, PAIR), BF16),
            pltpu.VMEM((steps, 2, rows, PAIR), BF16),
            pltpu.SemaphoreType.DMA((len(chunks),)),
            pltpu.SemaphoreType.DMA((len(chunks), npeer)),
            pltpu.SemaphoreType.DMA((len(chunks), npeer)),
            pltpu.SemaphoreType.DMA((steps,)),
            pltpu.SemaphoreType.DMA((steps,)),
            pltpu.SemaphoreType.DMA((steps // 2,)),
            pltpu.SemaphoreType.DMA((steps - steps // 2,)),
            pltpu.SemaphoreType.DMA((steps - steps // 2,)),
        ],
        compiler_params=pltpu.CompilerParams(
            vmem_limit_bytes=63 << 20, collective_id=1, has_side_effects=True),
        cost_estimate=cost(60 * rows * rows * width, 20 * rows * width),
        name="attend",
    )(flag, q, kv, kv, kvp, do, *shaped)


def dense_kernel(o_ref, wd_ref, db_ref, rb_ref, mid_ref, x_ref, og_ref, out_ref, dwd_ref, ot):
    @pl.when(pl.program_id(0) == 0)
    def _():
        ot[...] = o_ref[...].T

    total = x_ref[...].astype(F32) + mid_ref[...] + (db_ref[...] + rb_ref[...])
    out_ref[...] = (total + dot(o_ref[...], wd_ref[...])).astype(BF16)
    dwd_ref[...] = dot(ot[...], og_ref[...]).astype(BF16)


def dense(o, wd, db, rb, mid, x, og):
    rows, width = x.shape
    blk = 512
    col = lambda r: pl.BlockSpec((r, blk), lambda i: (0, i))
    return pl.pallas_call(
        dense_kernel,
        grid=(width // blk,),
        out_shape=(jax.ShapeDtypeStruct((rows, width), BF16), jax.ShapeDtypeStruct((width, width), BF16)),
        in_specs=[whole(o.shape), col(width), col(1), col(1), col(rows), col(rows), col(rows)],
        out_specs=(col(rows), col(width)),
        scratch_shapes=[pltpu.VMEM((width, rows), BF16)],
        compiler_params=params(),
        cost_estimate=cost(4 * rows * width * width, 12 * rows * width),
        name="dense",
    )(o, wd, db, rb, mid, x, og)


def tail_kernel(bits, parts, chunks, x_ref, gain_ref, gain2_ref, norm_t, w_ref, ang_ref, dq_ref, dkv_ref,
                dkvn_ref, og_ref, sg_ref, dwd_ref, partw_ref, partr_ref, dog_ref, dbe_ref,
                ig_ref, dw_out, dwd_out, dwe_out, dwr_out, vec_out, *refs):
    nchunk = len(chunks)
    recv = [refs[c * (bits + 1):(c + 1) * (bits + 1)] for c in range(nchunk)]
    (tab, fg, dw, db, dgain, dshift, dgain2, dshift2, zw, zr, state, vrecv, send_sem, recv_sem) = refs[
        nchunk * (bits + 1):]
    red = Halving(bits, parts, chunks, (dw, dwd_ref), None, recv, send_sem, recv_sem)
    step = pl.program_id(0)
    steps = pl.num_programs(0)
    width = x_ref.shape[1]
    nstep = width // (STEP_PAIRS * PAIR)
    cols = 3 * STEP_PAIRS * PAIR

    done = set()

    def forward(c, stage):
        if (c, stage) not in done:
            done.add((c, stage))
            red.add(c, stage)
            red.start(c, stage + 1)

    def z_copies():
        return [red.copy(nchunk + 1 + m, bits + n, part.at[peer[1]], dst.at[n], peer)
                for m, (part, dst) in enumerate(((partw_ref, zw), (partr_ref, zr)))
                for n, peer in enumerate(red.others)]

    @pl.when(step == 0)
    def _():
        red.barrier()
        for copy in z_copies():
            copy.start()
        for c in range(nstep, nchunk):
            red.start(c, 0)
        build_tables(ang_ref, tab)
        fg[...] = jnp.zeros_like(fg)

    for c in range(1, nstep):
        @pl.when(step == c)
        def _(c=c):
            red.start(c - 1, 0)
            if c == 1:
                for extra in range(nstep, nchunk):
                    forward(extra, 0)
            else:
                forward(c - 2, 0)
            if c == nstep - 1:
                for extra in range(nstep, nchunk):
                    forward(extra, 1)

    blocks = []
    for n in range(STEP_PAIRS):
        mine = slice(n * PAIR, (n + 1) * PAIR)
        dq = turn(dq_ref[:, mine].astype(F32), tab, -1.0)
        dk = turn(dkv_ref[0, :, mine].astype(F32) + dkvn_ref[0, :, mine].astype(F32), tab, -1.0)
        dv = dkv_ref[1, :, mine].astype(F32) + dkvn_ref[1, :, mine].astype(F32)
        low = low_lanes(dq.shape)
        dk = pltpu.roll(dk, HEAD_DIM, 1)
        blocks += [jnp.where(low, dq, dk), jnp.where(low, dv, dq), jnp.where(low, dk, dv)]
    dm = jnp.concatenate(blocks, axis=1).astype(BF16)
    at = pl.ds(pl.multiple_of(step * cols, cols), cols)
    db[:, at] = jnp.sum(dm.astype(F32), axis=0, keepdims=True)
    dw[(slice(None),) * (bits + 2) + (at,)] = dot(norm_t[...], dm).reshape(
        dw.shape[:-1] + (cols,)).astype(BF16)
    fg[...] += dot_t(dm, w_ref[...])

    def vec_copies(stage):
        if stage < bits:
            return [red.copy(nchunk, stage, state.at[stage], vrecv.at[stage], red.mate[stage])]
        return [red.copy(nchunk, bits + n, state.at[bits], vrecv.at[bits + n], peer)
                for n, peer in enumerate(red.others)]

    def vec_start(stage):
        for copy in vec_copies(stage):
            copy.start()

    def vec_add(stage):
        copies = vec_copies(stage)
        for copy in copies:
            copy.wait_recv()
        total = state[stage]
        for n in range(len(copies)):
            total = total + vrecv[stage + n]
        if stage < bits:
            state[stage + 1] = total
            vec_start(stage + 1)
        else:
            vec_out[...] = total

    @pl.when(step == steps - 1)
    def _():
        red.start(nstep - 1, 0)
        forward(nstep - 2, 0)

        def emit(rows, part):
            ig_ref[rows, :] = (og_ref[rows, :].astype(F32) + part).astype(BF16)

        forward(nstep - 1, 0)
        forward(0, 1)
        norm_args = (x_ref, (gain_ref, gain2_ref), (fg, sg_ref), (dgain, dgain2), (dshift, dshift2), emit)
        row_blocks = x_ref.shape[0] // ROWS
        norm_back(*norm_args, 0, row_blocks // 2)
        forward(1, 1)
        for extra in range(nstep, nchunk):
            forward(extra, 2)
        norm_back(*norm_args, row_blocks // 2, row_blocks)
        begin = 0
        for ref in (dgain, dshift, db, dog_ref, dgain2, dshift2, dbe_ref):
            state[0, :, begin:begin + ref.shape[1]] = ref[...]
            begin += ref.shape[1]
        vec_start(0)
        order = list(range(nstep, nchunk)) + list(range(nstep))
        for stage in range(1, bits):
            for c in order:
                forward(c, stage)
            vec_add(stage - 1)
        copies = z_copies()
        for m, (part, got, out) in enumerate(((partw_ref, zw, dwe_out), (partr_ref, zr, dwr_out))):
            total = part[red.me_s].astype(F32)
            for n in range(parts - 1):
                copies[m * (parts - 1) + n].wait_recv()
                total = total + got[n].astype(F32)
            if m == 0:
                out[...] = total
            else:
                fold_rows(out, total)
        vec_add(bits - 1)
        for c in order:
            mat, col, size, _ = chunks[c]
            (dw_out, dwd_out)[mat][:, col:col + size] = red.total(c)
        vec_add(bits)
        for c in range(nchunk):
            red.wait_sends(c, bits + 1)
        for copy in copies:
            copy.wait_send()
        for stage in range(bits + 1):
            for copy in vec_copies(stage):
                copy.wait_send()


def tail(bits, parts, x, gain, gain2, norm_t, w, ang, dq, dkv, dkvn, og, sg, dwd, partw, partr, dog, dbe):
    rows, width = x.shape
    full, vec = whole((rows, width)), whole((1, width))
    wide = STEP_PAIRS * PAIR
    cols = 3 * wide
    nstep = width // wide
    hidden, part = dbe.shape[1], partw.shape[2]
    take = width // (parts << bits)
    total = 5 * width + 3 * width + hidden
    npeer = bits + parts - 1
    lead = (2,) * bits + (parts, take)
    plain, other = halving_orders(bits)
    chunks = [(0, n * cols, cols, other if n % 2 else plain) for n in range(nstep)]
    chunks += [(1, n * (width // 2), width // 2, other if n % 2 else plain) for n in range(2)]
    tok = pl.BlockSpec((rows, wide), lambda i: (0, i))
    kvs = pl.BlockSpec((2, rows, wide), lambda i: (0, 0, i))
    up = pl.BlockSpec((width, cols), lambda i: (0, i))
    dwd = dwd.reshape(lead + (width,))
    outs = [((rows, width), BF16), ((take, 3 * width), F32), ((take, width), F32), ((take, part), F32),
            ((take * part // width, width), F32), ((1, total), F32)]
    row_vec = pltpu.VMEM((1, width), F32)
    nsem = (len(chunks) + 3, npeer)
    return pl.pallas_call(
        partial(tail_kernel, bits, parts, chunks),
        grid=(nstep,),
        out_shape=tuple(jax.ShapeDtypeStruct(s, d) for s, d in outs),
        in_specs=[full, vec, vec, whole(norm_t.shape), up, whole(ang.shape), tok, kvs, kvs, full, full,
                  whole(dwd.shape), whole(partw.shape), whole(partr.shape), vec, whole(dbe.shape)],
        out_specs=tuple(whole(s) for s, _ in outs),
        scratch_shapes=halving_scratch(bits, parts, take, chunks, [1] * len(chunks)) + [
            pltpu.VMEM((3, rows, PAIR), F32), pltpu.VMEM((rows, width), F32),
            pltpu.VMEM(lead + (3 * width,), BF16), pltpu.VMEM((1, 3 * width), F32),
            row_vec, row_vec, row_vec, row_vec,
            pltpu.VMEM((parts - 1, take, part), BF16), pltpu.VMEM((parts - 1, take, part), BF16),
            pltpu.VMEM((bits + 1, 1, total), F32), pltpu.VMEM((npeer, 1, total), F32),
            pltpu.SemaphoreType.DMA(nsem), pltpu.SemaphoreType.DMA(nsem),
        ],
        compiler_params=pltpu.CompilerParams(
            vmem_limit_bytes=63 << 20, collective_id=0, has_side_effects=True),
        cost_estimate=cost(12 * rows * width * width, 8 * rows * width),
        name="tail",
    )(x, gain, gain2, norm_t, w, ang, dq, dkv, dkvn, og, sg, dwd, partw, partr, dog, dbe)


def finish_kernel(sizes, index_ref, ig_ref, dw_ref, dwd_ref, dwe0_ref, dwe1_ref, dwr0_ref, dwr1_ref, vec_ref,
                  ig_out, dw_out, dwd_out, dwe_out, dwr_out, *outs):
    for src, dst in ((ig_ref, ig_out), (dw_ref, dw_out), (dwd_ref, dwd_out)):
        dst[...] = src[...]
    half = dwe0_ref.shape[1]
    dwe_out[:, :half] = dwe0_ref[...]
    dwe_out[:, half:] = dwe1_ref[...]
    half = dwr0_ref.shape[0]
    dwr_out[:half, :] = dwr0_ref[...]
    dwr_out[half:, :] = dwr1_ref[...]
    at = 0
    for size, out in zip(sizes, outs):
        own = out.shape[1]
        row = jnp.broadcast_to(vec_ref[:, at:at + size], (8, size))
        out[...] = pltpu.roll(row, lax.rem(size - index_ref[0] * own, size), 1)[:1, :own]
        at += size


def finish(index, ndev, sizes, ig, dw, dwd, dwe0, dwe1, dwr0, dwr1, vec):
    mats = (ig, dw, dwd, dwe0, dwe1, dwr0, dwr1)
    outs = [(m.shape, m.dtype) for m in (ig, dw, dwd)] + [
        ((dwe0.shape[0], 2 * dwe0.shape[1]), F32), ((2 * dwr0.shape[0], dwr0.shape[1]), F32)]
    outs += [((1, n // ndev), F32) for n in sizes]
    return pl.pallas_call(
        partial(finish_kernel, sizes),
        out_shape=tuple(jax.ShapeDtypeStruct(s, d) for s, d in outs),
        grid=(1,),
        in_specs=[pl.BlockSpec(memory_space=pltpu.SMEM)] + [whole(m.shape) for m in mats] + [whole(vec.shape)],
        out_specs=tuple(whole(s) for s, _ in outs),
        compiler_params=params(),
        name="finish",
    )(index, *mats, vec)


def body(
    tokens,
    seq_lengths,
    attn_gain,
    attn_shift,
    qkv_weight,
    qkv_bias,
    dense_weight,
    dense_bias,
    mlp_gain,
    mlp_shift,
    expand_weight,
    expand_bias,
    reduce_weight,
    reduce_bias,
    out_grad,
):
    seq_parts = lax.axis_size("seq")
    place = lax.axis_index("seq")
    rows, width = tokens.shape
    lengths = seq_lengths[0]
    starts = jnp.cumsum(lengths) - lengths
    row0 = place * rows
    offset = row0 - jnp.max(jnp.where(starts <= row0, starts, 0))
    flag = (offset > 0).astype(jnp.int32).reshape(1)
    positions = (offset + jnp.arange(rows, dtype=jnp.int32)).astype(F32)
    frequency = jnp.exp(jnp.arange(ROT // 2, dtype=F32) * (-2.0 * math.log(10000.0) / ROT))
    phases = frequency[:, None] * positions[None, :]
    ang = jnp.concatenate([jnp.cos(phases), jnp.sin(phases)], axis=0)

    row = lambda v: v.reshape(1, -1)
    ag, ash, mg, msh = row(attn_gain), row(attn_shift), row(mlp_gain), row(mlp_shift)

    batch_parts = lax.axis_size("batch")
    ndev = batch_parts * seq_parts
    bits = batch_parts.bit_length() - 1
    q, kv, kvh, do, n1t, n2, n2t = project(
        tokens, ag, ash, mg, msh, qkv_weight, row(qkv_bias), ang, out_grad, dense_weight)
    mid, dwr, dog, sg, dwe, dbe, kvp = mlp(
        ndev, seq_parts, n2, n2t, expand_weight, row(expand_bias), reduce_weight, out_grad, kvh)
    o, dq, dkv, dkvn, partw, partr, totw, totr = attend(bits, seq_parts, flag, q, kv, kvp, do, dwe, dwr)
    layer_out, dwd = dense(o, dense_weight, row(dense_bias), row(reduce_bias), mid, tokens, out_grad)
    input_grad, dw, dwd, dwe, dwr, vsum = tail(
        bits, seq_parts, tokens, ag, mg, n1t, qkv_weight, ang, dq, dkv, dkvn, out_grad, sg, dwd,
        partw, partr, dog, dbe)
    index = lax.axis_index("batch") * seq_parts + place
    sizes = (width, width, 3 * width, width, width, width, dbe.shape[1])
    input_grad, dw, dwd, dwe, dwr, *vectors = finish(
        index.astype(jnp.int32).reshape(1), ndev, sizes, input_grad, dw, dwd, totw, dwe, totr, dwr, vsum)
    dag, das, dqb, dog, dmg, dms, dbe = [v.reshape(-1) for v in vectors]
    return (
        layer_out,
        input_grad,
        dag,
        das,
        dw,
        dqb,
        dwd,
        dog,
        dmg,
        dms,
        dwe,
        dbe,
        dwr,
        dog,
    )


def solution(mesh):
    tok = P(("batch", "seq"), None)
    vec = P(("batch", "seq"))
    in_specs = (tok, P("batch", None)) + (P(),) * 12 + (tok,)
    out_specs = (tok, tok, vec, vec, tok, vec, tok, vec, vec, vec, tok, vec, tok, vec)
    return jax.shard_map(body, mesh=mesh, in_specs=in_specs, out_specs=out_specs, check_vma=False)
```
